32 devices in a mesh: dom: 8 (over z, y), ray: 4 (over x, core).
Axes of the slice: x: 2, y: 2, z: 4, core: 2. Of those that a mesh axis runs over, the one named last changes fastest.
Arguments:
- projections: bfloat16 [8, 64, 8192], P('dom', None, 'ray'), may hold values from -6 to 6
- phase_kernel: bfloat16 [129], replicated, may hold values from -0.5 to 0.5
- image: bfloat16 [16384, 64], P('dom'), may hold values from -6 to 6
- tile_library: bfloat16 [8, 4, 16, 128, 128], P('dom', 'ray'), may hold values from -0.09375 to 0.09375
- tile_entry: int32 [8, 4, 256], P('dom', 'ray'), may hold values from 0 to 15
- tile_image: int32 [8, 4, 256], P('dom', 'ray'), may hold values from 0 to 15
- tile_slot: int32 [8, 4, 256], P('dom', 'ray'), may hold values from 0 to 7
- tile_count: int32 [8, 4], P('dom', 'ray'), may hold values from 64 to 256, as said below
- slot_block: int32 [8, 4, 8], P('dom', 'ray'), may hold values from 0 to 15
Outputs:
- residual: bfloat16 [8, 64, 8192], P('dom', None, 'ray')
- image_next: float32 [16384, 64], P(('dom', 'ray'))
The draws below stay inside these ranges and needn't reach their ends.
Inputs may be any that keep to these rules, and one draw needn't show every extreme that they name: `tile_count`: each device has at most 256 live tiles; some device holds exactly 256. Entries beyond a device's count are not used.
All inputs are finite; a program needn't handle non-finite values.
Results may differ from the reference program's by a relative error of at most 0.0075.
Values may be sent and summed in bfloat16 or wider, within the bound.
A program may use at most 64 MiB of HBM per device.

```python
import jax
import jax.numpy as jnp
from jax import lax

DET = 8192
TILE = 128
HALF = 64
SMOOTH = 8
ANG_DEV = 1
SLICES = 64
IB_DEV = 16
TILE_CAP = 256
LIB = 16
NA = 8
RAY_BLOCKS = 16
PIX = 16384
N_DOM = 8
N_RAY = 4


def draw_projections(key, part):
    background_key, stripe_key = jax.random.split(jax.random.fold_in(key, 11), 2)
    background = jnp.clip(jax.random.normal(background_key, (NA, SLICES, DET), jnp.float32), -4.0, 4.0)
    stripes = jnp.clip(jax.random.normal(stripe_key, (1, SLICES, DET), jnp.float32), -2.0, 2.0)
    return (background + stripes).astype(jnp.bfloat16)


def draw_tile_count(key, part):
    divisor_key, busiest_key = jax.random.split(jax.random.fold_in(key, 7))
    divisor = jax.random.randint(divisor_key, (N_DOM * N_RAY,), 1, 5)
    counts = TILE_CAP // divisor
    busiest = jax.random.randint(busiest_key, (), 0, N_DOM * N_RAY)
    counts = counts.at[busiest].set(TILE_CAP)
    return counts.reshape(N_DOM, N_RAY).astype(jnp.int32)


def with_ends(values, rng, least, top_value):
    extent = values.shape
    spot = [jax.random.randint(jax.random.fold_in(rng, axis), (), 0, extent[axis]) for axis in range(len(extent))]
    values = values.at[tuple(spot)].set(least)
    longest = extent.index(max(extent))
    spot[longest] = (spot[longest] + 1) % extent[longest]
    return values.at[tuple(spot)].set(top_value)


def shard_levels(stream_key, extent, cuts, smallest, top_value):
    loudness, own = 1.0, jax.random.fold_in(stream_key, 6)
    for axis_at, shards_of in cuts:
        draws = jnp.exp(jax.random.uniform(jax.random.fold_in(own, axis_at), (shards_of,), jnp.float32, smallest / len(cuts), top_value / len(cuts)))
        loudness = loudness * jnp.repeat(draws, extent[axis_at] // shards_of).reshape([-1 if axis == axis_at else 1 for axis in range(len(extent))])
    return loudness


def bell_draw(rng, extent, spread, reach, pieces=(), kind=jnp.bfloat16):
    drawn = spread * jax.random.normal(rng, extent, jnp.float32)
    if pieces:
        drawn = drawn * shard_levels(rng, extent, pieces, -0.22, 0.18)
    return jnp.clip(drawn, -reach, reach).astype(kind)


def setup_inputs(seed: int = 0) -> dict:
    key_list = jax.random.split(jax.random.key(seed), 10)
    projections = draw_projections(jax.random.fold_in(key_list[9], 71), 0)
    phase_kernel = bell_draw(key_list[1], (2 * HALF + 1,), (2 * HALF + 1) ** -0.5, 0.5)
    image = bell_draw(key_list[2], (PIX, SLICES), 1.0, 6.0, ((0, 8),))
    tile_library = bell_draw(key_list[3], (N_DOM, N_RAY, LIB, TILE, TILE), (TILE * TILE_CAP // N_DOM) ** -0.5, 0.09375, ((0, 8), (1, 4)))
    tile_entry = with_ends(jax.random.randint(key_list[4], (N_DOM, N_RAY, TILE_CAP), 0, LIB), jax.random.fold_in(key_list[4], 1), 0, LIB - 1).astype(jnp.int32)
    tile_image = with_ends(jax.random.randint(key_list[5], (N_DOM, N_RAY, TILE_CAP), 0, IB_DEV), jax.random.fold_in(key_list[5], 1), 0, IB_DEV - 1).astype(jnp.int32)
    tile_slot = with_ends(jax.random.randint(key_list[6], (N_DOM, N_RAY, TILE_CAP), 0, N_DOM), jax.random.fold_in(key_list[6], 1), 0, N_DOM - 1).astype(jnp.int32)
    tile_count = draw_tile_count(jax.random.fold_in(key_list[9], 71), 0)
    slot_block = with_ends(jax.random.randint(key_list[8], (N_DOM, N_RAY, N_DOM), 0, RAY_BLOCKS), jax.random.fold_in(key_list[8], 1), 0, RAY_BLOCKS - 1).astype(jnp.int32)
    return dict(projections=projections, phase_kernel=phase_kernel, image=image, tile_library=tile_library, tile_entry=tile_entry, tile_image=tile_image, tile_slot=tile_slot, tile_count=tile_count, slot_block=slot_block)


relax_factor = 0.25


def toeplitz(kernel, tile_size):
    taps = kernel.shape[0]
    padded = jnp.concatenate([kernel, jnp.zeros((2 * tile_size + 1 - taps,), kernel.dtype)])
    tiled = jnp.tile(padded, tile_size)[: 2 * tile_size * tile_size]
    return tiled.reshape(tile_size, 2 * tile_size).T


def phase_angle(row_block, kernel):
    half_width = (kernel.shape[0] - 1) // 2
    block_count = DET // TILE
    padded = jnp.pad(row_block, ((0, 0), (half_width, 2 * TILE - half_width)))
    blocks = padded.reshape(SLICES, block_count + 2, TILE)
    windows = jnp.concatenate([blocks[:, :block_count], blocks[:, 1:block_count + 1]], axis=-1)
    weights = toeplitz(kernel, TILE).astype(jnp.float32)
    filtered = jnp.einsum("sbi,ij->sbj", windows.astype(jnp.float32), weights)
    return filtered.reshape(SLICES, DET).astype(jnp.bfloat16)


def reference(projections, phase_kernel, image, tile_library, tile_entry, tile_image, tile_slot, tile_count, slot_block):
    phase = lax.map(lambda row_block: phase_angle(row_block, phase_kernel), projections)
    by_slice = jnp.swapaxes(phase, 0, 1)
    profile = lax.map(lambda plane: jnp.median(plane.astype(jnp.float32), axis=0), by_slice)
    padded = jnp.pad(profile, ((0, 0), (SMOOTH, SMOOTH)))
    window_sum = jnp.zeros_like(profile)
    for offset in range(2 * SMOOTH + 1):
        window_sum = window_sum + padded[:, offset:offset + DET]
    position = jnp.arange(DET)
    in_range = (jnp.minimum(position + SMOOTH, DET - 1) - jnp.maximum(position - SMOOTH, 0) + 1).astype(jnp.float32)
    stripe = (profile - window_sum / in_range).astype(jnp.bfloat16)
    corrected = (phase.astype(jnp.float32) - stripe.astype(jnp.float32)[None]).astype(jnp.bfloat16)

    block_count = DET // TILE
    per_owner = DET // (N_RAY * TILE)
    image_blocks = image.reshape(N_DOM, IB_DEV, TILE, SLICES)

    def device_tiles(device_index):
        subdomain = device_index // N_RAY
        quarter = device_index % N_RAY
        library = tile_library[subdomain, quarter]
        entries = tile_entry[subdomain, quarter]
        images = tile_image[subdomain, quarter]
        slots = tile_slot[subdomain, quarter]
        live_mask = jnp.arange(TILE_CAP) < tile_count[subdomain, quarter]
        matrices = library[entries].astype(jnp.float32)
        return subdomain, quarter, matrices, images, slots, live_mask

    def ray_targets(subdomain, quarter):
        carried = slot_block[:, quarter, subdomain]
        angle_index = jnp.arange(N_DOM) * ANG_DEV + carried // per_owner
        column_block = quarter * per_owner + carried % per_owner
        return angle_index, column_block

    def forward_step(device_index, forward):
        subdomain, quarter, matrices, images, slots, live_mask = device_tiles(device_index)
        target = jnp.where(live_mask, slots, N_DOM)
        sources = image_blocks[subdomain][images].astype(jnp.float32)
        product = jnp.einsum("krp,kps->ksr", matrices, sources)
        partial_value = jnp.zeros((N_DOM, SLICES, TILE), jnp.float32).at[target].add(product, mode="drop")
        rounded = lax.optimization_barrier(partial_value.astype(jnp.bfloat16))
        angle_index, column_block = ray_targets(subdomain, quarter)
        return forward.at[angle_index, :, column_block, :].add(rounded.astype(jnp.float32))

    forward = lax.fori_loop(0, N_DOM * N_RAY, forward_step, jnp.zeros((NA, SLICES, block_count, TILE), jnp.float32))
    residual = (corrected.astype(jnp.float32) - forward.reshape(NA, SLICES, DET)).astype(jnp.bfloat16)
    residual_blocks = residual.reshape(NA, SLICES, block_count, TILE)

    def adjoint_step(device_index, gradient):
        subdomain, quarter, matrices, images, slots, live_mask = device_tiles(device_index)
        angle_index, column_block = ray_targets(subdomain, quarter)
        returned = residual_blocks[angle_index, :, column_block, :].astype(jnp.float32)
        image_target = jnp.where(live_mask, images, IB_DEV)
        product = jnp.einsum("krp,ksr->kps", matrices, returned[slots])
        local_sum = jnp.zeros((IB_DEV, TILE, SLICES), jnp.float32).at[image_target].add(product, mode="drop")
        return gradient.at[subdomain].add(local_sum)

    gradient = lax.fori_loop(0, N_DOM * N_RAY, adjoint_step, jnp.zeros((N_DOM, IB_DEV, TILE, SLICES), jnp.float32))
    image_next = image.astype(jnp.float32) + relax_factor * gradient.reshape(PIX, SLICES)
    return residual, image_next
```

```python
import functools

import jax
import jax.numpy as jnp
from jax import lax
from jax.experimental import pallas as pl
from jax.experimental.pallas import tpu as pltpu
from jax.sharding import PartitionSpec as P

SMOOTH = 8


relax_factor = 0.25


def with_halo(cells, sides, width):
    for axis, dim in sides:
        count = lax.axis_size(axis)
        ends = count - 1
        head = lax.slice_in_dim(cells, 0, width, axis=dim)
        tail = lax.slice_in_dim(cells, cells.shape[dim] - width, cells.shape[dim], axis=dim)
        cells = jnp.concatenate(
            [
                lax.ppermute(tail, axis, [(i, (i + 1) % count) for i in range(ends)]),
                cells,
                lax.ppermute(head, axis, [((i + 1) % count, i) for i in range(ends)]),
            ],
            axis=dim,
        )
    return cells


def toeplitz(kernel, tile_size):
    taps = kernel.shape[0]
    padded = jnp.concatenate([kernel, jnp.zeros((2 * tile_size + 1 - taps,), kernel.dtype)])
    tiled = jnp.tile(padded, tile_size)[: 2 * tile_size * tile_size]
    return tiled.reshape(tile_size, 2 * tile_size).T


def phase_filter(projections, phase_kernel, tile_size):
    half_width = (phase_kernel.shape[0] - 1) // 2
    angles, slices, columns = projections.shape
    block_count = columns // tile_size
    rimmed = with_halo(projections, (("ray", 2),), half_width)
    padded = jnp.pad(rimmed, ((0, 0), (0, 0), (0, 2 * tile_size - 2 * half_width)))
    blocks = padded.reshape(angles, slices, block_count + 2, tile_size)
    windows = jnp.concatenate(
        [blocks[:, :, :block_count], blocks[:, :, 1 : block_count + 1]], axis=-1
    )
    filtered = jnp.einsum(
        "asbi,ij->asbj",
        windows,
        toeplitz(phase_kernel, tile_size),
        preferred_element_type=jnp.float32,
    )
    return filtered.reshape(angles, slices, columns).astype(jnp.bfloat16)


def stripe_profile(gathered):
    profile = jnp.median(gathered.astype(jnp.float32), axis=0)
    columns = profile.shape[1]
    rimmed = with_halo(profile, (("ray", 1),), SMOOTH)
    window_sum = jnp.zeros_like(profile)
    for offset in range(2 * SMOOTH + 1):
        window_sum = window_sum + rimmed[:, offset : offset + columns]
    position = lax.axis_index("ray") * columns + jnp.arange(columns)
    detector = lax.axis_size("ray") * columns
    in_range = (
        jnp.minimum(position + SMOOTH, detector - 1) - jnp.maximum(position - SMOOTH, 0) + 1
    ).astype(jnp.float32)
    return (profile - window_sum / in_range).astype(jnp.bfloat16)


def shards(
    projections,
    phase_kernel,
    image,
    tile_library,
    tile_entry,
    tile_image,
    tile_slot,
    tile_count,
    slot_block,
):
    tile_size = tile_library.shape[-1]
    angles, slices, columns = projections.shape
    phase = phase_filter(projections, phase_kernel, tile_size)
    gathered = lax.all_to_all(phase, "dom", split_axis=1, concat_axis=0, tiled=True)
    stripe = stripe_profile(gathered)
    fixed_rows = (gathered.astype(jnp.float32) - stripe.astype(jnp.float32)[None]).astype(
        jnp.bfloat16
    )
    corrected = lax.all_to_all(fixed_rows, "dom", split_axis=0, concat_axis=1, tiled=True)
    owners = lax.axis_size("dom")
    library = tile_library[0, 0]
    entries = tile_entry[0, 0]
    images = tile_image[0, 0]
    slots = tile_slot[0, 0]
    capacity = entries.shape[0]
    block_size = 64
    turn_count = capacity // block_size
    image_blocks = image.reshape(-1, tile_size, slices)
    block_total = image_blocks.shape[0]
    live_mask = jnp.arange(capacity) < tile_count[0, 0]
    slot_target = jnp.where(live_mask, slots, owners)
    image_target = jnp.where(live_mask, images, block_total)

    def forward_turn(turn_index, partial_value):
        first_tile = turn_index * block_size
        chosen = lax.dynamic_slice_in_dim(entries, first_tile, block_size)
        placed = lax.dynamic_slice_in_dim(images, first_tile, block_size)
        destined = lax.dynamic_slice_in_dim(slot_target, first_tile, block_size)
        product = jnp.einsum(
            "krp,kps->ksr",
            library[chosen],
            image_blocks[placed],
            preferred_element_type=jnp.float32,
        )
        return partial_value.at[destined].add(product, mode="drop")

    partial_value = lax.fori_loop(
        0, turn_count, forward_turn, jnp.zeros((owners, slices, tile_size), jnp.float32)
    )
    received = lax.all_to_all(
        partial_value.astype(jnp.bfloat16), "dom", split_axis=0, concat_axis=0, tiled=True
    )
    per_owner = columns // tile_size
    carried = slot_block[0, 0]
    block_ids = jnp.arange(angles * per_owner).reshape(angles, per_owner)
    selector = (block_ids[:, :, None] == carried[None, None, :]).astype(jnp.bfloat16)
    forward = jnp.einsum("abd,dst->asbt", selector, received, preferred_element_type=jnp.float32)
    residual = (corrected.astype(jnp.float32) - forward.reshape(angles, slices, columns)).astype(
        jnp.bfloat16
    )
    back = jnp.einsum(
        "abd,asbt->dst",
        selector,
        residual.reshape(angles, slices, per_owner, tile_size),
        preferred_element_type=jnp.float32,
    ).astype(jnp.bfloat16)
    returned = lax.all_to_all(back, "dom", split_axis=0, concat_axis=0, tiled=True)

    def adjoint_turn(turn_index, gradient):
        first_tile = turn_index * block_size
        chosen = lax.dynamic_slice_in_dim(entries, first_tile, block_size)
        sourced = lax.dynamic_slice_in_dim(slots, first_tile, block_size)
        destined = lax.dynamic_slice_in_dim(image_target, first_tile, block_size)
        product = jnp.einsum(
            "krp,ksr->kps", library[chosen], returned[sourced], preferred_element_type=jnp.float32
        )
        return gradient.at[destined].add(product, mode="drop")

    gradient = lax.fori_loop(
        0, turn_count, adjoint_turn, jnp.zeros((block_total, tile_size, slices), jnp.float32)
    )
    gradient = gradient.reshape(-1, slices)
    rows_own = gradient.shape[0] // lax.axis_size("ray")
    update = lax.psum_scatter(gradient, "ray", scatter_dimension=0, tiled=True)
    own_image = lax.dynamic_slice_in_dim(image, lax.axis_index("ray") * rows_own, rows_own)
    image_next = own_image.astype(jnp.float32) + relax_factor * update
    return (residual, image_next)


MESH = pl.DeviceIdType.MESH
NT = (((1,), (1,)), ((), ()))
NN = (((1,), (0,)), ((), ()))
SUB = 16


def dot(a, b, dims):
    return lax.dot_general(a, b, dims, preferred_element_type=jnp.float32)


def ordered(a, b):
    return jnp.minimum(a, b), jnp.maximum(a, b)


def sorted_four(a, b, c, d):
    a, b = ordered(a, b)
    c, d = ordered(c, d)
    a, c = ordered(a, c)
    b, d = ordered(b, d)
    b, c = ordered(b, c)
    return a, b, c, d


def median_of_eight(values):
    low = sorted_four(*values[:4])
    high = sorted_four(*values[4:])
    below = [jnp.minimum(low[i], high[3 - i]) for i in range(4)]
    above = [jnp.maximum(low[i], high[3 - i]) for i in range(4)]
    fourth = jnp.maximum(jnp.maximum(below[0], below[1]), jnp.maximum(below[2], below[3]))
    fifth = jnp.minimum(jnp.minimum(above[0], above[1]), jnp.minimum(above[2], above[3]))
    return (fourth + fifth) * 0.5


def step_kernel(
    owners,
    quarters,
    taps_any,
    proj_any,
    image_any,
    library_any,
    entry_any,
    place_any,
    slot_any,
    count_any,
    carried_any,
    residual_ref,
    next_ref,
    taps_ref,
    proj_ref,
    image_ref,
    library_ref,
    entry_ref,
    place_ref,
    slot_ref,
    count_ref,
    carried_own,
    carried_all,
    carried_ref,
    taps_wide,
    rim,
    phase_out,
    phase_in,
    profile_ref,
    fixed,
    counted,
    spread_ref,
    matrix,
    partial_out,
    partial_in,
    same_ref,
    back_out,
    back_in,
    rest_out,
    rest_in,
    own_update,
    update_out,
    update_in,
    load_sem,
    halo_send,
    halo_recv,
    carried_send,
    carried_recv,
    phase_send,
    phase_recv,
    edge_send,
    edge_recv,
    partial_send,
    partial_recv,
    back_send,
    back_recv,
    rest_send,
    rest_recv,
    update_send,
    update_recv,
):
    f32, bf16 = jnp.float32, jnp.bfloat16
    me, ray = lax.axis_index("dom"), lax.axis_index("ray")
    slices, columns = proj_ref.shape
    entries, tile = library_ref.shape[0], library_ref.shape[-1]
    places = image_ref.shape[1] // tile
    count = columns // tile
    ring = count + 1
    inner = count - 2
    per = slices // owners
    side = owners // 2
    half = tile // 2
    share = places * tile // quarters
    rows_half = side * per

    group, spot = me // side, lax.rem(me, side)

    def dom_peer(k):
        if k >= side:
            return (1 - group) * side + lax.rem(spot + k - side, side)
        return group * side + lax.rem(spot + k, side)

    dom_order = list(range(side, owners)) + list(range(1, side))

    chip, core = ray // 2, lax.rem(ray, 2)

    def ray_twin(k):
        chip_to = 1 - chip if k >= 2 else chip
        core_to = 1 - core if k % 2 else core
        return chip_to * 2 + core_to

    def ray_next(k):
        return lax.rem(ray + k, quarters)

    barrier = pltpu.get_barrier_semaphore()
    for k in range(1, owners):
        pl.semaphore_signal(barrier, inc=1, device_id=(dom_peer(k), ray), device_id_type=MESH)
    for k in range(1, quarters):
        pl.semaphore_signal(barrier, inc=1, device_id=(me, ray_next(k)), device_id_type=MESH)

    pairs = [
        (proj_any.at[0], proj_ref),
        (taps_any, taps_ref),
        (entry_any, entry_ref),
        (place_any, place_ref),
        (slot_any, slot_ref),
        (count_any, count_ref),
        (carried_any, carried_own),
        (library_any.at[0, 0], library_ref),
        (image_any, image_ref),
    ]
    loads = [
        pltpu.make_async_copy(src, dst, load_sem.at[i]) for i, (src, dst) in enumerate(pairs)
    ]
    for copy in loads:
        copy.start()

    def dom_copy(src, dst, send, recv, k):
        return pltpu.make_async_remote_copy(
            src_ref=src,
            dst_ref=dst,
            send_sem=send.at[k],
            recv_sem=recv.at[k],
            device_id=(dom_peer(k), ray),
            device_id_type=MESH,
        )

    def ray_copy(src, dst, send, recv, slot, peer):
        return pltpu.make_async_remote_copy(
            src_ref=src,
            dst_ref=dst,
            send_sem=send.at[slot],
            recv_sem=recv.at[slot],
            device_id=(me, peer),
            device_id_type=MESH,
        )

    def block(b):
        return proj_ref[:, b * tile : (b + 1) * tile]

    loads[1].wait()
    taps_wide[...] = jnp.zeros(taps_wide.shape, f32)
    taps_wide[:, : taps_ref.shape[0]] = taps_ref[...].astype(f32)[None]
    spread = jnp.broadcast_to(taps_wide[...], (tile, taps_wide.shape[1]))
    weights = pltpu.roll(spread, half, 1, stride=1, stride_axis=0).astype(bf16)
    loads[0].wait()
    two = jnp.concatenate(
        [proj_ref[:, (b - 1) * tile : (b + 1) * tile] for b in range(1, count - 1)], axis=0
    )
    third = jnp.concatenate([block(b + 1) for b in range(1, count - 1)], axis=0)
    phase = dot(two, weights[:, : 2 * tile], NT) + dot(third, weights[:, 2 * tile :], NT)
    phase = phase.reshape(inner, owners, per, tile)
    for owner in range(owners):
        phase_out[owner, :inner] = phase[:, owner].astype(bf16)

    loads[6].wait()
    pl.semaphore_wait(barrier, owners + quarters - 2)

    halos = [
        ray_copy(
            proj_ref.at[:, pl.ds(columns - tile, tile)],
            rim.at[0],
            halo_send,
            halo_recv,
            0,
            ray_next(1),
        ),
        ray_copy(
            proj_ref.at[:, pl.ds(0, tile)], rim.at[1], halo_send, halo_recv, 1, ray_next(quarters - 1)
        ),
    ]
    for copy in halos:
        copy.start()
    phases = [
        dom_copy(
            phase_out.at[dom_peer(k), pl.ds(0, inner)],
            phase_in.at[me, pl.ds(0, inner)],
            phase_send,
            phase_recv,
            k,
        )
        for k in dom_order
    ]
    for copy in phases:
        copy.start()
    carries = [
        dom_copy(carried_own, carried_all.at[me], carried_send, carried_recv, k) for k in dom_order
    ]
    for copy in carries:
        copy.start()

    for i in range(2, 6):
        loads[i].wait()
    capacity = entry_ref.shape[1]
    alive = lax.broadcasted_iota(jnp.int32, (1, capacity), 1) < count_ref[0, 0]
    code = jnp.where(alive, slot_ref[...] * places + place_ref[...], -1)
    pick = jnp.where(
        lax.broadcasted_iota(jnp.int32, (owners * places, capacity), 0) == code, 1.0, 0.0
    ).astype(bf16)
    which = jnp.where(
        lax.broadcasted_iota(jnp.int32, (entries * SUB, capacity), 0) // SUB == entry_ref[...],
        1.0,
        0.0,
    ).astype(bf16)
    counted[...] = dot(pick, which, NT)
    diagonal = lax.rem(
        lax.broadcasted_iota(jnp.int32, (SUB, entries * SUB), 1), SUB
    ) == lax.broadcasted_iota(jnp.int32, (SUB, entries * SUB), 0)

    def widen(step, carry):
        for i in range(8):
            at = step * 8 + i
            row = jnp.broadcast_to(counted[pl.ds(at, 1), :], (SUB, entries * SUB))
            start = pl.multiple_of(at * SUB, SUB)
            spread_ref[pl.ds(start, SUB), :] = jnp.where(diagonal, row, 0.0).astype(bf16)
        return carry

    lax.fori_loop(0, owners * places // 8, widen, 0)

    loads[7].wait()

    def build(step, carry):
        first = pl.multiple_of(step * 2 * SUB, 2 * SUB)
        right = jnp.concatenate(
            [
                library_ref[:, pl.ds(first + i * SUB, SUB), :].reshape(entries * SUB, tile)
                for i in range(2)
            ],
            axis=1,
        )
        for owner in range(owners):
            rows = places * SUB
            made = dot(spread_ref[owner * rows : (owner + 1) * rows, :], right, NN)
            for place in range(places):
                for i in range(2):
                    start = pl.multiple_of(first + owner * tile + i * SUB, SUB)
                    matrix[pl.ds(start, SUB), place * tile : (place + 1) * tile] = made[
                        place * SUB : (place + 1) * SUB, i * tile : (i + 1) * tile
                    ].astype(bf16)
        return carry

    lax.fori_loop(0, tile // (2 * SUB), build, 0)

    for copy in halos:
        copy.wait()

    @pl.when(ray == 0)
    def _():
        rim[0] = jnp.zeros((slices, tile), bf16)

    @pl.when(ray == quarters - 1)
    def _():
        rim[1] = jnp.zeros((slices, tile), bf16)

    before, after = rim[0], rim[1]
    two = jnp.concatenate(
        [
            proj_ref[:, (count - 2) * tile : count * tile],
            jnp.concatenate([block(count - 1), after], axis=1),
            jnp.concatenate([before, block(0)], axis=1),
            jnp.concatenate([before, before], axis=1),
        ],
        axis=0,
    )
    third = jnp.concatenate([after, after, block(1), block(0)], axis=0)
    edge = dot(two, weights[:, : 2 * tile], NT) + dot(third, weights[:, 2 * tile :], NT)
    edge = edge.reshape(4, owners, per, tile)
    lane = lax.broadcasted_iota(jnp.int32, (owners, per, tile), 2)
    phase_out[:, inner] = edge[0].astype(bf16)
    phase_out[:, inner + 1] = jnp.where(lane < half, edge[1], edge[3]).astype(bf16)
    phase_out[:, inner + 2] = edge[2].astype(bf16)
    edges = [
        dom_copy(
            phase_out.at[dom_peer(k), pl.ds(inner, 3)],
            phase_in.at[me, pl.ds(inner, 3)],
            edge_send,
            edge_recv,
            k,
        )
        for k in dom_order
    ]
    for copy in edges:
        copy.start()
    phase_in[me] = phase_out[me]

    loads[8].wait()
    for owner in range(0, owners, 2):
        made = dot(image_ref[...], matrix[owner * tile : (owner + 2) * tile, :], NT)
        for i in range(2):
            partial_out[:, owner + i] = (
                made[:, i * tile : (i + 1) * tile].reshape(owners, per, tile).astype(bf16)
            )
    partials = [
        dom_copy(
            partial_out.at[dom_peer(k)], partial_in.at[me], partial_send, partial_recv, k
        )
        for k in dom_order
    ]
    for copy in partials:
        copy.start()
    partial_in[me] = partial_out[me]

    carried_all[me] = carried_own[...]
    for copy in carries:
        copy.wait_recv()
    to_scalar = pltpu.make_async_copy(carried_all, carried_ref, load_sem.at[len(loads)])
    to_scalar.start()
    to_scalar.wait()
    duos = [(a, b) for a in range(owners) for b in range(a + 1, owners)]

    def compare(owner, carry):
        for i, (a, b) in enumerate(duos):
            same = jnp.where(carried_ref[owner, 0, a] == carried_ref[owner, 0, b], 1.0, 0.0)
            same_ref[owner, i : i + 1, :] = jnp.full((1, tile), same, f32)
        return carry

    lax.fori_loop(0, owners, compare, 0)

    def profile_of(i):
        return median_of_eight([phase_in[a, i].astype(f32) for a in range(owners)])

    for copy in phases:
        copy.wait_recv()
    for i in range(inner):
        profile_ref[:, i * tile : (i + 1) * tile] = profile_of(i)
    for copy in edges:
        copy.wait_recv()
    for i in range(inner, ring):
        profile_ref[:, i * tile : (i + 1) * tile] = profile_of(i)

    width = ring * tile
    detector = quarters * columns
    at = lax.broadcasted_iota(jnp.int32, (1, width), 1)
    position = ray * columns + jnp.where(at < count * tile - half, at + tile, at - columns)
    profile = jnp.where((position >= 0) & (position < detector), profile_ref[...], 0.0)
    run = profile
    reach = 1
    while reach < 2 * SMOOTH:
        run = run + pltpu.roll(run, reach, 1)
        reach *= 2
    window = pltpu.roll(run, width - (SMOOTH - 1), 1) + pltpu.roll(profile, width - SMOOTH, 1)
    in_range = (
        jnp.minimum(position + SMOOTH, detector - 1) - jnp.maximum(position - SMOOTH, 0) + 1
    ).astype(f32)
    stripe = (profile - window / in_range).astype(bf16).astype(f32)
    for a in range(owners):
        for i in range(ring):
            if i != count - 1:
                fixed[a, i] = (
                    (phase_in[a, i].astype(f32) - stripe[:, i * tile : (i + 1) * tile])
                    .astype(bf16)
                    .astype(f32)
                )

    for copy in partials:
        copy.wait_recv()

    def ring_spot(b):
        return jnp.where(b == 0, ring - 1, b - 1)

    def carry_back(owner, carry):
        part = [partial_in[d, owner].astype(f32) for d in range(owners)]
        total = list(part)
        for i, (a, b) in enumerate(duos):
            same = jnp.broadcast_to(same_ref[owner, i : i + 1, :], (per, tile))
            total[a] = total[a] + same * part[b]
            total[b] = total[b] + same * part[a]
        for d in range(owners):
            back_out[d, owner] = (
                fixed[owner, ring_spot(carried_ref[owner, 0, d])] - total[d]
            ).astype(bf16)
        return carry

    lax.fori_loop(0, owners, carry_back, 0)
    backs = [
        dom_copy(back_out.at[dom_peer(k)], back_in.at[me], back_send, back_recv, k)
        for k in dom_order
    ]
    for copy in backs:
        copy.start()
    back_in[me] = back_out[me]

    def whole(owner, carry):
        part = [partial_in[d, owner].astype(f32) for d in range(owners)]
        where_to = [carried_ref[owner, 0, d] for d in range(owners)]
        for b in range(count):
            total = fixed[owner, (b - 1) % ring]
            taken = jnp.zeros((per, tile), f32)
            for d in range(owners):
                taken = taken + jnp.where(where_to[d] == b, 1.0, 0.0).astype(f32) * part[d]
            rest_out[owner, b] = (total - taken).astype(bf16)
        return carry

    lax.fori_loop(0, owners, whole, 0)
    rests = [
        dom_copy(rest_out.at[dom_peer(k)], rest_in.at[me], rest_send, rest_recv, k)
        for k in dom_order
    ]
    for copy in rests:
        copy.start()
    rest_in[me] = rest_out[me]

    updates = []
    for turn in range(2):
        held = group if turn == 0 else 1 - group
        for copy in backs[:side] if turn else backs[side:]:
            copy.wait_recv()
        first = held * side
        left = jnp.concatenate(
            [
                back_in[pl.ds(first, side), owner]
                .astype(f32)
                .reshape(rows_half, tile)
                .astype(bf16)
                for owner in range(owners)
            ],
            axis=1,
        )
        for k in (2, 3, 1, 0):
            start = pl.multiple_of(ray_twin(k) * share, share)
            made = dot(left, matrix[:, pl.ds(start, share)], NN)
            if k == 0:
                own_update[turn] = made
            else:
                update_out[turn, k] = made.astype(bf16)
                copy = ray_copy(
                    update_out.at[turn, k],
                    update_in.at[turn, k],
                    update_send,
                    update_recv,
                    turn * quarters + k,
                    ray_twin(k),
                )
                copy.start()
                updates.append(copy)

    for copy in rests:
        copy.wait_recv()
    for b in range(count):
        residual_ref[:, b * tile : (b + 1) * tile] = (
            rest_in[:, b].astype(f32).reshape(slices, tile).astype(bf16)
        )

    for turn in range(2):
        held = group if turn == 0 else 1 - group
        for copy in updates[turn * (quarters - 1) : (turn + 1) * (quarters - 1)]:
            copy.wait_recv()
        amount = own_update[turn]
        for k in range(1, quarters):
            amount = amount + update_in[turn, k].astype(f32)
        rows = pl.ds(pl.multiple_of(held * rows_half, rows_half), rows_half)
        old = image_ref[rows, pl.ds(pl.multiple_of(ray * share, share), share)].astype(f32)
        next_ref[rows, :] = old + relax_factor * amount
    for copy in carries + phases + edges + partials + backs + rests + updates:
        copy.wait_send()


def fast_shards(
    projections,
    phase_kernel,
    image,
    tile_library,
    tile_entry,
    tile_image,
    tile_slot,
    tile_count,
    slot_block,
):
    f32, bf16 = jnp.float32, jnp.bfloat16
    i32 = jnp.int32
    owners, quarters = lax.axis_size("dom"), lax.axis_size("ray")
    entries, tile = tile_library.shape[2], tile_library.shape[-1]
    _, slices, columns = projections.shape
    count = columns // tile
    ring = count + 1
    places = image.shape[0] // tile
    per = slices // owners
    capacity = tile_entry.shape[2]
    share = places * tile // quarters
    rows_half = slices // 2
    hbm = pl.BlockSpec(memory_space=pltpu.HBM)
    vmem = pl.BlockSpec(memory_space=pltpu.VMEM)
    sems = pltpu.SemaphoreType.DMA
    residual, image_next = pl.pallas_call(
        functools.partial(step_kernel, owners, quarters),
        out_shape=(
            jax.ShapeDtypeStruct((slices, columns), bf16),
            jax.ShapeDtypeStruct((slices, share), f32),
        ),
        in_specs=[hbm] * 9,
        out_specs=(vmem, vmem),
        scratch_shapes=[
            pltpu.VMEM(phase_kernel.shape, bf16),
            pltpu.VMEM((slices, columns), bf16),
            pltpu.VMEM((slices, places * tile), bf16),
            pltpu.VMEM((entries, tile, tile), bf16),
            pltpu.VMEM((1, capacity), i32),
            pltpu.VMEM((1, capacity), i32),
            pltpu.VMEM((1, capacity), i32),
            pltpu.SMEM((1, 1), i32),
            pltpu.VMEM((1, owners), i32),
            pltpu.VMEM((owners, 1, owners), i32),
            pltpu.SMEM((owners, 1, owners), i32),
            pltpu.VMEM((1, 3 * tile), f32),
            pltpu.VMEM((2, slices, tile), bf16),
            pltpu.VMEM((owners, ring, per, tile), bf16),
            pltpu.VMEM((owners, ring, per, tile), bf16),
            pltpu.VMEM((per, ring * tile), f32),
            pltpu.VMEM((owners, ring, per, tile), f32),
            pltpu.VMEM((owners * places, entries * SUB), f32),
            pltpu.VMEM((owners * places * SUB, entries * SUB), bf16),
            pltpu.VMEM((owners * tile, places * tile), bf16),
            pltpu.VMEM((owners, owners, per, tile), bf16),
            pltpu.VMEM((owners, owners, per, tile), bf16),
            pltpu.VMEM((owners, 32, tile), f32),
            pltpu.VMEM((owners, owners, per, tile), bf16),
            pltpu.VMEM((owners, owners, per, tile), bf16),
            pltpu.VMEM((owners, count, per, tile), bf16),
            pltpu.VMEM((owners, count, per, tile), bf16),
            pltpu.VMEM((2, rows_half, share), f32),
            pltpu.VMEM((2, quarters, rows_half, share), bf16),
            pltpu.VMEM((2, quarters, rows_half, share), bf16),
            sems((10,)),
            sems((2,)),
            sems((2,)),
        ]
        + [sems((owners,))] * 12
        + [sems((2 * quarters,))] * 2,
        compiler_params=pltpu.CompilerParams(
            collective_id=0, has_side_effects=True, vmem_limit_bytes=63 * 1024 * 1024
        ),
    )(
        phase_kernel,
        projections,
        image.T,
        tile_library,
        tile_entry[0],
        tile_image[0],
        tile_slot[0],
        tile_count,
        slot_block[0],
    )
    return residual[None], image_next.T


def fits_kernel(projections, phase_kernel, image, tile_library, tile_entry, *rest):
    owners, quarters = lax.axis_size("dom"), lax.axis_size("ray")
    tile = tile_library.shape[-1]
    angles, slices, columns = projections.shape
    return (
        angles == 1
        and slices % 16 == 0
        and slices == 8 * owners
        and owners == 8
        and tile == 128
        and phase_kernel.shape[0] == tile + 1
        and columns % tile == 0
        and tile_library.shape[2] == 16
        and quarters == 4
        and image.shape[0] == 16 * tile
        and tile_entry.shape[2] <= 256
    )


def any_shards(*args):
    if fits_kernel(*args):
        return fast_shards(*args)
    return shards(*args)


def solution(mesh):
    return jax.shard_map(
        any_shards,
        mesh=mesh,
        in_specs=(
            P("dom", None, "ray"),
            P(),
            P("dom", None),
            P("dom", "ray", None, None, None),
            P("dom", "ray", None),
            P("dom", "ray", None),
            P("dom", "ray", None),
            P("dom", "ray"),
            P("dom", "ray", None),
        ),
        out_specs=(P("dom", None, "ray"), P(("dom", "ray"), None)),
        check_vma=False,
    )
```

```python
import functools

import jax
import jax.numpy as jnp
from jax import lax
from jax.experimental import pallas as pl
from jax.experimental.pallas import tpu as pltpu
from jax.sharding import PartitionSpec as P

SMOOTH = 8


relax_factor = 0.25


def with_halo(cells, sides, width):
    for axis, dim in sides:
        count = lax.axis_size(axis)
        ends = count - 1
        head = lax.slice_in_dim(cells, 0, width, axis=dim)
        tail = lax.slice_in_dim(cells, cells.shape[dim] - width, cells.shape[dim], axis=dim)
        cells = jnp.concatenate(
            [
                lax.ppermute(tail, axis, [(i, (i + 1) % count) for i in range(ends)]),
                cells,
                lax.ppermute(head, axis, [((i + 1) % count, i) for i in range(ends)]),
            ],
            axis=dim,
        )
    return cells


def toeplitz(kernel, tile_size):
    taps = kernel.shape[0]
    padded = jnp.concatenate([kernel, jnp.zeros((2 * tile_size + 1 - taps,), kernel.dtype)])
    tiled = jnp.tile(padded, tile_size)[: 2 * tile_size * tile_size]
    return tiled.reshape(tile_size, 2 * tile_size).T


def phase_filter(projections, phase_kernel, tile_size):
    half_width = (phase_kernel.shape[0] - 1) // 2
    angles, slices, columns = projections.shape
    block_count = columns // tile_size
    rimmed = with_halo(projections, (("ray", 2),), half_width)
    padded = jnp.pad(rimmed, ((0, 0), (0, 0), (0, 2 * tile_size - 2 * half_width)))
    blocks = padded.reshape(angles, slices, block_count + 2, tile_size)
    windows = jnp.concatenate(
        [blocks[:, :, :block_count], blocks[:, :, 1 : block_count + 1]], axis=-1
    )
    filtered = jnp.einsum(
        "asbi,ij->asbj",
        windows,
        toeplitz(phase_kernel, tile_size),
        preferred_element_type=jnp.float32,
    )
    return filtered.reshape(angles, slices, columns).astype(jnp.bfloat16)


def stripe_profile(gathered):
    profile = jnp.median(gathered.astype(jnp.float32), axis=0)
    columns = profile.shape[1]
    rimmed = with_halo(profile, (("ray", 1),), SMOOTH)
    window_sum = jnp.zeros_like(profile)
    for offset in range(2 * SMOOTH + 1):
        window_sum = window_sum + rimmed[:, offset : offset + columns]
    position = lax.axis_index("ray") * columns + jnp.arange(columns)
    detector = lax.axis_size("ray") * columns
    in_range = (
        jnp.minimum(position + SMOOTH, detector - 1) - jnp.maximum(position - SMOOTH, 0) + 1
    ).astype(jnp.float32)
    return (profile - window_sum / in_range).astype(jnp.bfloat16)


def shards(
    projections,
    phase_kernel,
    image,
    tile_library,
    tile_entry,
    tile_image,
    tile_slot,
    tile_count,
    slot_block,
):
    tile_size = tile_library.shape[-1]
    angles, slices, columns = projections.shape
    phase = phase_filter(projections, phase_kernel, tile_size)
    gathered = lax.all_to_all(phase, "dom", split_axis=1, concat_axis=0, tiled=True)
    stripe = stripe_profile(gathered)
    fixed_rows = (gathered.astype(jnp.float32) - stripe.astype(jnp.float32)[None]).astype(
        jnp.bfloat16
    )
    corrected = lax.all_to_all(fixed_rows, "dom", split_axis=0, concat_axis=1, tiled=True)
    owners = lax.axis_size("dom")
    library = tile_library[0, 0]
    entries = tile_entry[0, 0]
    images = tile_image[0, 0]
    slots = tile_slot[0, 0]
    capacity = entries.shape[0]
    block_size = 64
    turn_count = capacity // block_size
    image_blocks = image.reshape(-1, tile_size, slices)
    block_total = image_blocks.shape[0]
    live_mask = jnp.arange(capacity) < tile_count[0, 0]
    slot_target = jnp.where(live_mask, slots, owners)
    image_target = jnp.where(live_mask, images, block_total)

    def forward_turn(turn_index, partial_value):
        first_tile = turn_index * block_size
        chosen = lax.dynamic_slice_in_dim(entries, first_tile, block_size)
        placed = lax.dynamic_slice_in_dim(images, first_tile, block_size)
        destined = lax.dynamic_slice_in_dim(slot_target, first_tile, block_size)
        product = jnp.einsum(
            "krp,kps->ksr",
            library[chosen],
            image_blocks[placed],
            preferred_element_type=jnp.float32,
        )
        return partial_value.at[destined].add(product, mode="drop")

    partial_value = lax.fori_loop(
        0, turn_count, forward_turn, jnp.zeros((owners, slices, tile_size), jnp.float32)
    )
    received = lax.all_to_all(
        partial_value.astype(jnp.bfloat16), "dom", split_axis=0, concat_axis=0, tiled=True
    )
    per_owner = columns // tile_size
    carried = slot_block[0, 0]
    block_ids = jnp.arange(angles * per_owner).reshape(angles, per_owner)
    selector = (block_ids[:, :, None] == carried[None, None, :]).astype(jnp.bfloat16)
    forward = jnp.einsum("abd,dst->asbt", selector, received, preferred_element_type=jnp.float32)
    residual = (corrected.astype(jnp.float32) - forward.reshape(angles, slices, columns)).astype(
        jnp.bfloat16
    )
    back = jnp.einsum(
        "abd,asbt->dst",
        selector,
        residual.reshape(angles, slices, per_owner, tile_size),
        preferred_element_type=jnp.float32,
    ).astype(jnp.bfloat16)
    returned = lax.all_to_all(back, "dom", split_axis=0, concat_axis=0, tiled=True)

    def adjoint_turn(turn_index, gradient):
        first_tile = turn_index * block_size
        chosen = lax.dynamic_slice_in_dim(entries, first_tile, block_size)
        sourced = lax.dynamic_slice_in_dim(slots, first_tile, block_size)
        destined = lax.dynamic_slice_in_dim(image_target, first_tile, block_size)
        product = jnp.einsum(
            "krp,ksr->kps", library[chosen], returned[sourced], preferred_element_type=jnp.float32
        )
        return gradient.at[destined].add(product, mode="drop")

    gradient = lax.fori_loop(
        0, turn_count, adjoint_turn, jnp.zeros((block_total, tile_size, slices), jnp.float32)
    )
    gradient = gradient.reshape(-1, slices)
    rows_own = gradient.shape[0] // lax.axis_size("ray")
    update = lax.psum_scatter(gradient, "ray", scatter_dimension=0, tiled=True)
    own_image = lax.dynamic_slice_in_dim(image, lax.axis_index("ray") * rows_own, rows_own)
    image_next = own_image.astype(jnp.float32) + relax_factor * update
    return (residual, image_next)


MESH = pl.DeviceIdType.MESH
NT = (((1,), (1,)), ((), ()))
NN = (((1,), (0,)), ((), ()))
SUB = 16


def dot(a, b, dims):
    return lax.dot_general(a, b, dims, preferred_element_type=jnp.float32)


def ordered(a, b):
    return jnp.minimum(a, b), jnp.maximum(a, b)


def sorted_four(a, b, c, d):
    a, b = ordered(a, b)
    c, d = ordered(c, d)
    a, c = ordered(a, c)
    b, d = ordered(b, d)
    b, c = ordered(b, c)
    return a, b, c, d


def median_of_eight(values):
    low = sorted_four(*values[:4])
    high = sorted_four(*values[4:])
    below = [jnp.minimum(low[i], high[3 - i]) for i in range(4)]
    above = [jnp.maximum(low[i], high[3 - i]) for i in range(4)]
    fourth = jnp.maximum(jnp.maximum(below[0], below[1]), jnp.maximum(below[2], below[3]))
    fifth = jnp.minimum(jnp.minimum(above[0], above[1]), jnp.minimum(above[2], above[3]))
    return (fourth + fifth) * 0.5


def step_kernel(
    owners,
    quarters,
    taps_any,
    proj_any,
    image_any,
    library_any,
    entry_any,
    place_any,
    slot_any,
    carried_any,
    count_ref,
    residual_ref,
    next_ref,
    taps_ref,
    proj_ref,
    image_ref,
    library_ref,
    entry_ref,
    place_ref,
    slot_ref,
    carried_own,
    carried_all,
    carried_ref,
    taps_wide,
    rim,
    phase_out,
    phase_in,
    profile_ref,
    fixed,
    counted,
    spread_ref,
    matrix,
    partial_out,
    partial_in,
    same_ref,
    back_out,
    back_in,
    rest_out,
    rest_in,
    own_update,
    update_out,
    update_in,
    load_sem,
    halo_send,
    halo_recv,
    carried_send,
    carried_recv,
    phase_send,
    phase_recv,
    edge_send,
    edge_recv,
    partial_send,
    partial_recv,
    back_send,
    back_recv,
    rest_send,
    rest_recv,
    update_send,
    update_recv,
):
    f32, bf16 = jnp.float32, jnp.bfloat16
    me, ray = lax.axis_index("dom"), lax.axis_index("ray")
    slices, columns = proj_ref.shape
    entries, tile = library_ref.shape[0], library_ref.shape[-1]
    places = image_ref.shape[1] // tile
    count = columns // tile
    ring = count + 1
    inner = count - 2
    per = slices // owners
    side = owners // 2
    half = tile // 2
    share = places * tile // quarters
    rows_half = side * per

    group, spot = me // side, lax.rem(me, side)

    def dom_peer(k):
        if k >= side:
            return (1 - group) * side + lax.rem(spot + k - side, side)
        return group * side + lax.rem(spot + k, side)

    dom_order = list(range(1, owners))

    chip, core = ray // 2, lax.rem(ray, 2)

    def ray_twin(k):
        chip_to = 1 - chip if k >= 2 else chip
        core_to = 1 - core if k % 2 else core
        return chip_to * 2 + core_to

    def ray_next(k):
        return lax.rem(ray + k, quarters)

    barrier = pltpu.get_barrier_semaphore()
    for k in range(1, owners):
        pl.semaphore_signal(barrier, inc=1, device_id=(dom_peer(k), ray), device_id_type=MESH)
    for k in range(1, quarters):
        pl.semaphore_signal(barrier, inc=1, device_id=(me, ray_next(k)), device_id_type=MESH)

    pairs = [
        (proj_any.at[0], proj_ref),
        (taps_any, taps_ref),
        (entry_any, entry_ref),
        (place_any, place_ref),
        (slot_any, slot_ref),
        (carried_any, carried_own),
        (library_any.at[0, 0], library_ref),
        (image_any, image_ref),
    ]
    loads = [
        pltpu.make_async_copy(src, dst, load_sem.at[i]) for i, (src, dst) in enumerate(pairs)
    ]
    for copy in loads:
        copy.start()

    def dom_copy(src, dst, send, recv, k):
        return pltpu.make_async_remote_copy(
            src_ref=src,
            dst_ref=dst,
            send_sem=send.at[k],
            recv_sem=recv.at[k],
            device_id=(dom_peer(k), ray),
            device_id_type=MESH,
        )

    def ray_copy(src, dst, send, recv, slot, peer):
        return pltpu.make_async_remote_copy(
            src_ref=src,
            dst_ref=dst,
            send_sem=send.at[slot],
            recv_sem=recv.at[slot],
            device_id=(me, peer),
            device_id_type=MESH,
        )

    def block(b):
        return proj_ref[:, b * tile : (b + 1) * tile]

    loads[1].wait()
    taps_wide[...] = jnp.zeros(taps_wide.shape, f32)
    taps_wide[:, : taps_ref.shape[0]] = taps_ref[...].astype(f32)[None]
    spread = jnp.broadcast_to(taps_wide[...], (tile, taps_wide.shape[1]))
    weights = pltpu.roll(spread, half, 1, stride=1, stride_axis=0).astype(bf16)
    loads[0].wait()
    two = jnp.concatenate(
        [proj_ref[:, (b - 1) * tile : (b + 1) * tile] for b in range(1, count - 1)], axis=0
    )
    third = jnp.concatenate([block(b + 1) for b in range(1, count - 1)], axis=0)
    phase = dot(two, weights[:, : 2 * tile], NT) + dot(third, weights[:, 2 * tile :], NT)
    phase = phase.reshape(inner, owners, per, tile)
    for owner in range(owners):
        phase_out[owner, :inner] = phase[:, owner].astype(bf16)

    loads[5].wait()
    pl.semaphore_wait(barrier, owners + quarters - 2)

    carries = [
        dom_copy(carried_own, carried_all.at[me], carried_send, carried_recv, k) for k in dom_order
    ]
    for copy in carries:
        copy.start()

    halos = [
        ray_copy(
            proj_ref.at[:, pl.ds(columns - tile, tile)],
            rim.at[0],
            halo_send,
            halo_recv,
            0,
            ray_next(1),
        ),
        ray_copy(
            proj_ref.at[:, pl.ds(0, tile)], rim.at[1], halo_send, halo_recv, 1, ray_next(quarters - 1)
        ),
    ]
    for copy in halos:
        copy.start()
    phases = [
        dom_copy(
            phase_out.at[dom_peer(k), pl.ds(0, inner)],
            phase_in.at[me, pl.ds(0, inner)],
            phase_send,
            phase_recv,
            k,
        )
        for k in dom_order
    ]
    for copy in phases:
        copy.start()
    for i in range(2, 5):
        loads[i].wait()
    capacity = entry_ref.shape[1]
    alive = lax.broadcasted_iota(jnp.int32, (1, capacity), 1) < count_ref[0, 0]
    code = jnp.where(alive, slot_ref[...] * places + place_ref[...], -1)
    pick = jnp.where(
        lax.broadcasted_iota(jnp.int32, (owners * places, capacity), 0) == code, 1.0, 0.0
    ).astype(bf16)
    which = jnp.where(
        lax.broadcasted_iota(jnp.int32, (entries * SUB, capacity), 0) // SUB == entry_ref[...],
        1.0,
        0.0,
    ).astype(bf16)
    counted[...] = dot(pick, which, NT)
    diagonal = lax.rem(
        lax.broadcasted_iota(jnp.int32, (SUB, entries * SUB), 1), SUB
    ) == lax.broadcasted_iota(jnp.int32, (SUB, entries * SUB), 0)

    def widen(step, carry):
        for i in range(8):
            at = step * 8 + i
            row = jnp.broadcast_to(counted[pl.ds(at, 1), :], (SUB, entries * SUB))
            start = pl.multiple_of(at * SUB, SUB)
            spread_ref[pl.ds(start, SUB), :] = jnp.where(diagonal, row, 0.0).astype(bf16)
        return carry

    lax.fori_loop(0, owners * places // 8, widen, 0)

    loads[6].wait()

    def build(step, carry):
        first = pl.multiple_of(step * 2 * SUB, 2 * SUB)
        right = jnp.concatenate(
            [
                library_ref[:, pl.ds(first + i * SUB, SUB), :].reshape(entries * SUB, tile)
                for i in range(2)
            ],
            axis=1,
        )
        for owner in range(owners):
            rows = places * SUB
            made = dot(spread_ref[owner * rows : (owner + 1) * rows, :], right, NN)
            for place in range(places):
                for i in range(2):
                    start = pl.multiple_of(first + owner * tile + i * SUB, SUB)
                    matrix[pl.ds(start, SUB), place * tile : (place + 1) * tile] = made[
                        place * SUB : (place + 1) * SUB, i * tile : (i + 1) * tile
                    ].astype(bf16)
        return carry

    lax.fori_loop(0, tile // (2 * SUB), build, 0)

    for copy in halos:
        copy.wait()

    @pl.when(ray == 0)
    def _():
        rim[0] = jnp.zeros((slices, tile), bf16)

    @pl.when(ray == quarters - 1)
    def _():
        rim[1] = jnp.zeros((slices, tile), bf16)

    before, after = rim[0], rim[1]
    two = jnp.concatenate(
        [
            proj_ref[:, (count - 2) * tile : count * tile],
            jnp.concatenate([block(count - 1), after], axis=1),
            jnp.concatenate([before, block(0)], axis=1),
            jnp.concatenate([before, before], axis=1),
        ],
        axis=0,
    )
    third = jnp.concatenate([after, after, block(1), block(0)], axis=0)
    edge = dot(two, weights[:, : 2 * tile], NT) + dot(third, weights[:, 2 * tile :], NT)
    edge = edge.reshape(4, owners, per, tile)
    lane = lax.broadcasted_iota(jnp.int32, (owners, per, tile), 2)
    phase_out[:, inner] = edge[0].astype(bf16)
    phase_out[:, inner + 1] = jnp.where(lane < half, edge[1], edge[3]).astype(bf16)
    phase_out[:, inner + 2] = edge[2].astype(bf16)
    edges = [
        dom_copy(
            phase_out.at[dom_peer(k), pl.ds(inner, 3)],
            phase_in.at[me, pl.ds(inner, 3)],
            edge_send,
            edge_recv,
            k,
        )
        for k in dom_order
    ]
    for copy in edges:
        copy.start()
    phase_in[me] = phase_out[me]

    loads[7].wait()
    for owner in range(0, owners, 2):
        made = dot(image_ref[...], matrix[owner * tile : (owner + 2) * tile, :], NT)
        for i in range(2):
            partial_out[:, owner + i] = (
                made[:, i * tile : (i + 1) * tile].reshape(owners, per, tile).astype(bf16)
            )
    partials = [
        dom_copy(
            partial_out.at[dom_peer(k)], partial_in.at[me], partial_send, partial_recv, k
        )
        for k in dom_order
    ]
    for copy in partials:
        copy.start()
    partial_in[me] = partial_out[me]

    carried_all[me] = carried_own[...]
    for copy in carries:
        copy.wait_recv()
    to_scalar = pltpu.make_async_copy(carried_all, carried_ref, load_sem.at[len(loads)])
    to_scalar.start()
    to_scalar.wait()
    duos = [(a, b) for a in range(owners) for b in range(a + 1, owners)]

    def compare(owner, carry):
        for i, (a, b) in enumerate(duos):
            same = jnp.where(carried_ref[owner, 0, a] == carried_ref[owner, 0, b], 1.0, 0.0)
            same_ref[owner, i : i + 1, :] = jnp.full((1, tile), same, f32)
        return carry

    lax.fori_loop(0, owners, compare, 0)

    def profile_of(i):
        return median_of_eight([phase_in[a, i].astype(f32) for a in range(owners)])

    for copy in phases:
        copy.wait_recv()
    for i in range(inner):
        profile_ref[:, i * tile : (i + 1) * tile] = profile_of(i)
    for copy in edges:
        copy.wait_recv()
    for i in range(inner, ring):
        profile_ref[:, i * tile : (i + 1) * tile] = profile_of(i)

    width = ring * tile
    detector = quarters * columns
    at = lax.broadcasted_iota(jnp.int32, (1, width), 1)
    position = ray * columns + jnp.where(at < count * tile - half, at + tile, at - columns)
    profile = jnp.where((position >= 0) & (position < detector), profile_ref[...], 0.0)
    run = profile
    reach = 1
    while reach < 2 * SMOOTH:
        run = run + pltpu.roll(run, reach, 1)
        reach *= 2
    window = pltpu.roll(run, width - (SMOOTH - 1), 1) + pltpu.roll(profile, width - SMOOTH, 1)
    in_range = (
        jnp.minimum(position + SMOOTH, detector - 1) - jnp.maximum(position - SMOOTH, 0) + 1
    ).astype(f32)
    stripe = (profile - window / in_range).astype(bf16).astype(f32)
    for a in range(owners):
        for i in range(ring):
            if i != count - 1:
                fixed[a, i] = (
                    (phase_in[a, i].astype(f32) - stripe[:, i * tile : (i + 1) * tile])
                    .astype(bf16)
                    .astype(f32)
                )

    for copy in partials:
        copy.wait_recv()

    def ring_spot(b):
        return jnp.where(b == 0, ring - 1, b - 1)

    def carry_back(owner, carry):
        part = [partial_in[d, owner].astype(f32) for d in range(owners)]
        total = list(part)
        for i, (a, b) in enumerate(duos):
            same = jnp.broadcast_to(same_ref[owner, i : i + 1, :], (per, tile))
            total[a] = total[a] + same * part[b]
            total[b] = total[b] + same * part[a]
        for d in range(owners):
            back_out[d, owner] = (
                fixed[owner, ring_spot(carried_ref[owner, 0, d])] - total[d]
            ).astype(bf16)
        return carry

    lax.fori_loop(0, owners, carry_back, 0)
    backs = [
        dom_copy(back_out.at[dom_peer(k)], back_in.at[me], back_send, back_recv, k)
        for k in dom_order
    ]
    for copy in backs:
        copy.start()
    back_in[me] = back_out[me]

    def whole(owner, carry):
        part = [partial_in[d, owner].astype(f32) for d in range(owners)]
        where_to = [carried_ref[owner, 0, d] for d in range(owners)]
        for b in range(count):
            total = fixed[owner, (b - 1) % ring]
            taken = jnp.zeros((per, tile), f32)
            for d in range(owners):
                taken = taken + jnp.where(where_to[d] == b, 1.0, 0.0).astype(f32) * part[d]
            rest_out[owner, b] = (total - taken).astype(bf16)
        return carry

    lax.fori_loop(0, owners, whole, 0)
    rests = [
        dom_copy(rest_out.at[dom_peer(k)], rest_in.at[me], rest_send, rest_recv, k)
        for k in dom_order
    ]
    for copy in rests:
        copy.start()
    rest_in[me] = rest_out[me]

    updates = []
    for turn in range(2):
        held = group if turn == 0 else 1 - group
        for copy in backs[side - 1 :] if turn else backs[: side - 1]:
            copy.wait_recv()
        first = held * side
        left = jnp.concatenate(
            [
                back_in[pl.ds(first, side), owner]
                .astype(f32)
                .reshape(rows_half, tile)
                .astype(bf16)
                for owner in range(owners)
            ],
            axis=1,
        )
        for k in (2, 3, 1, 0):
            start = pl.multiple_of(ray_twin(k) * share, share)
            made = dot(left, matrix[:, pl.ds(start, share)], NN)
            if k == 0:
                own_update[turn] = made
            else:
                update_out[turn, k] = made.astype(bf16)
                copy = ray_copy(
                    update_out.at[turn, k],
                    update_in.at[turn, k],
                    update_send,
                    update_recv,
                    turn * quarters + k,
                    ray_twin(k),
                )
                copy.start()
                updates.append(copy)

    for copy in rests:
        copy.wait_recv()
    for b in range(count):
        residual_ref[:, b * tile : (b + 1) * tile] = (
            rest_in[:, b].astype(f32).reshape(slices, tile).astype(bf16)
        )

    for turn in range(2):
        held = group if turn == 0 else 1 - group
        for copy in updates[turn * (quarters - 1) : (turn + 1) * (quarters - 1)]:
            copy.wait_recv()
        amount = own_update[turn]
        for k in range(1, quarters):
            amount = amount + update_in[turn, k].astype(f32)
        rows = pl.ds(pl.multiple_of(held * rows_half, rows_half), rows_half)
        old = image_ref[rows, pl.ds(pl.multiple_of(ray * share, share), share)].astype(f32)
        next_ref[rows, :] = old + relax_factor * amount
    for copy in carries + phases + edges + partials + backs + rests + updates:
        copy.wait_send()


def fast_shards(
    projections,
    phase_kernel,
    image,
    tile_library,
    tile_entry,
    tile_image,
    tile_slot,
    tile_count,
    slot_block,
):
    f32, bf16 = jnp.float32, jnp.bfloat16
    i32 = jnp.int32
    owners, quarters = lax.axis_size("dom"), lax.axis_size("ray")
    entries, tile = tile_library.shape[2], tile_library.shape[-1]
    _, slices, columns = projections.shape
    count = columns // tile
    ring = count + 1
    places = image.shape[0] // tile
    per = slices // owners
    capacity = tile_entry.shape[2]
    share = places * tile // quarters
    rows_half = slices // 2
    hbm = pl.BlockSpec(memory_space=pltpu.HBM)
    vmem = pl.BlockSpec(memory_space=pltpu.VMEM)
    sems = pltpu.SemaphoreType.DMA
    residual, image_next = pl.pallas_call(
        functools.partial(step_kernel, owners, quarters),
        out_shape=(
            jax.ShapeDtypeStruct((slices, columns), bf16),
            jax.ShapeDtypeStruct((slices, share), f32),
        ),
        in_specs=[hbm] * 8 + [pl.BlockSpec(memory_space=pltpu.SMEM)],
        out_specs=(vmem, vmem),
        scratch_shapes=[
            pltpu.VMEM(phase_kernel.shape, bf16),
            pltpu.VMEM((slices, columns), bf16),
            pltpu.VMEM((slices, places * tile), bf16),
            pltpu.VMEM((entries, tile, tile), bf16),
            pltpu.VMEM((1, capacity), i32),
            pltpu.VMEM((1, capacity), i32),
            pltpu.VMEM((1, capacity), i32),
            pltpu.VMEM((1, owners), i32),
            pltpu.VMEM((owners, 1, owners), i32),
            pltpu.SMEM((owners, 1, owners), i32),
            pltpu.VMEM((1, 3 * tile), f32),
            pltpu.VMEM((2, slices, tile), bf16),
            pltpu.VMEM((owners, ring, per, tile), bf16),
            pltpu.VMEM((owners, ring, per, tile), bf16),
            pltpu.VMEM((per, ring * tile), f32),
            pltpu.VMEM((owners, ring, per, tile), f32),
            pltpu.VMEM((owners * places, entries * SUB), f32),
            pltpu.VMEM((owners * places * SUB, entries * SUB), bf16),
            pltpu.VMEM((owners * tile, places * tile), bf16),
            pltpu.VMEM((owners, owners, per, tile), bf16),
            pltpu.VMEM((owners, owners, per, tile), bf16),
            pltpu.VMEM((owners, 32, tile), f32),
            pltpu.VMEM((owners, owners, per, tile), bf16),
            pltpu.VMEM((owners, owners, per, tile), bf16),
            pltpu.VMEM((owners, count, per, tile), bf16),
            pltpu.VMEM((owners, count, per, tile), bf16),
            pltpu.VMEM((2, rows_half, share), f32),
            pltpu.VMEM((2, quarters, rows_half, share), bf16),
            pltpu.VMEM((2, quarters, rows_half, share), bf16),
            sems((10,)),
            sems((2,)),
            sems((2,)),
        ]
        + [sems((owners,))] * 12
        + [sems((2 * quarters,))] * 2,
        compiler_params=pltpu.CompilerParams(
            collective_id=0, has_side_effects=True, vmem_limit_bytes=48 * 1024 * 1024
        ),
    )(
        *[
            pltpu.with_memory_space_constraint(x, pltpu.HBM)
            for x in (
                phase_kernel,
                projections,
                image.T,
                tile_library,
                tile_entry[0],
                tile_image[0],
                tile_slot[0],
                slot_block[0],
            )
        ],
        tile_count,
    )
    return residual[None], image_next.T


def fits_kernel(projections, phase_kernel, image, tile_library, tile_entry, *rest):
    owners, quarters = lax.axis_size("dom"), lax.axis_size("ray")
    tile = tile_library.shape[-1]
    angles, slices, columns = projections.shape
    return (
        angles == 1
        and slices % 16 == 0
        and slices == 8 * owners
        and owners == 8
        and tile == 128
        and phase_kernel.shape[0] == tile + 1
        and columns % tile == 0
        and tile_library.shape[2] == 16
        and quarters == 4
        and image.shape[0] == 16 * tile
        and tile_entry.shape[2] <= 256
    )


def any_shards(*args):
    if fits_kernel(*args):
        return fast_shards(*args)
    return shards(*args)


def solution(mesh):
    return jax.shard_map(
        any_shards,
        mesh=mesh,
        in_specs=(
            P("dom", None, "ray"),
            P(),
            P("dom", None),
            P("dom", "ray", None, None, None),
            P("dom", "ray", None),
            P("dom", "ray", None),
            P("dom", "ray", None),
            P("dom", "ray"),
            P("dom", "ray", None),
        ),
        out_specs=(P("dom", None, "ray"), P(("dom", "ray"), None)),
        check_vma=False,
    )
```

```python
import functools

import jax
import jax.numpy as jnp
from jax import lax
from jax.experimental import pallas as pl
from jax.experimental.pallas import tpu as pltpu
from jax.sharding import PartitionSpec as P

SMOOTH = 8


relax_factor = 0.25


def with_halo(cells, sides, width):
    for axis, dim in sides:
        count = lax.axis_size(axis)
        ends = count - 1
        head = lax.slice_in_dim(cells, 0, width, axis=dim)
        tail = lax.slice_in_dim(cells, cells.shape[dim] - width, cells.shape[dim], axis=dim)
        cells = jnp.concatenate(
            [
                lax.ppermute(tail, axis, [(i, (i + 1) % count) for i in range(ends)]),
                cells,
                lax.ppermute(head, axis, [((i + 1) % count, i) for i in range(ends)]),
            ],
            axis=dim,
        )
    return cells


def toeplitz(kernel, tile_size):
    taps = kernel.shape[0]
    padded = jnp.concatenate([kernel, jnp.zeros((2 * tile_size + 1 - taps,), kernel.dtype)])
    tiled = jnp.tile(padded, tile_size)[: 2 * tile_size * tile_size]
    return tiled.reshape(tile_size, 2 * tile_size).T


def phase_filter(projections, phase_kernel, tile_size):
    half_width = (phase_kernel.shape[0] - 1) // 2
    angles, slices, columns = projections.shape
    block_count = columns // tile_size
    rimmed = with_halo(projections, (("ray", 2),), half_width)
    padded = jnp.pad(rimmed, ((0, 0), (0, 0), (0, 2 * tile_size - 2 * half_width)))
    blocks = padded.reshape(angles, slices, block_count + 2, tile_size)
    windows = jnp.concatenate(
        [blocks[:, :, :block_count], blocks[:, :, 1 : block_count + 1]], axis=-1
    )
    filtered = jnp.einsum(
        "asbi,ij->asbj",
        windows,
        toeplitz(phase_kernel, tile_size),
        preferred_element_type=jnp.float32,
    )
    return filtered.reshape(angles, slices, columns).astype(jnp.bfloat16)


def stripe_profile(gathered):
    profile = jnp.median(gathered.astype(jnp.float32), axis=0)
    columns = profile.shape[1]
    rimmed = with_halo(profile, (("ray", 1),), SMOOTH)
    window_sum = jnp.zeros_like(profile)
    for offset in range(2 * SMOOTH + 1):
        window_sum = window_sum + rimmed[:, offset : offset + columns]
    position = lax.axis_index("ray") * columns + jnp.arange(columns)
    detector = lax.axis_size("ray") * columns
    in_range = (
        jnp.minimum(position + SMOOTH, detector - 1) - jnp.maximum(position - SMOOTH, 0) + 1
    ).astype(jnp.float32)
    return (profile - window_sum / in_range).astype(jnp.bfloat16)


def shards(
    projections,
    phase_kernel,
    image,
    tile_library,
    tile_entry,
    tile_image,
    tile_slot,
    tile_count,
    slot_block,
):
    tile_size = tile_library.shape[-1]
    angles, slices, columns = projections.shape
    phase = phase_filter(projections, phase_kernel, tile_size)
    gathered = lax.all_to_all(phase, "dom", split_axis=1, concat_axis=0, tiled=True)
    stripe = stripe_profile(gathered)
    fixed_rows = (gathered.astype(jnp.float32) - stripe.astype(jnp.float32)[None]).astype(
        jnp.bfloat16
    )
    corrected = lax.all_to_all(fixed_rows, "dom", split_axis=0, concat_axis=1, tiled=True)
    owners = lax.axis_size("dom")
    library = tile_library[0, 0]
    entries = tile_entry[0, 0]
    images = tile_image[0, 0]
    slots = tile_slot[0, 0]
    capacity = entries.shape[0]
    block_size = 64
    turn_count = capacity // block_size
    image_blocks = image.reshape(-1, tile_size, slices)
    block_total = image_blocks.shape[0]
    live_mask = jnp.arange(capacity) < tile_count[0, 0]
    slot_target = jnp.where(live_mask, slots, owners)
    image_target = jnp.where(live_mask, images, block_total)

    def forward_turn(turn_index, partial_value):
        first_tile = turn_index * block_size
        chosen = lax.dynamic_slice_in_dim(entries, first_tile, block_size)
        placed = lax.dynamic_slice_in_dim(images, first_tile, block_size)
        destined = lax.dynamic_slice_in_dim(slot_target, first_tile, block_size)
        product = jnp.einsum(
            "krp,kps->ksr",
            library[chosen],
            image_blocks[placed],
            preferred_element_type=jnp.float32,
        )
        return partial_value.at[destined].add(product, mode="drop")

    partial_value = lax.fori_loop(
        0, turn_count, forward_turn, jnp.zeros((owners, slices, tile_size), jnp.float32)
    )
    received = lax.all_to_all(
        partial_value.astype(jnp.bfloat16), "dom", split_axis=0, concat_axis=0, tiled=True
    )
    per_owner = columns // tile_size
    carried = slot_block[0, 0]
    block_ids = jnp.arange(angles * per_owner).reshape(angles, per_owner)
    selector = (block_ids[:, :, None] == carried[None, None, :]).astype(jnp.bfloat16)
    forward = jnp.einsum("abd,dst->asbt", selector, received, preferred_element_type=jnp.float32)
    residual = (corrected.astype(jnp.float32) - forward.reshape(angles, slices, columns)).astype(
        jnp.bfloat16
    )
    back = jnp.einsum(
        "abd,asbt->dst",
        selector,
        residual.reshape(angles, slices, per_owner, tile_size),
        preferred_element_type=jnp.float32,
    ).astype(jnp.bfloat16)
    returned = lax.all_to_all(back, "dom", split_axis=0, concat_axis=0, tiled=True)

    def adjoint_turn(turn_index, gradient):
        first_tile = turn_index * block_size
        chosen = lax.dynamic_slice_in_dim(entries, first_tile, block_size)
        sourced = lax.dynamic_slice_in_dim(slots, first_tile, block_size)
        destined = lax.dynamic_slice_in_dim(image_target, first_tile, block_size)
        product = jnp.einsum(
            "krp,ksr->kps", library[chosen], returned[sourced], preferred_element_type=jnp.float32
        )
        return gradient.at[destined].add(product, mode="drop")

    gradient = lax.fori_loop(
        0, turn_count, adjoint_turn, jnp.zeros((block_total, tile_size, slices), jnp.float32)
    )
    gradient = gradient.reshape(-1, slices)
    rows_own = gradient.shape[0] // lax.axis_size("ray")
    update = lax.psum_scatter(gradient, "ray", scatter_dimension=0, tiled=True)
    own_image = lax.dynamic_slice_in_dim(image, lax.axis_index("ray") * rows_own, rows_own)
    image_next = own_image.astype(jnp.float32) + relax_factor * update
    return (residual, image_next)


MESH = pl.DeviceIdType.MESH
NT = (((1,), (1,)), ((), ()))
NN = (((1,), (0,)), ((), ()))
SUB = 16
PARTS = 2


def dot(a, b, dims):
    return lax.dot_general(a, b, dims, preferred_element_type=jnp.float32)


def ordered(a, b):
    return jnp.minimum(a, b), jnp.maximum(a, b)


def sorted_four(a, b, c, d):
    a, b = ordered(a, b)
    c, d = ordered(c, d)
    a, c = ordered(a, c)
    b, d = ordered(b, d)
    b, c = ordered(b, c)
    return a, b, c, d


def median_of_eight(values):
    low = sorted_four(*values[:4])
    high = sorted_four(*values[4:])
    below = [jnp.minimum(low[i], high[3 - i]) for i in range(4)]
    above = [jnp.maximum(low[i], high[3 - i]) for i in range(4)]
    fourth = jnp.maximum(jnp.maximum(below[0], below[1]), jnp.maximum(below[2], below[3]))
    fifth = jnp.minimum(jnp.minimum(above[0], above[1]), jnp.minimum(above[2], above[3]))
    return (fourth + fifth) * 0.5


def step_kernel(
    owners,
    quarters,
    taps_any,
    proj_any,
    image_any,
    library_any,
    entry_any,
    place_any,
    slot_any,
    carried_any,
    count_ref,
    residual_ref,
    next_ref,
    taps_ref,
    proj_ref,
    image_ref,
    library_ref,
    entry_ref,
    place_ref,
    slot_ref,
    carried_own,
    carried_all,
    carried_ref,
    taps_wide,
    rim,
    phase_out,
    phase_in,
    profile_ref,
    fixed,
    counted,
    spread_ref,
    matrix,
    partial_out,
    partial_in,
    same_ref,
    back_out,
    back_in,
    rest_out,
    rest_in,
    stripe_own,
    stripe_far,
    twin_in,
    forward,
    gathered,
    own_update,
    update_out,
    update_in,
    load_sem,
    halo_send,
    halo_recv,
    carried_send,
    carried_recv,
    phase_send,
    phase_recv,
    edge_send,
    edge_recv,
    partial_send,
    partial_recv,
    back_send,
    back_recv,
    rest_send,
    rest_recv,
    stripe_send,
    stripe_recv,
    twin_send,
    twin_recv,
    update_send,
    update_recv,
):
    f32, bf16 = jnp.float32, jnp.bfloat16
    me, ray = lax.axis_index("dom"), lax.axis_index("ray")
    slices, columns = proj_ref.shape
    entries, tile = library_ref.shape[0], library_ref.shape[-1]
    places = image_ref.shape[1] // tile
    count = columns // tile
    ring = count + 1
    inner = count - 2
    per = slices // owners
    side = owners // 2
    half = tile // 2
    share = places * tile // quarters
    rows_half = side * per
    some = owners // PARTS

    group, spot = me // side, lax.rem(me, side)

    def dom_peer(k):
        if k >= side:
            return (1 - group) * side + lax.rem(spot + k - side, side)
        return group * side + lax.rem(spot + k, side)

    dom_order = list(range(1, owners))

    chip, core = ray // 2, lax.rem(ray, 2)

    def ray_twin(k):
        chip_to = 1 - chip if k >= 2 else chip
        core_to = 1 - core if k % 2 else core
        return chip_to * 2 + core_to

    def ray_next(k):
        return lax.rem(ray + k, quarters)

    barrier = pltpu.get_barrier_semaphore()
    for k in range(1, owners):
        pl.semaphore_signal(barrier, inc=1, device_id=(dom_peer(k), ray), device_id_type=MESH)
    for k in range(1, quarters):
        pl.semaphore_signal(barrier, inc=1, device_id=(me, ray_next(k)), device_id_type=MESH)

    pairs = [
        (proj_any.at[0], proj_ref),
        (taps_any, taps_ref),
        (entry_any, entry_ref),
        (place_any, place_ref),
        (slot_any, slot_ref),
        (carried_any, carried_own),
        (library_any.at[0, 0], library_ref),
        (image_any, image_ref),
    ]
    loads = [
        pltpu.make_async_copy(src, dst, load_sem.at[i]) for i, (src, dst) in enumerate(pairs)
    ]
    for copy in loads:
        copy.start()

    def dom_copy(src, dst, send, recv, k, base=0):
        return pltpu.make_async_remote_copy(
            src_ref=src,
            dst_ref=dst,
            send_sem=send.at[base + k],
            recv_sem=recv.at[base + k],
            device_id=(dom_peer(k), ray),
            device_id_type=MESH,
        )

    def ray_copy(src, dst, send, recv, slot, peer):
        return pltpu.make_async_remote_copy(
            src_ref=src,
            dst_ref=dst,
            send_sem=send.at[slot],
            recv_sem=recv.at[slot],
            device_id=(me, peer),
            device_id_type=MESH,
        )

    def block(b):
        return proj_ref[:, b * tile : (b + 1) * tile]

    loads[1].wait()
    taps_wide[...] = jnp.zeros(taps_wide.shape, f32)
    taps_wide[:, : taps_ref.shape[0]] = taps_ref[...].astype(f32)[None]
    spread = jnp.broadcast_to(taps_wide[...], (tile, taps_wide.shape[1]))
    weights = pltpu.roll(spread, half, 1, stride=1, stride_axis=0).astype(bf16)
    loads[0].wait()
    two = jnp.concatenate(
        [proj_ref[:, (b - 1) * tile : (b + 1) * tile] for b in range(1, count - 1)], axis=0
    )
    third = jnp.concatenate([block(b + 1) for b in range(1, count - 1)], axis=0)
    phase = dot(two, weights[:, : 2 * tile], NT) + dot(third, weights[:, 2 * tile :], NT)
    phase = phase.reshape(inner, owners, per, tile)
    for owner in range(owners):
        phase_out[owner, :inner] = phase[:, owner].astype(bf16)

    loads[5].wait()
    pl.semaphore_wait(barrier, owners + quarters - 2)

    carries = [
        dom_copy(carried_own, carried_all.at[me], carried_send, carried_recv, k) for k in dom_order
    ]
    for copy in carries:
        copy.start()

    halos = [
        ray_copy(
            proj_ref.at[:, pl.ds(columns - tile, tile)],
            rim.at[0],
            halo_send,
            halo_recv,
            0,
            ray_next(1),
        ),
        ray_copy(
            proj_ref.at[:, pl.ds(0, tile)], rim.at[1], halo_send, halo_recv, 1, ray_next(quarters - 1)
        ),
    ]
    for copy in halos:
        copy.start()
    phases = [
        dom_copy(
            phase_out.at[dom_peer(k), pl.ds(0, inner)],
            phase_in.at[me, pl.ds(0, inner)],
            phase_send,
            phase_recv,
            k,
        )
        for k in dom_order
    ]
    for copy in phases:
        copy.start()
    for i in range(2, 5):
        loads[i].wait()
    capacity = entry_ref.shape[1]
    alive = lax.broadcasted_iota(jnp.int32, (1, capacity), 1) < count_ref[0, 0]
    code = jnp.where(alive, slot_ref[...] * places + place_ref[...], -1)
    pick = jnp.where(
        lax.broadcasted_iota(jnp.int32, (owners * places, capacity), 0) == code, 1.0, 0.0
    ).astype(bf16)
    which = jnp.where(
        lax.broadcasted_iota(jnp.int32, (entries * SUB, capacity), 0) // SUB == entry_ref[...],
        1.0,
        0.0,
    ).astype(bf16)
    counted[...] = dot(pick, which, NT)
    diagonal = lax.rem(
        lax.broadcasted_iota(jnp.int32, (SUB, entries * SUB), 1), SUB
    ) == lax.broadcasted_iota(jnp.int32, (SUB, entries * SUB), 0)

    def widen(step, carry):
        for i in range(8):
            at = step * 8 + i
            row = jnp.broadcast_to(counted[pl.ds(at, 1), :], (SUB, entries * SUB))
            start = pl.multiple_of(at * SUB, SUB)
            spread_ref[pl.ds(start, SUB), :] = jnp.where(diagonal, row, 0.0).astype(bf16)
        return carry

    lax.fori_loop(0, owners * places // 8, widen, 0)

    loads[6].wait()

    def build(step, carry):
        first = pl.multiple_of(step * 2 * SUB, 2 * SUB)
        right = jnp.concatenate(
            [
                library_ref[:, pl.ds(first + i * SUB, SUB), :].reshape(entries * SUB, tile)
                for i in range(2)
            ],
            axis=1,
        )
        for owner in range(owners):
            rows = places * SUB
            made = dot(spread_ref[owner * rows : (owner + 1) * rows, :], right, NN)
            for place in range(places):
                for i in range(2):
                    start = pl.multiple_of(first + owner * tile + i * SUB, SUB)
                    matrix[pl.ds(start, SUB), place * tile : (place + 1) * tile] = made[
                        place * SUB : (place + 1) * SUB, i * tile : (i + 1) * tile
                    ].astype(bf16)
        return carry

    lax.fori_loop(0, tile // (2 * SUB), build, 0)

    for copy in halos:
        copy.wait()

    @pl.when(ray == 0)
    def _():
        rim[0] = jnp.zeros((slices, tile), bf16)

    @pl.when(ray == quarters - 1)
    def _():
        rim[1] = jnp.zeros((slices, tile), bf16)

    before, after = rim[0], rim[1]
    two = jnp.concatenate(
        [
            proj_ref[:, (count - 2) * tile : count * tile],
            jnp.concatenate([block(count - 1), after], axis=1),
            jnp.concatenate([before, block(0)], axis=1),
            jnp.concatenate([before, before], axis=1),
        ],
        axis=0,
    )
    third = jnp.concatenate([after, after, block(1), block(0)], axis=0)
    edge = dot(two, weights[:, : 2 * tile], NT) + dot(third, weights[:, 2 * tile :], NT)
    edge = edge.reshape(4, owners, per, tile)
    lane = lax.broadcasted_iota(jnp.int32, (owners, per, tile), 2)
    phase_out[:, inner] = edge[0].astype(bf16)
    phase_out[:, inner + 1] = jnp.where(lane < half, edge[1], edge[3]).astype(bf16)
    phase_out[:, inner + 2] = edge[2].astype(bf16)
    edges = [
        dom_copy(
            phase_out.at[dom_peer(k), pl.ds(inner, 3)],
            phase_in.at[me, pl.ds(inner, 3)],
            edge_send,
            edge_recv,
            k,
        )
        for k in dom_order
    ]
    for copy in edges:
        copy.start()
    phase_in[me] = phase_out[me]

    loads[7].wait()
    partials = []
    for part in range(PARTS):
        for owner in range(part * some, (part + 1) * some, 2):
            made = dot(image_ref[...], matrix[owner * tile : (owner + 2) * tile, :], NT)
            for i in range(2):
                partial_out[:, owner + i] = (
                    made[:, i * tile : (i + 1) * tile].reshape(owners, per, tile).astype(bf16)
                )
        chosen = pl.ds(part * some, some)
        partials.append(
            [
                dom_copy(
                    partial_out.at[dom_peer(k), chosen],
                    partial_in.at[me, chosen],
                    partial_send,
                    partial_recv,
                    k,
                    part * owners,
                )
                for k in dom_order
            ]
        )
        for copy in partials[part]:
            copy.start()
    partial_in[me] = partial_out[me]

    carried_all[me] = carried_own[...]
    for copy in carries:
        copy.wait_recv()
    to_scalar = pltpu.make_async_copy(carried_all, carried_ref, load_sem.at[len(loads)])
    to_scalar.start()
    to_scalar.wait()
    duos = [(a, b) for a in range(owners) for b in range(a + 1, owners)]

    def compare(owner, carry):
        for i, (a, b) in enumerate(duos):
            same = jnp.where(carried_ref[owner, 0, a] == carried_ref[owner, 0, b], 1.0, 0.0)
            same_ref[owner, i : i + 1, :] = jnp.full((1, tile), same, f32)
        return carry

    lax.fori_loop(0, owners, compare, 0)

    def profile_of(i):
        return median_of_eight([phase_in[a, i].astype(f32) for a in range(owners)])

    for copy in phases:
        copy.wait_recv()
    for i in range(inner):
        profile_ref[:, i * tile : (i + 1) * tile] = profile_of(i)
    for copy in edges:
        copy.wait_recv()
    for i in range(inner, ring):
        profile_ref[:, i * tile : (i + 1) * tile] = profile_of(i)

    width = ring * tile
    detector = quarters * columns
    at = lax.broadcasted_iota(jnp.int32, (1, width), 1)
    position = ray * columns + jnp.where(at < count * tile - half, at + tile, at - columns)
    profile = jnp.where((position >= 0) & (position < detector), profile_ref[...], 0.0)
    run = profile
    reach = 1
    while reach < 2 * SMOOTH:
        run = run + pltpu.roll(run, reach, 1)
        reach *= 2
    window = pltpu.roll(run, width - (SMOOTH - 1), 1) + pltpu.roll(profile, width - SMOOTH, 1)
    in_range = (
        jnp.minimum(position + SMOOTH, detector - 1) - jnp.maximum(position - SMOOTH, 0) + 1
    ).astype(f32)
    stripe = (profile - window / in_range).astype(bf16).astype(f32)
    for b in range(count):
        i = (b - 1) % ring
        stripe_own[b] = stripe[:, i * tile : (i + 1) * tile].astype(bf16)
    for a in range(owners):
        for i in range(ring):
            if i != count - 1:
                fixed[a, i] = (
                    (phase_in[a, i].astype(f32) - stripe[:, i * tile : (i + 1) * tile])
                    .astype(bf16)
                    .astype(f32)
                )

    def ring_spot(b):
        return jnp.where(b == 0, ring - 1, b - 1)

    def carry_back(owner, carry):
        part = [partial_in[d, owner].astype(f32) for d in range(owners)]
        total = list(part)
        for i, (a, b) in enumerate(duos):
            same = jnp.broadcast_to(same_ref[owner, i : i + 1, :], (per, tile))
            total[a] = total[a] + same * part[b]
            total[b] = total[b] + same * part[a]
        for d in range(owners):
            back_out[d, owner] = (
                fixed[owner, ring_spot(carried_ref[owner, 0, d])] - total[d]
            ).astype(bf16)
        return carry

    backs = []
    for part in range(PARTS):
        for copy in partials[part]:
            copy.wait_recv()
        lax.fori_loop(part * some, (part + 1) * some, carry_back, 0)
        chosen = pl.ds(part * some, some)
        backs.append(
            [
                dom_copy(
                    back_out.at[dom_peer(k), chosen],
                    back_in.at[me, chosen],
                    back_send,
                    back_recv,
                    k,
                    part * owners,
                )
                for k in dom_order
            ]
        )
        for copy in backs[part]:
            copy.start()
    back_in[me] = back_out[me]

    crossing = dom_copy(stripe_own, stripe_far.at[spot], stripe_send, stripe_recv, side)
    crossing.start()
    twins = [
        dom_copy(
            partial_out.at[pl.ds((1 - dom_peer(k) // side) * side, side), dom_peer(k)],
            twin_in.at[me],
            twin_send,
            twin_recv,
            k,
        )
        for k in dom_order
    ]
    for copy in twins:
        copy.start()
    twin_in[me] = partial_out[pl.ds((1 - group) * side, side), me]

    def whole(i, carry):
        owner = group * side + i
        part = [partial_in[d, owner].astype(f32) for d in range(owners)]
        where_to = [carried_ref[owner, 0, d] for d in range(owners)]
        for b in range(count):
            total = fixed[owner, (b - 1) % ring]
            taken = jnp.zeros((per, tile), f32)
            for d in range(owners):
                taken = taken + jnp.where(where_to[d] == b, 1.0, 0.0).astype(f32) * part[d]
            rest_out[i, b] = (total - taken).astype(bf16)
        return carry

    lax.fori_loop(0, side, whole, 0)
    rests = [
        dom_copy(
            rest_out.at[lax.rem(spot + k, side)], rest_in.at[me], rest_send, rest_recv, k
        )
        for k in range(1, side)
    ]
    for copy in rests:
        copy.start()
    rest_in[me] = rest_out[spot]

    updates = []
    for turn in range(2):
        held = group if turn == 0 else 1 - group
        first = held * side
        for part in range(PARTS):
            for copy in backs[part][side - 1 :] if turn else backs[part][: side - 1]:
                copy.wait_recv()
            left = jnp.concatenate(
                [
                    back_in[pl.ds(first, side), owner]
                    .astype(f32)
                    .reshape(rows_half, tile)
                    .astype(bf16)
                    for owner in range(part * some, (part + 1) * some)
                ],
                axis=1,
            )
            rows = slice(part * some * tile, (part + 1) * some * tile)
            for k in (2, 3, 1, 0):
                start = pl.multiple_of(ray_twin(k) * share, share)
                made = dot(left, matrix[rows, pl.ds(start, share)], NN)
                if part > 0:
                    made = made + gathered[k]
                if part < PARTS - 1:
                    gathered[k] = made
                elif k == 0:
                    own_update[turn] = made
                else:
                    update_out[turn, k] = made.astype(bf16)
                    copy = ray_copy(
                        update_out.at[turn, k],
                        update_in.at[turn, k],
                        update_send,
                        update_recv,
                        turn * quarters + k,
                        ray_twin(k),
                    )
                    copy.start()
                    updates.append(copy)

    crossing.wait_recv()
    relays = [
        dom_copy(stripe_far.at[spot], stripe_far.at[spot], stripe_send, stripe_recv, k)
        for k in range(1, side)
    ]
    for copy in relays:
        copy.start()

    for copy in twins:
        copy.wait_recv()
    other = pl.ds((1 - group) * side, side)
    own_spots = [carried_ref[me, 0, d] for d in range(owners)]
    taken_by = [twin_in[d].astype(f32) for d in range(owners)]
    for b in range(count):
        taken = jnp.zeros((side, per, tile), f32)
        for d in range(owners):
            taken = taken + jnp.where(own_spots[d] == b, 1.0, 0.0).astype(f32) * taken_by[d]
        forward[b] = taken
    for copy in relays:
        copy.wait_recv()
    for b in range(count):
        clean = (
            (phase_out[other, (b - 1) % ring].astype(f32) - stripe_far[:, b].astype(f32))
            .astype(bf16)
            .astype(f32)
        )
        rest_in[other, b] = (clean - forward[b]).astype(bf16)
    for copy in rests:
        copy.wait_recv()
    for b in range(count):
        residual_ref[:, b * tile : (b + 1) * tile] = (
            rest_in[:, b].astype(f32).reshape(slices, tile).astype(bf16)
        )

    for turn in range(2):
        held = group if turn == 0 else 1 - group
        for copy in updates[turn * (quarters - 1) : (turn + 1) * (quarters - 1)]:
            copy.wait_recv()
        amount = own_update[turn]
        for k in range(1, quarters):
            amount = amount + update_in[turn, k].astype(f32)
        rows = pl.ds(pl.multiple_of(held * rows_half, rows_half), rows_half)
        old = image_ref[rows, pl.ds(pl.multiple_of(ray * share, share), share)].astype(f32)
        next_ref[rows, :] = old + relax_factor * amount
    sent = carries + phases + edges + sum(partials, []) + sum(backs, [])
    for copy in sent + [crossing] + twins + rests + relays + updates:
        copy.wait_send()


def store_kernel(residual_ref, next_ref, residual_out, next_out, sem):
    copies = [
        pltpu.make_async_copy(residual_ref, residual_out, sem.at[0]),
        pltpu.make_async_copy(next_ref, next_out, sem.at[1]),
    ]
    for copy in copies:
        copy.start()
    for copy in copies:
        copy.wait()


def fast_shards(
    projections,
    phase_kernel,
    image,
    tile_library,
    tile_entry,
    tile_image,
    tile_slot,
    tile_count,
    slot_block,
):
    f32, bf16 = jnp.float32, jnp.bfloat16
    i32 = jnp.int32
    owners, quarters = lax.axis_size("dom"), lax.axis_size("ray")
    entries, tile = tile_library.shape[2], tile_library.shape[-1]
    _, slices, columns = projections.shape
    count = columns // tile
    ring = count + 1
    places = image.shape[0] // tile
    per = slices // owners
    capacity = tile_entry.shape[2]
    share = places * tile // quarters
    rows_half = slices // 2
    hbm = pl.BlockSpec(memory_space=pltpu.HBM)
    vmem = pl.BlockSpec(memory_space=pltpu.VMEM)
    sems = pltpu.SemaphoreType.DMA
    residual, image_next = pl.pallas_call(
        functools.partial(step_kernel, owners, quarters),
        out_shape=(
            jax.ShapeDtypeStruct((slices, columns), bf16),
            jax.ShapeDtypeStruct((slices, share), f32),
        ),
        in_specs=[hbm] * 8 + [pl.BlockSpec(memory_space=pltpu.SMEM)],
        out_specs=(vmem, vmem),
        scratch_shapes=[
            pltpu.VMEM(phase_kernel.shape, bf16),
            pltpu.VMEM((slices, columns), bf16),
            pltpu.VMEM((slices, places * tile), bf16),
            pltpu.VMEM((entries, tile, tile), bf16),
            pltpu.VMEM((1, capacity), i32),
            pltpu.VMEM((1, capacity), i32),
            pltpu.VMEM((1, capacity), i32),
            pltpu.VMEM((1, owners), i32),
            pltpu.VMEM((owners, 1, owners), i32),
            pltpu.SMEM((owners, 1, owners), i32),
            pltpu.VMEM((1, 3 * tile), f32),
            pltpu.VMEM((2, slices, tile), bf16),
            pltpu.VMEM((owners, ring, per, tile), bf16),
            pltpu.VMEM((owners, ring, per, tile), bf16),
            pltpu.VMEM((per, ring * tile), f32),
            pltpu.VMEM((owners, ring, per, tile), f32),
            pltpu.VMEM((owners * places, entries * SUB), f32),
            pltpu.VMEM((owners * places * SUB, entries * SUB), bf16),
            pltpu.VMEM((owners * tile, places * tile), bf16),
            pltpu.VMEM((owners, owners, per, tile), bf16),
            pltpu.VMEM((owners, owners, per, tile), bf16),
            pltpu.VMEM((owners, 32, tile), f32),
            pltpu.VMEM((owners, owners, per, tile), bf16),
            pltpu.VMEM((owners, owners, per, tile), bf16),
            pltpu.VMEM((owners // 2, count, per, tile), bf16),
            pltpu.VMEM((owners, count, per, tile), bf16),
            pltpu.VMEM((count, per, tile), bf16),
            pltpu.VMEM((owners // 2, count, per, tile), bf16),
            pltpu.VMEM((owners, owners // 2, per, tile), bf16),
            pltpu.VMEM((count, owners // 2, per, tile), f32),
            pltpu.VMEM((quarters, rows_half, share), f32),
            pltpu.VMEM((2, rows_half, share), f32),
            pltpu.VMEM((2, quarters, rows_half, share), bf16),
            pltpu.VMEM((2, quarters, rows_half, share), bf16),
            sems((10,)),
            sems((2,)),
            sems((2,)),
        ]
        + [sems((owners,))] * 6
        + [sems((PARTS * owners,))] * 4
        + [sems((owners,))] * 6
        + [sems((2 * quarters,))] * 2,
        compiler_params=pltpu.CompilerParams(
            collective_id=0, has_side_effects=True, vmem_limit_bytes=48 * 1024 * 1024
        ),
    )(
        *[
            pltpu.with_memory_space_constraint(x, pltpu.HBM)
            for x in (
                phase_kernel,
                projections,
                image.T,
                tile_library,
                tile_entry[0],
                tile_image[0],
                tile_slot[0],
                slot_block[0],
            )
        ],
        tile_count,
    )
    residual, image_next = pl.pallas_call(
        store_kernel,
        out_shape=(
            jax.ShapeDtypeStruct(residual.shape, bf16),
            jax.ShapeDtypeStruct(image_next.shape, f32),
        ),
        in_specs=[pl.BlockSpec(memory_space=pl.ANY)] * 2,
        out_specs=[pl.BlockSpec(memory_space=pl.ANY)] * 2,
        scratch_shapes=[sems((2,))],
    )(
        pltpu.with_memory_space_constraint(residual, pltpu.VMEM),
        pltpu.with_memory_space_constraint(image_next, pltpu.VMEM),
    )
    return residual[None], image_next.T


def fits_kernel(projections, phase_kernel, image, tile_library, tile_entry, *rest):
    owners, quarters = lax.axis_size("dom"), lax.axis_size("ray")
    tile = tile_library.shape[-1]
    angles, slices, columns = projections.shape
    return (
        angles == 1
        and slices % 16 == 0
        and slices == 8 * owners
        and owners == 8
        and tile == 128
        and phase_kernel.shape[0] == tile + 1
        and columns % tile == 0
        and tile_library.shape[2] == 16
        and quarters == 4
        and image.shape[0] == 16 * tile
        and tile_entry.shape[2] <= 256
    )


def any_shards(*args):
    if fits_kernel(*args):
        return fast_shards(*args)
    return shards(*args)


def solution(mesh):
    return jax.shard_map(
        any_shards,
        mesh=mesh,
        in_specs=(
            P("dom", None, "ray"),
            P(),
            P("dom", None),
            P("dom", "ray", None, None, None),
            P("dom", "ray", None),
            P("dom", "ray", None),
            P("dom", "ray", None),
            P("dom", "ray"),
            P("dom", "ray", None),
        ),
        out_specs=(P("dom", None, "ray"), P(("dom", "ray"), None)),
        check_vma=False,
    )
```

```python
import functools

import jax
import jax.numpy as jnp
from jax import lax
from jax.experimental import pallas as pl
from jax.experimental.pallas import tpu as pltpu
from jax.sharding import PartitionSpec as P

SMOOTH = 8


relax_factor = 0.25


def with_halo(cells, sides, width):
    for axis, dim in sides:
        count = lax.axis_size(axis)
        ends = count - 1
        head = lax.slice_in_dim(cells, 0, width, axis=dim)
        tail = lax.slice_in_dim(cells, cells.shape[dim] - width, cells.shape[dim], axis=dim)
        cells = jnp.concatenate(
            [
                lax.ppermute(tail, axis, [(i, (i + 1) % count) for i in range(ends)]),
                cells,
                lax.ppermute(head, axis, [((i + 1) % count, i) for i in range(ends)]),
            ],
            axis=dim,
        )
    return cells


def toeplitz(kernel, tile_size):
    taps = kernel.shape[0]
    padded = jnp.concatenate([kernel, jnp.zeros((2 * tile_size + 1 - taps,), kernel.dtype)])
    tiled = jnp.tile(padded, tile_size)[: 2 * tile_size * tile_size]
    return tiled.reshape(tile_size, 2 * tile_size).T


def phase_filter(projections, phase_kernel, tile_size):
    half_width = (phase_kernel.shape[0] - 1) // 2
    angles, slices, columns = projections.shape
    block_count = columns // tile_size
    rimmed = with_halo(projections, (("ray", 2),), half_width)
    padded = jnp.pad(rimmed, ((0, 0), (0, 0), (0, 2 * tile_size - 2 * half_width)))
    blocks = padded.reshape(angles, slices, block_count + 2, tile_size)
    windows = jnp.concatenate(
        [blocks[:, :, :block_count], blocks[:, :, 1 : block_count + 1]], axis=-1
    )
    filtered = jnp.einsum(
        "asbi,ij->asbj",
        windows,
        toeplitz(phase_kernel, tile_size),
        preferred_element_type=jnp.float32,
    )
    return filtered.reshape(angles, slices, columns).astype(jnp.bfloat16)


def stripe_profile(gathered):
    profile = jnp.median(gathered.astype(jnp.float32), axis=0)
    columns = profile.shape[1]
    rimmed = with_halo(profile, (("ray", 1),), SMOOTH)
    window_sum = jnp.zeros_like(profile)
    for offset in range(2 * SMOOTH + 1):
        window_sum = window_sum + rimmed[:, offset : offset + columns]
    position = lax.axis_index("ray") * columns + jnp.arange(columns)
    detector = lax.axis_size("ray") * columns
    in_range = (
        jnp.minimum(position + SMOOTH, detector - 1) - jnp.maximum(position - SMOOTH, 0) + 1
    ).astype(jnp.float32)
    return (profile - window_sum / in_range).astype(jnp.bfloat16)


def shards(
    projections,
    phase_kernel,
    image,
    tile_library,
    tile_entry,
    tile_image,
    tile_slot,
    tile_count,
    slot_block,
):
    tile_size = tile_library.shape[-1]
    angles, slices, columns = projections.shape
    phase = phase_filter(projections, phase_kernel, tile_size)
    gathered = lax.all_to_all(phase, "dom", split_axis=1, concat_axis=0, tiled=True)
    stripe = stripe_profile(gathered)
    fixed_rows = (gathered.astype(jnp.float32) - stripe.astype(jnp.float32)[None]).astype(
        jnp.bfloat16
    )
    corrected = lax.all_to_all(fixed_rows, "dom", split_axis=0, concat_axis=1, tiled=True)
    owners = lax.axis_size("dom")
    library = tile_library[0, 0]
    entries = tile_entry[0, 0]
    images = tile_image[0, 0]
    slots = tile_slot[0, 0]
    capacity = entries.shape[0]
    block_size = 64
    turn_count = capacity // block_size
    image_blocks = image.reshape(-1, tile_size, slices)
    block_total = image_blocks.shape[0]
    live_mask = jnp.arange(capacity) < tile_count[0, 0]
    slot_target = jnp.where(live_mask, slots, owners)
    image_target = jnp.where(live_mask, images, block_total)

    def forward_turn(turn_index, partial_value):
        first_tile = turn_index * block_size
        chosen = lax.dynamic_slice_in_dim(entries, first_tile, block_size)
        placed = lax.dynamic_slice_in_dim(images, first_tile, block_size)
        destined = lax.dynamic_slice_in_dim(slot_target, first_tile, block_size)
        product = jnp.einsum(
            "krp,kps->ksr",
            library[chosen],
            image_blocks[placed],
            preferred_element_type=jnp.float32,
        )
        return partial_value.at[destined].add(product, mode="drop")

    partial_value = lax.fori_loop(
        0, turn_count, forward_turn, jnp.zeros((owners, slices, tile_size), jnp.float32)
    )
    received = lax.all_to_all(
        partial_value.astype(jnp.bfloat16), "dom", split_axis=0, concat_axis=0, tiled=True
    )
    per_owner = columns // tile_size
    carried = slot_block[0, 0]
    block_ids = jnp.arange(angles * per_owner).reshape(angles, per_owner)
    selector = (block_ids[:, :, None] == carried[None, None, :]).astype(jnp.bfloat16)
    forward = jnp.einsum("abd,dst->asbt", selector, received, preferred_element_type=jnp.float32)
    residual = (corrected.astype(jnp.float32) - forward.reshape(angles, slices, columns)).astype(
        jnp.bfloat16
    )
    back = jnp.einsum(
        "abd,asbt->dst",
        selector,
        residual.reshape(angles, slices, per_owner, tile_size),
        preferred_element_type=jnp.float32,
    ).astype(jnp.bfloat16)
    returned = lax.all_to_all(back, "dom", split_axis=0, concat_axis=0, tiled=True)

    def adjoint_turn(turn_index, gradient):
        first_tile = turn_index * block_size
        chosen = lax.dynamic_slice_in_dim(entries, first_tile, block_size)
        sourced = lax.dynamic_slice_in_dim(slots, first_tile, block_size)
        destined = lax.dynamic_slice_in_dim(image_target, first_tile, block_size)
        product = jnp.einsum(
            "krp,ksr->kps", library[chosen], returned[sourced], preferred_element_type=jnp.float32
        )
        return gradient.at[destined].add(product, mode="drop")

    gradient = lax.fori_loop(
        0, turn_count, adjoint_turn, jnp.zeros((block_total, tile_size, slices), jnp.float32)
    )
    gradient = gradient.reshape(-1, slices)
    rows_own = gradient.shape[0] // lax.axis_size("ray")
    update = lax.psum_scatter(gradient, "ray", scatter_dimension=0, tiled=True)
    own_image = lax.dynamic_slice_in_dim(image, lax.axis_index("ray") * rows_own, rows_own)
    image_next = own_image.astype(jnp.float32) + relax_factor * update
    return (residual, image_next)


MESH = pl.DeviceIdType.MESH
NT = (((1,), (1,)), ((), ()))
NN = (((1,), (0,)), ((), ()))
SUB = 16
PARTS = 2


def dot(a, b, dims):
    return lax.dot_general(a, b, dims, preferred_element_type=jnp.float32)


def ordered(a, b):
    return jnp.minimum(a, b), jnp.maximum(a, b)


def sorted_four(a, b, c, d):
    a, b = ordered(a, b)
    c, d = ordered(c, d)
    a, c = ordered(a, c)
    b, d = ordered(b, d)
    b, c = ordered(b, c)
    return a, b, c, d


def median_of_eight(values):
    low = sorted_four(*values[:4])
    high = sorted_four(*values[4:])
    below = [jnp.minimum(low[i], high[3 - i]) for i in range(4)]
    above = [jnp.maximum(low[i], high[3 - i]) for i in range(4)]
    fourth = jnp.maximum(jnp.maximum(below[0], below[1]), jnp.maximum(below[2], below[3]))
    fifth = jnp.minimum(jnp.minimum(above[0], above[1]), jnp.minimum(above[2], above[3]))
    return (fourth + fifth) * 0.5


def step_kernel(
    owners,
    quarters,
    taps_any,
    proj_any,
    image_any,
    library_any,
    entry_any,
    place_any,
    slot_any,
    carried_any,
    count_ref,
    residual_ref,
    next_ref,
    taps_ref,
    proj_ref,
    image_ref,
    library_ref,
    lists_ref,
    carried_own,
    carried_all,
    carried_ref,
    taps_wide,
    rim,
    phase_out,
    phase_in,
    profile_ref,
    fixed,
    counted,
    spread_ref,
    matrix,
    partial_out,
    partial_in,
    same_ref,
    back_out,
    back_in,
    rest_out,
    rest_in,
    stripe_own,
    stripe_far,
    twin_in,
    forward,
    gathered,
    own_update,
    update_out,
    update_in,
    load_sem,
    halo_send,
    halo_recv,
    carried_send,
    carried_recv,
    phase_send,
    phase_recv,
    partial_send,
    partial_recv,
    back_send,
    back_recv,
    rest_send,
    rest_recv,
    stripe_send,
    stripe_recv,
    twin_send,
    twin_recv,
    update_send,
    update_recv,
):
    f32, bf16 = jnp.float32, jnp.bfloat16
    me, ray = lax.axis_index("dom"), lax.axis_index("ray")
    slices, columns = proj_ref.shape
    entries, tile = library_ref.shape[0], library_ref.shape[-1]
    places = image_ref.shape[1] // tile
    count = columns // tile
    ring = count + 1
    inner = count - 2
    per = slices // owners
    side = owners // 2
    half = tile // 2
    share = places * tile // quarters
    rows_half = side * per
    some = owners // PARTS

    group, spot = me // side, lax.rem(me, side)

    def dom_peer(k):
        if k >= side:
            return (1 - group) * side + lax.rem(spot + k - side, side)
        return group * side + lax.rem(spot + k, side)

    dom_order = list(range(1, owners))

    chip, core = ray // 2, lax.rem(ray, 2)

    def ray_twin(k):
        chip_to = 1 - chip if k >= 2 else chip
        core_to = 1 - core if k % 2 else core
        return chip_to * 2 + core_to

    def ray_next(k):
        return lax.rem(ray + k, quarters)

    barrier = pltpu.get_barrier_semaphore()
    for k in range(1, owners):
        pl.semaphore_signal(barrier, inc=1, device_id=(dom_peer(k), ray), device_id_type=MESH)
    for k in range(1, quarters):
        pl.semaphore_signal(barrier, inc=1, device_id=(me, ray_next(k)), device_id_type=MESH)

    pairs = [
        (proj_any.at[0], proj_ref, 0),
        (taps_any, taps_ref, 1),
        (carried_any, carried_own, 2),
        (entry_any, lists_ref.at[0], 3),
        (place_any, lists_ref.at[1], 3),
        (slot_any, lists_ref.at[2], 3),
        (library_any.at[0, 0], library_ref, 4),
        (image_any, image_ref, 5),
    ]
    for src, dst, i in pairs:
        pltpu.make_async_copy(src, dst, load_sem.at[i]).start()

    def await_bytes(ref, sem):
        pltpu.make_async_copy(ref, ref, sem).wait()

    def dom_copy(src, dst, send, recv, k):
        pltpu.make_async_remote_copy(
            src_ref=src,
            dst_ref=dst,
            send_sem=send,
            recv_sem=recv,
            device_id=(dom_peer(k), ray),
            device_id_type=MESH,
        ).start()

    def ray_copy(src, dst, send, recv, peer):
        pltpu.make_async_remote_copy(
            src_ref=src,
            dst_ref=dst,
            send_sem=send,
            recv_sem=recv,
            device_id=(me, peer),
            device_id_type=MESH,
        ).start()

    def block(b):
        return proj_ref[:, b * tile : (b + 1) * tile]

    await_bytes(taps_ref, load_sem.at[1])
    taps_wide[...] = jnp.zeros(taps_wide.shape, f32)
    taps_wide[:, : taps_ref.shape[0]] = taps_ref[...].astype(f32)[None]
    spread = jnp.broadcast_to(taps_wide[...], (tile, taps_wide.shape[1]))
    weights = pltpu.roll(spread, half, 1, stride=1, stride_axis=0).astype(bf16)
    await_bytes(proj_ref, load_sem.at[0])
    two = jnp.concatenate(
        [proj_ref[:, (b - 1) * tile : (b + 1) * tile] for b in range(1, count - 1)], axis=0
    )
    third = jnp.concatenate([block(b + 1) for b in range(1, count - 1)], axis=0)
    phase = dot(two, weights[:, : 2 * tile], NT) + dot(third, weights[:, 2 * tile :], NT)
    phase = phase.reshape(inner, owners, per, tile)
    for owner in range(owners):
        phase_out[owner, :inner] = phase[:, owner].astype(bf16)

    await_bytes(carried_own, load_sem.at[2])
    pl.semaphore_wait(barrier, owners + quarters - 2)

    for k in dom_order:
        dom_copy(carried_own, carried_all.at[me], carried_send.at[0], carried_recv.at[0], k)
    ray_copy(
        proj_ref.at[:, pl.ds(columns - tile, tile)],
        rim.at[0],
        halo_send.at[0],
        halo_recv.at[0],
        ray_next(1),
    )
    ray_copy(
        proj_ref.at[:, pl.ds(0, tile)],
        rim.at[1],
        halo_send.at[0],
        halo_recv.at[0],
        ray_next(quarters - 1),
    )
    for k in dom_order:
        dom_copy(
            phase_out.at[dom_peer(k), pl.ds(0, inner)],
            phase_in.at[me, pl.ds(0, inner)],
            phase_send.at[0],
            phase_recv.at[0],
            k,
        )

    await_bytes(lists_ref, load_sem.at[3])
    capacity = lists_ref.shape[2]
    entry, place, slot = lists_ref[0], lists_ref[1], lists_ref[2]
    alive = lax.broadcasted_iota(jnp.int32, (1, capacity), 1) < count_ref[0, 0]
    code = jnp.where(alive, slot * places + place, -1)
    pick = jnp.where(
        lax.broadcasted_iota(jnp.int32, (owners * places, capacity), 0) == code, 1.0, 0.0
    ).astype(bf16)
    which = jnp.where(
        lax.broadcasted_iota(jnp.int32, (entries * SUB, capacity), 0) // SUB == entry,
        1.0,
        0.0,
    ).astype(bf16)
    counted[...] = dot(pick, which, NT)
    diagonal = lax.rem(
        lax.broadcasted_iota(jnp.int32, (SUB, entries * SUB), 1), SUB
    ) == lax.broadcasted_iota(jnp.int32, (SUB, entries * SUB), 0)

    def widen(step, carry):
        for i in range(8):
            at = step * 8 + i
            row = jnp.broadcast_to(counted[pl.ds(at, 1), :], (SUB, entries * SUB))
            start = pl.multiple_of(at * SUB, SUB)
            spread_ref[pl.ds(start, SUB), :] = jnp.where(diagonal, row, 0.0).astype(bf16)
        return carry

    lax.fori_loop(0, owners * places // 8, widen, 0)

    await_bytes(library_ref, load_sem.at[4])

    def build(step, carry):
        first = pl.multiple_of(step * 2 * SUB, 2 * SUB)
        right = jnp.concatenate(
            [
                library_ref[:, pl.ds(first + i * SUB, SUB), :].reshape(entries * SUB, tile)
                for i in range(2)
            ],
            axis=1,
        )
        for owner in range(owners):
            rows = places * SUB
            made = dot(spread_ref[owner * rows : (owner + 1) * rows, :], right, NN)
            for place in range(places):
                for i in range(2):
                    start = pl.multiple_of(first + owner * tile + i * SUB, SUB)
                    matrix[pl.ds(start, SUB), place * tile : (place + 1) * tile] = made[
                        place * SUB : (place + 1) * SUB, i * tile : (i + 1) * tile
                    ].astype(bf16)
        return carry

    lax.fori_loop(0, tile // (2 * SUB), build, 0)

    await_bytes(rim, halo_recv.at[0])

    @pl.when(ray == 0)
    def _():
        rim[0] = jnp.zeros((slices, tile), bf16)

    @pl.when(ray == quarters - 1)
    def _():
        rim[1] = jnp.zeros((slices, tile), bf16)

    before, after = rim[0], rim[1]
    two = jnp.concatenate(
        [
            proj_ref[:, (count - 2) * tile : count * tile],
            jnp.concatenate([block(count - 1), after], axis=1),
            jnp.concatenate([before, block(0)], axis=1),
            jnp.concatenate([before, before], axis=1),
        ],
        axis=0,
    )
    third = jnp.concatenate([after, after, block(1), block(0)], axis=0)
    edge = dot(two, weights[:, : 2 * tile], NT) + dot(third, weights[:, 2 * tile :], NT)
    edge = edge.reshape(4, owners, per, tile)
    lane = lax.broadcasted_iota(jnp.int32, (owners, per, tile), 2)
    phase_out[:, inner] = edge[0].astype(bf16)
    phase_out[:, inner + 1] = jnp.where(lane < half, edge[1], edge[3]).astype(bf16)
    phase_out[:, inner + 2] = edge[2].astype(bf16)
    for k in dom_order:
        dom_copy(
            phase_out.at[dom_peer(k), pl.ds(inner, 3)],
            phase_in.at[me, pl.ds(inner, 3)],
            phase_send.at[1],
            phase_recv.at[1],
            k,
        )
    phase_in[me] = phase_out[me]

    await_bytes(image_ref, load_sem.at[5])
    for part in range(PARTS):
        for owner in range(part * some, (part + 1) * some, 2):
            made = dot(image_ref[...], matrix[owner * tile : (owner + 2) * tile, :], NT)
            for i in range(2):
                partial_out[:, owner + i] = (
                    made[:, i * tile : (i + 1) * tile].reshape(owners, per, tile).astype(bf16)
                )
        chosen = pl.ds(part * some, some)
        for k in dom_order:
            dom_copy(
                partial_out.at[dom_peer(k), chosen],
                partial_in.at[me, chosen],
                partial_send.at[0],
                partial_recv.at[part],
                k,
            )
    partial_in[me] = partial_out[me]

    carried_all[me] = carried_own[...]
    await_bytes(carried_all.at[pl.ds(0, owners - 1)], carried_recv.at[0])
    to_scalar = pltpu.make_async_copy(carried_all, carried_ref, load_sem.at[6])
    to_scalar.start()
    to_scalar.wait()
    duos = [(a, b) for a in range(owners) for b in range(a + 1, owners)]

    def compare(owner, carry):
        for i, (a, b) in enumerate(duos):
            same = jnp.where(carried_ref[owner, 0, a] == carried_ref[owner, 0, b], 1.0, 0.0)
            same_ref[owner, i : i + 1, :] = jnp.full((1, tile), same, f32)
        return carry

    lax.fori_loop(0, owners, compare, 0)

    def profile_of(i):
        return median_of_eight([phase_in[a, i].astype(f32) for a in range(owners)])

    others = pl.ds(0, owners - 1)
    await_bytes(phase_in.at[others, pl.ds(0, inner)], phase_recv.at[0])
    for i in range(inner):
        profile_ref[:, i * tile : (i + 1) * tile] = profile_of(i)
    await_bytes(phase_in.at[others, pl.ds(inner, 3)], phase_recv.at[1])
    for i in range(inner, ring):
        profile_ref[:, i * tile : (i + 1) * tile] = profile_of(i)

    width = ring * tile
    detector = quarters * columns
    at = lax.broadcasted_iota(jnp.int32, (1, width), 1)
    position = ray * columns + jnp.where(at < count * tile - half, at + tile, at - columns)
    profile = jnp.where((position >= 0) & (position < detector), profile_ref[...], 0.0)
    run = profile
    reach = 1
    while reach < 2 * SMOOTH:
        run = run + pltpu.roll(run, reach, 1)
        reach *= 2
    window = pltpu.roll(run, width - (SMOOTH - 1), 1) + pltpu.roll(profile, width - SMOOTH, 1)
    in_range = (
        jnp.minimum(position + SMOOTH, detector - 1) - jnp.maximum(position - SMOOTH, 0) + 1
    ).astype(f32)
    stripe = (profile - window / in_range).astype(bf16).astype(f32)
    for b in range(count):
        i = (b - 1) % ring
        stripe_own[b] = stripe[:, i * tile : (i + 1) * tile].astype(bf16)
    for a in range(owners):
        for i in range(ring):
            if i != count - 1:
                fixed[a, i] = (
                    (phase_in[a, i].astype(f32) - stripe[:, i * tile : (i + 1) * tile])
                    .astype(bf16)
                    .astype(f32)
                )

    def ring_spot(b):
        return jnp.where(b == 0, ring - 1, b - 1)

    def carry_back(owner, carry):
        part = [partial_in[d, owner].astype(f32) for d in range(owners)]
        total = list(part)
        for i, (a, b) in enumerate(duos):
            same = jnp.broadcast_to(same_ref[owner, i : i + 1, :], (per, tile))
            total[a] = total[a] + same * part[b]
            total[b] = total[b] + same * part[a]
        for d in range(owners):
            back_out[d, owner] = (
                fixed[owner, ring_spot(carried_ref[owner, 0, d])] - total[d]
            ).astype(bf16)
        return carry

    for part in range(PARTS):
        chosen = pl.ds(part * some, some)
        await_bytes(partial_in.at[others, chosen], partial_recv.at[part])
        lax.fori_loop(part * some, (part + 1) * some, carry_back, 0)
        for k in dom_order:
            dom_copy(
                back_out.at[dom_peer(k), chosen],
                back_in.at[me, chosen],
                back_send.at[0],
                back_recv.at[part * 2 + k // side],
                k,
            )
    back_in[me] = back_out[me]

    dom_copy(stripe_own, stripe_far.at[spot], stripe_send.at[0], stripe_recv.at[0], side)
    for k in dom_order:
        dom_copy(
            partial_out.at[pl.ds((1 - dom_peer(k) // side) * side, side), dom_peer(k)],
            twin_in.at[me],
            twin_send.at[0],
            twin_recv.at[0],
            k,
        )
    twin_in[me] = partial_out[pl.ds((1 - group) * side, side), me]

    def whole(i, carry):
        owner = group * side + i
        part = [partial_in[d, owner].astype(f32) for d in range(owners)]
        where_to = [carried_ref[owner, 0, d] for d in range(owners)]
        for b in range(count):
            total = fixed[owner, (b - 1) % ring]
            taken = jnp.zeros((per, tile), f32)
            for d in range(owners):
                taken = taken + jnp.where(where_to[d] == b, 1.0, 0.0).astype(f32) * part[d]
            rest_out[i, b] = (total - taken).astype(bf16)
        return carry

    lax.fori_loop(0, side, whole, 0)
    for k in range(1, side):
        dom_copy(
            rest_out.at[lax.rem(spot + k, side)],
            rest_in.at[me],
            rest_send.at[0],
            rest_recv.at[0],
            k,
        )
    rest_in[me] = rest_out[spot]

    for turn in range(2):
        held = group if turn == 0 else 1 - group
        first = held * side
        for part in range(PARTS):
            await_bytes(
                back_in.at[pl.ds(0, side - 1 + turn), pl.ds(part * some, some)],
                back_recv.at[part * 2 + turn],
            )
            left = jnp.concatenate(
                [
                    back_in[pl.ds(first, side), owner]
                    .astype(f32)
                    .reshape(rows_half, tile)
                    .astype(bf16)
                    for owner in range(part * some, (part + 1) * some)
                ],
                axis=1,
            )
            rows = slice(part * some * tile, (part + 1) * some * tile)
            for k in (2, 3, 1, 0):
                start = pl.multiple_of(ray_twin(k) * share, share)
                made = dot(left, matrix[rows, pl.ds(start, share)], NN)
                if part > 0:
                    made = made + gathered[k]
                if part < PARTS - 1:
                    gathered[k] = made
                elif k == 0:
                    own_update[turn] = made
                else:
                    update_out[turn, k] = made.astype(bf16)
                    ray_copy(
                        update_out.at[turn, k],
                        update_in.at[turn, k],
                        update_send.at[0],
                        update_recv.at[turn],
                        ray_twin(k),
                    )

    await_bytes(stripe_own, stripe_recv.at[0])
    for k in range(1, side):
        dom_copy(
            stripe_far.at[spot], stripe_far.at[spot], stripe_send.at[0], stripe_recv.at[1], k
        )

    await_bytes(twin_in.at[others], twin_recv.at[0])
    other = pl.ds((1 - group) * side, side)
    own_spots = [carried_ref[me, 0, d] for d in range(owners)]
    taken_by = [twin_in[d].astype(f32) for d in range(owners)]
    for b in range(count):
        taken = jnp.zeros((side, per, tile), f32)
        for d in range(owners):
            taken = taken + jnp.where(own_spots[d] == b, 1.0, 0.0).astype(f32) * taken_by[d]
        forward[b] = taken
    await_bytes(stripe_far.at[pl.ds(0, side - 1)], stripe_recv.at[1])
    for b in range(count):
        clean = (
            (phase_out[other, (b - 1) % ring].astype(f32) - stripe_far[:, b].astype(f32))
            .astype(bf16)
            .astype(f32)
        )
        rest_in[other, b] = (clean - forward[b]).astype(bf16)
    await_bytes(rest_in.at[pl.ds(0, side - 1)], rest_recv.at[0])
    for b in range(count):
        residual_ref[:, b * tile : (b + 1) * tile] = (
            rest_in[:, b].astype(f32).reshape(slices, tile).astype(bf16)
        )

    for turn in range(2):
        held = group if turn == 0 else 1 - group
        await_bytes(update_in.at[turn, pl.ds(1, quarters - 1)], update_recv.at[turn])
        amount = own_update[turn]
        for k in range(1, quarters):
            amount = amount + update_in[turn, k].astype(f32)
        rows = pl.ds(pl.multiple_of(held * rows_half, rows_half), rows_half)
        old = image_ref[rows, pl.ds(pl.multiple_of(ray * share, share), share)].astype(f32)
        next_ref[rows, :] = old + relax_factor * amount
    await_bytes(carried_all.at[others], carried_send.at[0])
    await_bytes(rim, halo_send.at[0])
    await_bytes(phase_out.at[others, pl.ds(0, inner)], phase_send.at[0])
    await_bytes(phase_out.at[others, pl.ds(inner, 3)], phase_send.at[1])
    await_bytes(partial_out.at[others], partial_send.at[0])
    await_bytes(back_out.at[others], back_send.at[0])
    await_bytes(twin_in.at[others], twin_send.at[0])
    await_bytes(rest_out.at[pl.ds(0, side - 1)], rest_send.at[0])
    await_bytes(stripe_far, stripe_send.at[0])
    await_bytes(update_out.at[:, pl.ds(1, quarters - 1)], update_send.at[0])


def store_kernel(residual_ref, next_ref, residual_out, next_out, sem):
    copies = [
        pltpu.make_async_copy(residual_ref, residual_out, sem.at[0]),
        pltpu.make_async_copy(next_ref, next_out, sem.at[1]),
    ]
    for copy in copies:
        copy.start()
    for copy in copies:
        copy.wait()


def fast_shards(
    projections,
    phase_kernel,
    image,
    tile_library,
    tile_entry,
    tile_image,
    tile_slot,
    tile_count,
    slot_block,
):
    f32, bf16 = jnp.float32, jnp.bfloat16
    i32 = jnp.int32
    owners, quarters = lax.axis_size("dom"), lax.axis_size("ray")
    entries, tile = tile_library.shape[2], tile_library.shape[-1]
    _, slices, columns = projections.shape
    count = columns // tile
    ring = count + 1
    places = image.shape[0] // tile
    per = slices // owners
    capacity = tile_entry.shape[2]
    share = places * tile // quarters
    rows_half = slices // 2
    hbm = pl.BlockSpec(memory_space=pltpu.HBM)
    vmem = pl.BlockSpec(memory_space=pltpu.VMEM)
    sems = pltpu.SemaphoreType.DMA
    residual, image_next = pl.pallas_call(
        functools.partial(step_kernel, owners, quarters),
        out_shape=(
            jax.ShapeDtypeStruct((slices, columns), bf16),
            jax.ShapeDtypeStruct((slices, share), f32),
        ),
        in_specs=[hbm] * 8 + [pl.BlockSpec(memory_space=pltpu.SMEM)],
        out_specs=(vmem, vmem),
        scratch_shapes=[
            pltpu.VMEM(phase_kernel.shape, bf16),
            pltpu.VMEM((slices, columns), bf16),
            pltpu.VMEM((slices, places * tile), bf16),
            pltpu.VMEM((entries, tile, tile), bf16),
            pltpu.VMEM((3, 1, capacity), i32),
            pltpu.VMEM((1, owners), i32),
            pltpu.VMEM((owners, 1, owners), i32),
            pltpu.SMEM((owners, 1, owners), i32),
            pltpu.VMEM((1, 3 * tile), f32),
            pltpu.VMEM((2, slices, tile), bf16),
            pltpu.VMEM((owners, ring, per, tile), bf16),
            pltpu.VMEM((owners, ring, per, tile), bf16),
            pltpu.VMEM((per, ring * tile), f32),
            pltpu.VMEM((owners, ring, per, tile), f32),
            pltpu.VMEM((owners * places, entries * SUB), f32),
            pltpu.VMEM((owners * places * SUB, entries * SUB), bf16),
            pltpu.VMEM((owners * tile, places * tile), bf16),
            pltpu.VMEM((owners, owners, per, tile), bf16),
            pltpu.VMEM((owners, owners, per, tile), bf16),
            pltpu.VMEM((owners, 32, tile), f32),
            pltpu.VMEM((owners, owners, per, tile), bf16),
            pltpu.VMEM((owners, owners, per, tile), bf16),
            pltpu.VMEM((owners // 2, count, per, tile), bf16),
            pltpu.VMEM((owners, count, per, tile), bf16),
            pltpu.VMEM((count, per, tile), bf16),
            pltpu.VMEM((owners // 2, count, per, tile), bf16),
            pltpu.VMEM((owners, owners // 2, per, tile), bf16),
            pltpu.VMEM((count, owners // 2, per, tile), f32),
            pltpu.VMEM((quarters, rows_half, share), f32),
            pltpu.VMEM((2, rows_half, share), f32),
            pltpu.VMEM((2, quarters, rows_half, share), bf16),
            pltpu.VMEM((2, quarters, rows_half, share), bf16),
            sems((7,)),
            sems((1,)),
            sems((1,)),
            sems((1,)),
            sems((1,)),
            sems((2,)),
            sems((2,)),
            sems((1,)),
            sems((PARTS,)),
            sems((1,)),
            sems((2 * PARTS,)),
            sems((1,)),
            sems((1,)),
            sems((1,)),
            sems((2,)),
            sems((1,)),
            sems((1,)),
            sems((1,)),
            sems((2,)),
        ],
        compiler_params=pltpu.CompilerParams(
            collective_id=0, has_side_effects=True, vmem_limit_bytes=48 * 1024 * 1024
        ),
    )(
        *[
            pltpu.with_memory_space_constraint(x, pltpu.HBM)
            for x in (
                phase_kernel,
                projections,
                image.T,
                tile_library,
                tile_entry[0],
                tile_image[0],
                tile_slot[0],
                slot_block[0],
            )
        ],
        tile_count,
    )
    residual, image_next = pl.pallas_call(
        store_kernel,
        out_shape=(
            jax.ShapeDtypeStruct(residual.shape, bf16),
            jax.ShapeDtypeStruct(image_next.shape, f32),
        ),
        in_specs=[pl.BlockSpec(memory_space=pl.ANY)] * 2,
        out_specs=[pl.BlockSpec(memory_space=pl.ANY)] * 2,
        scratch_shapes=[sems((2,))],
    )(
        pltpu.with_memory_space_constraint(residual, pltpu.VMEM),
        pltpu.with_memory_space_constraint(image_next, pltpu.VMEM),
    )
    return residual[None], image_next.T


def fits_kernel(projections, phase_kernel, image, tile_library, tile_entry, *rest):
    owners, quarters = lax.axis_size("dom"), lax.axis_size("ray")
    tile = tile_library.shape[-1]
    angles, slices, columns = projections.shape
    return (
        angles == 1
        and slices % 16 == 0
        and slices == 8 * owners
        and owners == 8
        and tile == 128
        and phase_kernel.shape[0] == tile + 1
        and columns % tile == 0
        and tile_library.shape[2] == 16
        and quarters == 4
        and image.shape[0] == 16 * tile
        and tile_entry.shape[2] <= 256
    )


def any_shards(*args):
    if fits_kernel(*args):
        return fast_shards(*args)
    return shards(*args)


def solution(mesh):
    return jax.shard_map(
        any_shards,
        mesh=mesh,
        in_specs=(
            P("dom", None, "ray"),
            P(),
            P("dom", None),
            P("dom", "ray", None, None, None),
            P("dom", "ray", None),
            P("dom", "ray", None),
            P("dom", "ray", None),
            P("dom", "ray"),
            P("dom", "ray", None),
        ),
        out_specs=(P("dom", None, "ray"), P(("dom", "ray"), None)),
        check_vma=False,
    )
```

```python
import functools

import jax
import jax.numpy as jnp
from jax import lax
from jax.experimental import pallas as pl
from jax.experimental.pallas import tpu as pltpu
from jax.sharding import PartitionSpec as P

SMOOTH = 8


relax_factor = 0.25


def with_halo(cells, sides, width):
    for axis, dim in sides:
        count = lax.axis_size(axis)
        ends = count - 1
        head = lax.slice_in_dim(cells, 0, width, axis=dim)
        tail = lax.slice_in_dim(cells, cells.shape[dim] - width, cells.shape[dim], axis=dim)
        cells = jnp.concatenate(
            [
                lax.ppermute(tail, axis, [(i, (i + 1) % count) for i in range(ends)]),
                cells,
                lax.ppermute(head, axis, [((i + 1) % count, i) for i in range(ends)]),
            ],
            axis=dim,
        )
    return cells


def toeplitz(kernel, tile_size):
    taps = kernel.shape[0]
    padded = jnp.concatenate([kernel, jnp.zeros((2 * tile_size + 1 - taps,), kernel.dtype)])
    tiled = jnp.tile(padded, tile_size)[: 2 * tile_size * tile_size]
    return tiled.reshape(tile_size, 2 * tile_size).T


def phase_filter(projections, phase_kernel, tile_size):
    half_width = (phase_kernel.shape[0] - 1) // 2
    angles, slices, columns = projections.shape
    block_count = columns // tile_size
    rimmed = with_halo(projections, (("ray", 2),), half_width)
    padded = jnp.pad(rimmed, ((0, 0), (0, 0), (0, 2 * tile_size - 2 * half_width)))
    blocks = padded.reshape(angles, slices, block_count + 2, tile_size)
    windows = jnp.concatenate(
        [blocks[:, :, :block_count], blocks[:, :, 1 : block_count + 1]], axis=-1
    )
    filtered = jnp.einsum(
        "asbi,ij->asbj",
        windows,
        toeplitz(phase_kernel, tile_size),
        preferred_element_type=jnp.float32,
    )
    return filtered.reshape(angles, slices, columns).astype(jnp.bfloat16)


def stripe_profile(gathered):
    profile = jnp.median(gathered.astype(jnp.float32), axis=0)
    columns = profile.shape[1]
    rimmed = with_halo(profile, (("ray", 1),), SMOOTH)
    window_sum = jnp.zeros_like(profile)
    for offset in range(2 * SMOOTH + 1):
        window_sum = window_sum + rimmed[:, offset : offset + columns]
    position = lax.axis_index("ray") * columns + jnp.arange(columns)
    detector = lax.axis_size("ray") * columns
    in_range = (
        jnp.minimum(position + SMOOTH, detector - 1) - jnp.maximum(position - SMOOTH, 0) + 1
    ).astype(jnp.float32)
    return (profile - window_sum / in_range).astype(jnp.bfloat16)


def shards(
    projections,
    phase_kernel,
    image,
    tile_library,
    tile_entry,
    tile_image,
    tile_slot,
    tile_count,
    slot_block,
):
    tile_size = tile_library.shape[-1]
    angles, slices, columns = projections.shape
    phase = phase_filter(projections, phase_kernel, tile_size)
    gathered = lax.all_to_all(phase, "dom", split_axis=1, concat_axis=0, tiled=True)
    stripe = stripe_profile(gathered)
    fixed_rows = (gathered.astype(jnp.float32) - stripe.astype(jnp.float32)[None]).astype(
        jnp.bfloat16
    )
    corrected = lax.all_to_all(fixed_rows, "dom", split_axis=0, concat_axis=1, tiled=True)
    owners = lax.axis_size("dom")
    library = tile_library[0, 0]
    entries = tile_entry[0, 0]
    images = tile_image[0, 0]
    slots = tile_slot[0, 0]
    capacity = entries.shape[0]
    block_size = 64
    turn_count = capacity // block_size
    image_blocks = image.reshape(-1, tile_size, slices)
    block_total = image_blocks.shape[0]
    live_mask = jnp.arange(capacity) < tile_count[0, 0]
    slot_target = jnp.where(live_mask, slots, owners)
    image_target = jnp.where(live_mask, images, block_total)

    def forward_turn(turn_index, partial_value):
        first_tile = turn_index * block_size
        chosen = lax.dynamic_slice_in_dim(entries, first_tile, block_size)
        placed = lax.dynamic_slice_in_dim(images, first_tile, block_size)
        destined = lax.dynamic_slice_in_dim(slot_target, first_tile, block_size)
        product = jnp.einsum(
            "krp,kps->ksr",
            library[chosen],
            image_blocks[placed],
            preferred_element_type=jnp.float32,
        )
        return partial_value.at[destined].add(product, mode="drop")

    partial_value = lax.fori_loop(
        0, turn_count, forward_turn, jnp.zeros((owners, slices, tile_size), jnp.float32)
    )
    received = lax.all_to_all(
        partial_value.astype(jnp.bfloat16), "dom", split_axis=0, concat_axis=0, tiled=True
    )
    per_owner = columns // tile_size
    carried = slot_block[0, 0]
    block_ids = jnp.arange(angles * per_owner).reshape(angles, per_owner)
    selector = (block_ids[:, :, None] == carried[None, None, :]).astype(jnp.bfloat16)
    forward = jnp.einsum("abd,dst->asbt", selector, received, preferred_element_type=jnp.float32)
    residual = (corrected.astype(jnp.float32) - forward.reshape(angles, slices, columns)).astype(
        jnp.bfloat16
    )
    back = jnp.einsum(
        "abd,asbt->dst",
        selector,
        residual.reshape(angles, slices, per_owner, tile_size),
        preferred_element_type=jnp.float32,
    ).astype(jnp.bfloat16)
    returned = lax.all_to_all(back, "dom", split_axis=0, concat_axis=0, tiled=True)

    def adjoint_turn(turn_index, gradient):
        first_tile = turn_index * block_size
        chosen = lax.dynamic_slice_in_dim(entries, first_tile, block_size)
        sourced = lax.dynamic_slice_in_dim(slots, first_tile, block_size)
        destined = lax.dynamic_slice_in_dim(image_target, first_tile, block_size)
        product = jnp.einsum(
            "krp,ksr->kps", library[chosen], returned[sourced], preferred_element_type=jnp.float32
        )
        return gradient.at[destined].add(product, mode="drop")

    gradient = lax.fori_loop(
        0, turn_count, adjoint_turn, jnp.zeros((block_total, tile_size, slices), jnp.float32)
    )
    gradient = gradient.reshape(-1, slices)
    rows_own = gradient.shape[0] // lax.axis_size("ray")
    update = lax.psum_scatter(gradient, "ray", scatter_dimension=0, tiled=True)
    own_image = lax.dynamic_slice_in_dim(image, lax.axis_index("ray") * rows_own, rows_own)
    image_next = own_image.astype(jnp.float32) + relax_factor * update
    return (residual, image_next)


MESH = pl.DeviceIdType.MESH
NT = (((1,), (1,)), ((), ()))
NN = (((1,), (0,)), ((), ()))
SUB = 16
PARTS = 4


def dot(a, b, dims):
    return lax.dot_general(a, b, dims, preferred_element_type=jnp.float32)


def ordered(a, b):
    return jnp.minimum(a, b), jnp.maximum(a, b)


def sorted_four(a, b, c, d):
    a, b = ordered(a, b)
    c, d = ordered(c, d)
    a, c = ordered(a, c)
    b, d = ordered(b, d)
    b, c = ordered(b, c)
    return a, b, c, d


def median_of_eight(values):
    low = sorted_four(*values[:4])
    high = sorted_four(*values[4:])
    below = [jnp.minimum(low[i], high[3 - i]) for i in range(4)]
    above = [jnp.maximum(low[i], high[3 - i]) for i in range(4)]
    fourth = jnp.maximum(jnp.maximum(below[0], below[1]), jnp.maximum(below[2], below[3]))
    fifth = jnp.minimum(jnp.minimum(above[0], above[1]), jnp.minimum(above[2], above[3]))
    return (fourth + fifth) * 0.5


def step_kernel(
    owners,
    quarters,
    taps_any,
    proj_any,
    image_any,
    library_any,
    entry_any,
    place_any,
    slot_any,
    carried_any,
    count_ref,
    residual_ref,
    next_ref,
    taps_ref,
    proj_ref,
    image_ref,
    library_ref,
    lists_ref,
    carried_own,
    carried_all,
    carried_ref,
    taps_wide,
    rim,
    phase_out,
    phase_in,
    profile_ref,
    fixed,
    counted,
    spread_ref,
    matrix,
    partial_out,
    partial_in,
    same_ref,
    back_out,
    back_in,
    rest_out,
    rest_in,
    stripe_own,
    stripe_far,
    twin_in,
    forward,
    gathered,
    own_update,
    update_out,
    update_in,
    load_sem,
    halo_send,
    halo_recv,
    carried_send,
    carried_recv,
    phase_send,
    phase_recv,
    partial_send,
    partial_recv,
    back_send,
    back_recv,
    rest_send,
    rest_recv,
    stripe_send,
    stripe_recv,
    twin_send,
    twin_recv,
    update_send,
    update_recv,
):
    f32, bf16 = jnp.float32, jnp.bfloat16
    me, ray = lax.axis_index("dom"), lax.axis_index("ray")
    slices, columns = proj_ref.shape
    entries, tile = library_ref.shape[0], library_ref.shape[-1]
    places = image_ref.shape[1] // tile
    count = columns // tile
    ring = count + 1
    inner = count - 2
    per = slices // owners
    side = owners // 2
    half = tile // 2
    share = places * tile // quarters
    rows_half = side * per
    some = owners // PARTS

    group, spot = me // side, lax.rem(me, side)

    def dom_peer(k):
        if k >= side:
            return (1 - group) * side + lax.rem(spot + k - side, side)
        return group * side + lax.rem(spot + k, side)

    dom_order = list(range(1, owners))

    chip, core = ray // 2, lax.rem(ray, 2)

    def ray_twin(k):
        chip_to = 1 - chip if k >= 2 else chip
        core_to = 1 - core if k % 2 else core
        return chip_to * 2 + core_to

    def ray_next(k):
        return lax.rem(ray + k, quarters)

    barrier = pltpu.get_barrier_semaphore()
    for k in range(1, owners):
        pl.semaphore_signal(barrier, inc=1, device_id=(dom_peer(k), ray), device_id_type=MESH)
    for k in range(1, quarters):
        pl.semaphore_signal(barrier, inc=1, device_id=(me, ray_next(k)), device_id_type=MESH)

    pairs = [
        (proj_any.at[0], proj_ref, 0),
        (taps_any, taps_ref, 1),
        (carried_any, carried_own, 2),
        (entry_any, lists_ref.at[0], 3),
        (place_any, lists_ref.at[1], 3),
        (slot_any, lists_ref.at[2], 3),
        (library_any.at[0, 0], library_ref, 4),
        (image_any, image_ref, 5),
    ]
    for src, dst, i in pairs:
        pltpu.make_async_copy(src, dst, load_sem.at[i]).start()

    def await_bytes(ref, sem):
        pltpu.make_async_copy(ref, ref, sem).wait()

    def dom_copy(src, dst, send, recv, k):
        pltpu.make_async_remote_copy(
            src_ref=src,
            dst_ref=dst,
            send_sem=send,
            recv_sem=recv,
            device_id=(dom_peer(k), ray),
            device_id_type=MESH,
        ).start()

    def ray_copy(src, dst, send, recv, peer):
        pltpu.make_async_remote_copy(
            src_ref=src,
            dst_ref=dst,
            send_sem=send,
            recv_sem=recv,
            device_id=(me, peer),
            device_id_type=MESH,
        ).start()

    def block(b):
        return proj_ref[:, b * tile : (b + 1) * tile]

    await_bytes(taps_ref, load_sem.at[1])
    taps_wide[...] = jnp.zeros(taps_wide.shape, f32)
    taps_wide[:, : taps_ref.shape[0]] = taps_ref[...].astype(f32)[None]
    spread = jnp.broadcast_to(taps_wide[...], (tile, taps_wide.shape[1]))
    weights = pltpu.roll(spread, half, 1, stride=1, stride_axis=0).astype(bf16)
    await_bytes(proj_ref, load_sem.at[0])
    two = jnp.concatenate(
        [proj_ref[:, (b - 1) * tile : (b + 1) * tile] for b in range(1, count - 1)], axis=0
    )
    third = jnp.concatenate([block(b + 1) for b in range(1, count - 1)], axis=0)
    phase = dot(two, weights[:, : 2 * tile], NT) + dot(third, weights[:, 2 * tile :], NT)
    phase = phase.reshape(inner, owners, per, tile)
    for owner in range(owners):
        phase_out[owner, :inner] = phase[:, owner].astype(bf16)

    await_bytes(carried_own, load_sem.at[2])
    pl.semaphore_wait(barrier, owners + quarters - 2)

    for k in dom_order:
        dom_copy(carried_own, carried_all.at[me], carried_send.at[0], carried_recv.at[0], k)
    ray_copy(
        proj_ref.at[:, pl.ds(columns - tile, tile)],
        rim.at[0],
        halo_send.at[0],
        halo_recv.at[0],
        ray_next(1),
    )
    ray_copy(
        proj_ref.at[:, pl.ds(0, tile)],
        rim.at[1],
        halo_send.at[0],
        halo_recv.at[0],
        ray_next(quarters - 1),
    )
    for k in dom_order:
        dom_copy(
            phase_out.at[dom_peer(k), pl.ds(0, inner)],
            phase_in.at[me, pl.ds(0, inner)],
            phase_send.at[0],
            phase_recv.at[0],
            k,
        )

    await_bytes(lists_ref, load_sem.at[3])
    capacity = lists_ref.shape[2]
    entry, place, slot = lists_ref[0], lists_ref[1], lists_ref[2]
    alive = lax.broadcasted_iota(jnp.int32, (1, capacity), 1) < count_ref[0, 0]
    code = jnp.where(alive, slot * places + place, -1)
    pick = jnp.where(
        lax.broadcasted_iota(jnp.int32, (owners * places, capacity), 0) == code, 1.0, 0.0
    ).astype(bf16)
    which = jnp.where(
        lax.broadcasted_iota(jnp.int32, (entries * SUB, capacity), 0) // SUB == entry,
        1.0,
        0.0,
    ).astype(bf16)
    counted[...] = dot(pick, which, NT)
    diagonal = lax.rem(
        lax.broadcasted_iota(jnp.int32, (SUB, entries * SUB), 1), SUB
    ) == lax.broadcasted_iota(jnp.int32, (SUB, entries * SUB), 0)

    def widen(step, carry):
        for i in range(8):
            at = step * 8 + i
            row = jnp.broadcast_to(counted[pl.ds(at, 1), :], (SUB, entries * SUB))
            start = pl.multiple_of(at * SUB, SUB)
            spread_ref[pl.ds(start, SUB), :] = jnp.where(diagonal, row, 0.0).astype(bf16)
        return carry

    lax.fori_loop(0, owners * places // 8, widen, 0)

    await_bytes(library_ref, load_sem.at[4])

    def build(step, carry):
        first = pl.multiple_of(step * 2 * SUB, 2 * SUB)
        right = jnp.concatenate(
            [
                library_ref[:, pl.ds(first + i * SUB, SUB), :].reshape(entries * SUB, tile)
                for i in range(2)
            ],
            axis=1,
        )
        for owner in range(owners):
            rows = places * SUB
            made = dot(spread_ref[owner * rows : (owner + 1) * rows, :], right, NN)
            for place in range(places):
                for i in range(2):
                    start = pl.multiple_of(first + owner * tile + i * SUB, SUB)
                    matrix[pl.ds(start, SUB), place * tile : (place + 1) * tile] = made[
                        place * SUB : (place + 1) * SUB, i * tile : (i + 1) * tile
                    ].astype(bf16)
        return carry

    lax.fori_loop(0, tile // (2 * SUB), build, 0)

    await_bytes(rim, halo_recv.at[0])

    @pl.when(ray == 0)
    def _():
        rim[0] = jnp.zeros((slices, tile), bf16)

    @pl.when(ray == quarters - 1)
    def _():
        rim[1] = jnp.zeros((slices, tile), bf16)

    before, after = rim[0], rim[1]
    two = jnp.concatenate(
        [
            proj_ref[:, (count - 2) * tile : count * tile],
            jnp.concatenate([block(count - 1), after], axis=1),
            jnp.concatenate([before, block(0)], axis=1),
            jnp.concatenate([before, before], axis=1),
        ],
        axis=0,
    )
    third = jnp.concatenate([after, after, block(1), block(0)], axis=0)
    edge = dot(two, weights[:, : 2 * tile], NT) + dot(third, weights[:, 2 * tile :], NT)
    edge = edge.reshape(4, owners, per, tile)
    lane = lax.broadcasted_iota(jnp.int32, (owners, per, tile), 2)
    phase_out[:, inner] = edge[0].astype(bf16)
    phase_out[:, inner + 1] = jnp.where(lane < half, edge[1], edge[3]).astype(bf16)
    phase_out[:, inner + 2] = edge[2].astype(bf16)
    for k in dom_order:
        dom_copy(
            phase_out.at[dom_peer(k), pl.ds(inner, 3)],
            phase_in.at[me, pl.ds(inner, 3)],
            phase_send.at[1],
            phase_recv.at[1],
            k,
        )
    phase_in[me] = phase_out[me]

    def send_partials(part):
        chosen = pl.ds(part * some, some)
        for k in dom_order:
            dom_copy(
                partial_out.at[dom_peer(k), chosen],
                partial_in.at[me, chosen],
                partial_send.at[0],
                partial_recv.at[part],
                k,
            )

    def send_all_partials():
        for part in range(PARTS):
            send_partials(part)

    await_bytes(image_ref, load_sem.at[5])
    for part in range(PARTS):
        for owner in range(part * some, (part + 1) * some, 2):
            made = dot(image_ref[...], matrix[owner * tile : (owner + 2) * tile, :], NT)
            for i in range(2):
                partial_out[:, owner + i] = (
                    made[:, i * tile : (i + 1) * tile].reshape(owners, per, tile).astype(bf16)
                )
        pl.when(core == 0)(functools.partial(send_partials, part))
    partial_in[me] = partial_out[me]

    def send_twins():
        for k in dom_order:
            dom_copy(
                partial_out.at[pl.ds((1 - dom_peer(k) // side) * side, side), dom_peer(k)],
                twin_in.at[me],
                twin_send.at[0],
                twin_recv.at[0],
                k,
            )

    twin_in[me] = partial_out[pl.ds((1 - group) * side, side), me]

    carried_all[me] = carried_own[...]
    await_bytes(carried_all.at[pl.ds(0, owners - 1)], carried_recv.at[0])
    to_scalar = pltpu.make_async_copy(carried_all, carried_ref, load_sem.at[6])
    to_scalar.start()
    to_scalar.wait()
    duos = [(a, b) for a in range(owners) for b in range(a + 1, owners)]

    def compare(owner, carry):
        for i, (a, b) in enumerate(duos):
            same = jnp.where(carried_ref[owner, 0, a] == carried_ref[owner, 0, b], 1.0, 0.0)
            same_ref[owner, i : i + 1, :] = jnp.full((1, tile), same, f32)
        return carry

    lax.fori_loop(0, owners, compare, 0)

    def profile_of(i):
        return median_of_eight([phase_in[a, i].astype(f32) for a in range(owners)])

    others = pl.ds(0, owners - 1)
    await_bytes(phase_in.at[others, pl.ds(0, inner)], phase_recv.at[0])
    for i in range(inner):
        profile_ref[:, i * tile : (i + 1) * tile] = profile_of(i)
    await_bytes(phase_in.at[others, pl.ds(inner, 3)], phase_recv.at[1])
    pl.when(core == 1)(send_all_partials)
    for i in range(inner, ring):
        profile_ref[:, i * tile : (i + 1) * tile] = profile_of(i)

    width = ring * tile
    detector = quarters * columns
    at = lax.broadcasted_iota(jnp.int32, (1, width), 1)
    position = ray * columns + jnp.where(at < count * tile - half, at + tile, at - columns)
    profile = jnp.where((position >= 0) & (position < detector), profile_ref[...], 0.0)
    run = profile
    reach = 1
    while reach < 2 * SMOOTH:
        run = run + pltpu.roll(run, reach, 1)
        reach *= 2
    window = pltpu.roll(run, width - (SMOOTH - 1), 1) + pltpu.roll(profile, width - SMOOTH, 1)
    in_range = (
        jnp.minimum(position + SMOOTH, detector - 1) - jnp.maximum(position - SMOOTH, 0) + 1
    ).astype(f32)
    stripe = (profile - window / in_range).astype(bf16).astype(f32)
    for b in range(count):
        i = (b - 1) % ring
        stripe_own[b] = stripe[:, i * tile : (i + 1) * tile].astype(bf16)
    for a in range(owners):
        for i in range(ring):
            if i != count - 1:
                fixed[a, i] = (
                    (phase_in[a, i].astype(f32) - stripe[:, i * tile : (i + 1) * tile])
                    .astype(bf16)
                    .astype(f32)
                )

    def ring_spot(b):
        return jnp.where(b == 0, ring - 1, b - 1)

    def carry_back(owner, carry):
        part = [partial_in[d, owner].astype(f32) for d in range(owners)]
        total = list(part)
        for i, (a, b) in enumerate(duos):
            same = jnp.broadcast_to(same_ref[owner, i : i + 1, :], (per, tile))
            total[a] = total[a] + same * part[b]
            total[b] = total[b] + same * part[a]
        for d in range(owners):
            back_out[d, owner] = (
                fixed[owner, ring_spot(carried_ref[owner, 0, d])] - total[d]
            ).astype(bf16)
        return carry

    for part in range(PARTS):
        chosen = pl.ds(part * some, some)
        await_bytes(partial_in.at[others, chosen], partial_recv.at[part])
        lax.fori_loop(part * some, (part + 1) * some, carry_back, 0)
        for k in dom_order:
            dom_copy(
                back_out.at[dom_peer(k), chosen],
                back_in.at[me, chosen],
                back_send.at[0],
                back_recv.at[part * 2 + k // side],
                k,
            )
    back_in[me] = back_out[me]

    def whole(i, carry):
        owner = group * side + i
        part = [partial_in[d, owner].astype(f32) for d in range(owners)]
        where_to = [carried_ref[owner, 0, d] for d in range(owners)]
        for b in range(count):
            total = fixed[owner, (b - 1) % ring]
            taken = jnp.zeros((per, tile), f32)
            for d in range(owners):
                taken = taken + jnp.where(where_to[d] == b, 1.0, 0.0).astype(f32) * part[d]
            rest_out[i, b] = (total - taken).astype(bf16)
        return carry

    lax.fori_loop(0, side, whole, 0)
    dom_copy(stripe_own, stripe_far.at[spot], stripe_send.at[0], stripe_recv.at[0], side)
    rest_in[me] = rest_out[spot]

    def rows_of(turn, part):
        first = (group if turn == 0 else 1 - group) * side
        return jnp.concatenate(
            [
                back_in[pl.ds(first, side), owner]
                .astype(f32)
                .reshape(rows_half, tile)
                .astype(bf16)
                for owner in range(part * some, (part + 1) * some)
            ],
            axis=1,
        )

    def send_update(turn, k, sem):
        ray_copy(
            update_out.at[turn, k],
            update_in.at[turn, k],
            update_send.at[0],
            update_recv.at[sem],
            ray_twin(k),
        )

    for turn in range(2):
        for part in range(PARTS):
            await_bytes(
                back_in.at[pl.ds(0, side - 1 + turn), pl.ds(part * some, some)],
                back_recv.at[part * 2 + turn],
            )
            left = rows_of(turn, part)
            rows = slice(part * some * tile, (part + 1) * some * tile)
            for k in (2, 3):
                start = pl.multiple_of(ray_twin(k) * share, share)
                made = dot(left, matrix[rows, pl.ds(start, share)], NN)
                if part > 0:
                    made = made + gathered[k - 2]
                if part < PARTS - 1:
                    gathered[k - 2] = made
                else:
                    update_out[turn, k] = made.astype(bf16)
                    send_update(turn, k, turn)
        if turn == 0:
            send_twins()
            for k in range(1, side):
                dom_copy(
                    rest_out.at[lax.rem(spot + k, side)],
                    rest_in.at[me],
                    rest_send.at[0],
                    rest_recv.at[0],
                    k,
                )

    left = jnp.concatenate(
        [
            jnp.concatenate([rows_of(turn, part) for part in range(PARTS)], axis=1)
            for turn in range(2)
        ],
        axis=0,
    )
    start = pl.multiple_of(ray_twin(1) * share, share)
    made = dot(left, matrix[:, pl.ds(start, share)], NN).reshape(2, rows_half, share)
    update_out[:, 1] = made.astype(bf16)
    for turn in range(2):
        send_update(turn, 1, 2)

    await_bytes(stripe_own, stripe_recv.at[0])
    for k in range(1, side):
        dom_copy(
            stripe_far.at[spot], stripe_far.at[spot], stripe_send.at[0], stripe_recv.at[1], k
        )

    start = pl.multiple_of(ray * share, share)
    own_update[...] = dot(left, matrix[:, pl.ds(start, share)], NN).reshape(2, rows_half, share)

    await_bytes(twin_in.at[others], twin_recv.at[0])
    other = pl.ds((1 - group) * side, side)
    own_spots = [carried_ref[me, 0, d] for d in range(owners)]
    taken_by = [twin_in[d].astype(f32) for d in range(owners)]
    for b in range(count):
        taken = jnp.zeros((side, per, tile), f32)
        for d in range(owners):
            taken = taken + jnp.where(own_spots[d] == b, 1.0, 0.0).astype(f32) * taken_by[d]
        forward[b] = taken
    await_bytes(stripe_far.at[pl.ds(0, side - 1)], stripe_recv.at[1])
    for b in range(count):
        clean = (
            (phase_out[other, (b - 1) % ring].astype(f32) - stripe_far[:, b].astype(f32))
            .astype(bf16)
            .astype(f32)
        )
        rest_in[other, b] = (clean - forward[b]).astype(bf16)
    await_bytes(rest_in.at[pl.ds(0, side - 1)], rest_recv.at[0])
    for b in range(count):
        residual_ref[:, b * tile : (b + 1) * tile] = (
            rest_in[:, b].astype(f32).reshape(slices, tile).astype(bf16)
        )

    await_bytes(update_in.at[:, 1], update_recv.at[2])
    for turn in range(2):
        held = group if turn == 0 else 1 - group
        await_bytes(update_in.at[turn, pl.ds(2, quarters - 2)], update_recv.at[turn])
        amount = own_update[turn]
        for k in range(1, quarters):
            amount = amount + update_in[turn, k].astype(f32)
        rows = pl.ds(pl.multiple_of(held * rows_half, rows_half), rows_half)
        old = image_ref[rows, pl.ds(pl.multiple_of(ray * share, share), share)].astype(f32)
        next_ref[rows, :] = old + relax_factor * amount
    await_bytes(carried_all.at[others], carried_send.at[0])
    await_bytes(rim, halo_send.at[0])
    await_bytes(phase_out.at[others, pl.ds(0, inner)], phase_send.at[0])
    await_bytes(phase_out.at[others, pl.ds(inner, 3)], phase_send.at[1])
    await_bytes(partial_out.at[others], partial_send.at[0])
    await_bytes(back_out.at[others], back_send.at[0])
    await_bytes(twin_in.at[others], twin_send.at[0])
    await_bytes(rest_out.at[pl.ds(0, side - 1)], rest_send.at[0])
    await_bytes(stripe_far, stripe_send.at[0])
    await_bytes(update_out.at[:, pl.ds(1, quarters - 1)], update_send.at[0])


def store_kernel(residual_ref, next_ref, residual_out, next_out, sem):
    copies = [
        pltpu.make_async_copy(residual_ref, residual_out, sem.at[0]),
        pltpu.make_async_copy(next_ref, next_out, sem.at[1]),
    ]
    for copy in copies:
        copy.start()
    for copy in copies:
        copy.wait()


def fast_shards(
    projections,
    phase_kernel,
    image,
    tile_library,
    tile_entry,
    tile_image,
    tile_slot,
    tile_count,
    slot_block,
):
    f32, bf16 = jnp.float32, jnp.bfloat16
    i32 = jnp.int32
    owners, quarters = lax.axis_size("dom"), lax.axis_size("ray")
    entries, tile = tile_library.shape[2], tile_library.shape[-1]
    _, slices, columns = projections.shape
    count = columns // tile
    ring = count + 1
    places = image.shape[0] // tile
    per = slices // owners
    capacity = tile_entry.shape[2]
    share = places * tile // quarters
    rows_half = slices // 2
    hbm = pl.BlockSpec(memory_space=pltpu.HBM)
    vmem = pl.BlockSpec(memory_space=pltpu.VMEM)
    sems = pltpu.SemaphoreType.DMA
    residual, image_next = pl.pallas_call(
        functools.partial(step_kernel, owners, quarters),
        out_shape=(
            jax.ShapeDtypeStruct((slices, columns), bf16),
            jax.ShapeDtypeStruct((slices, share), f32),
        ),
        in_specs=[hbm] * 8 + [pl.BlockSpec(memory_space=pltpu.SMEM)],
        out_specs=(vmem, vmem),
        scratch_shapes=[
            pltpu.VMEM(phase_kernel.shape, bf16),
            pltpu.VMEM((slices, columns), bf16),
            pltpu.VMEM((slices, places * tile), bf16),
            pltpu.VMEM((entries, tile, tile), bf16),
            pltpu.VMEM((3, 1, capacity), i32),
            pltpu.VMEM((1, owners), i32),
            pltpu.VMEM((owners, 1, owners), i32),
            pltpu.SMEM((owners, 1, owners), i32),
            pltpu.VMEM((1, 3 * tile), f32),
            pltpu.VMEM((2, slices, tile), bf16),
            pltpu.VMEM((owners, ring, per, tile), bf16),
            pltpu.VMEM((owners, ring, per, tile), bf16),
            pltpu.VMEM((per, ring * tile), f32),
            pltpu.VMEM((owners, ring, per, tile), f32),
            pltpu.VMEM((owners * places, entries * SUB), f32),
            pltpu.VMEM((owners * places * SUB, entries * SUB), bf16),
            pltpu.VMEM((owners * tile, places * tile), bf16),
            pltpu.VMEM((owners, owners, per, tile), bf16),
            pltpu.VMEM((owners, owners, per, tile), bf16),
            pltpu.VMEM((owners, 32, tile), f32),
            pltpu.VMEM((owners, owners, per, tile), bf16),
            pltpu.VMEM((owners, owners, per, tile), bf16),
            pltpu.VMEM((owners // 2, count, per, tile), bf16),
            pltpu.VMEM((owners, count, per, tile), bf16),
            pltpu.VMEM((count, per, tile), bf16),
            pltpu.VMEM((owners // 2, count, per, tile), bf16),
            pltpu.VMEM((owners, owners // 2, per, tile), bf16),
            pltpu.VMEM((count, owners // 2, per, tile), f32),
            pltpu.VMEM((2, rows_half, share), f32),
            pltpu.VMEM((2, rows_half, share), f32),
            pltpu.VMEM((2, quarters, rows_half, share), bf16),
            pltpu.VMEM((2, quarters, rows_half, share), bf16),
            sems((7,)),
            sems((1,)),
            sems((1,)),
            sems((1,)),
            sems((1,)),
            sems((2,)),
            sems((2,)),
            sems((1,)),
            sems((PARTS,)),
            sems((1,)),
            sems((2 * PARTS,)),
            sems((1,)),
            sems((1,)),
            sems((1,)),
            sems((2,)),
            sems((1,)),
            sems((1,)),
            sems((1,)),
            sems((3,)),
        ],
        compiler_params=pltpu.CompilerParams(
            collective_id=0, has_side_effects=True, vmem_limit_bytes=48 * 1024 * 1024
        ),
    )(
        *[
            pltpu.with_memory_space_constraint(x, pltpu.HBM)
            for x in (
                phase_kernel,
                projections,
                image.T,
                tile_library,
                tile_entry[0],
                tile_image[0],
                tile_slot[0],
                slot_block[0],
            )
        ],
        tile_count,
    )
    residual, image_next = pl.pallas_call(
        store_kernel,
        out_shape=(
            jax.ShapeDtypeStruct(residual.shape, bf16),
            jax.ShapeDtypeStruct(image_next.shape, f32),
        ),
        in_specs=[pl.BlockSpec(memory_space=pl.ANY)] * 2,
        out_specs=[pl.BlockSpec(memory_space=pl.ANY)] * 2,
        scratch_shapes=[sems((2,))],
    )(
        pltpu.with_memory_space_constraint(residual, pltpu.VMEM),
        pltpu.with_memory_space_constraint(image_next, pltpu.VMEM),
    )
    return residual[None], image_next.T


def fits_kernel(projections, phase_kernel, image, tile_library, tile_entry, *rest):
    owners, quarters = lax.axis_size("dom"), lax.axis_size("ray")
    tile = tile_library.shape[-1]
    angles, slices, columns = projections.shape
    return (
        angles == 1
        and slices % 16 == 0
        and slices == 8 * owners
        and owners == 8
        and tile == 128
        and phase_kernel.shape[0] == tile + 1
        and columns % tile == 0
        and tile_library.shape[2] == 16
        and quarters == 4
        and image.shape[0] == 16 * tile
        and tile_entry.shape[2] <= 256
    )


def any_shards(*args):
    if fits_kernel(*args):
        return fast_shards(*args)
    return shards(*args)


def solution(mesh):
    return jax.shard_map(
        any_shards,
        mesh=mesh,
        in_specs=(
            P("dom", None, "ray"),
            P(),
            P("dom", None),
            P("dom", "ray", None, None, None),
            P("dom", "ray", None),
            P("dom", "ray", None),
            P("dom", "ray", None),
            P("dom", "ray"),
            P("dom", "ray", None),
        ),
        out_specs=(P("dom", None, "ray"), P(("dom", "ray"), None)),
        check_vma=False,
    )
```

```python
import functools

import jax
import jax.numpy as jnp
from jax import lax
from jax.experimental import pallas as pl
from jax.experimental.pallas import tpu as pltpu
from jax.sharding import PartitionSpec as P

SMOOTH = 8


relax_factor = 0.25


def with_halo(cells, sides, width):
    for axis, dim in sides:
        count = lax.axis_size(axis)
        ends = count - 1
        head = lax.slice_in_dim(cells, 0, width, axis=dim)
        tail = lax.slice_in_dim(cells, cells.shape[dim] - width, cells.shape[dim], axis=dim)
        cells = jnp.concatenate(
            [
                lax.ppermute(tail, axis, [(i, (i + 1) % count) for i in range(ends)]),
                cells,
                lax.ppermute(head, axis, [((i + 1) % count, i) for i in range(ends)]),
            ],
            axis=dim,
        )
    return cells


def toeplitz(kernel, tile_size):
    taps = kernel.shape[0]
    padded = jnp.concatenate([kernel, jnp.zeros((2 * tile_size + 1 - taps,), kernel.dtype)])
    tiled = jnp.tile(padded, tile_size)[: 2 * tile_size * tile_size]
    return tiled.reshape(tile_size, 2 * tile_size).T


def phase_filter(projections, phase_kernel, tile_size):
    half_width = (phase_kernel.shape[0] - 1) // 2
    angles, slices, columns = projections.shape
    block_count = columns // tile_size
    rimmed = with_halo(projections, (("ray", 2),), half_width)
    padded = jnp.pad(rimmed, ((0, 0), (0, 0), (0, 2 * tile_size - 2 * half_width)))
    blocks = padded.reshape(angles, slices, block_count + 2, tile_size)
    windows = jnp.concatenate(
        [blocks[:, :, :block_count], blocks[:, :, 1 : block_count + 1]], axis=-1
    )
    filtered = jnp.einsum(
        "asbi,ij->asbj",
        windows,
        toeplitz(phase_kernel, tile_size),
        preferred_element_type=jnp.float32,
    )
    return filtered.reshape(angles, slices, columns).astype(jnp.bfloat16)


def stripe_profile(gathered):
    profile = jnp.median(gathered.astype(jnp.float32), axis=0)
    columns = profile.shape[1]
    rimmed = with_halo(profile, (("ray", 1),), SMOOTH)
    window_sum = jnp.zeros_like(profile)
    for offset in range(2 * SMOOTH + 1):
        window_sum = window_sum + rimmed[:, offset : offset + columns]
    position = lax.axis_index("ray") * columns + jnp.arange(columns)
    detector = lax.axis_size("ray") * columns
    in_range = (
        jnp.minimum(position + SMOOTH, detector - 1) - jnp.maximum(position - SMOOTH, 0) + 1
    ).astype(jnp.float32)
    return (profile - window_sum / in_range).astype(jnp.bfloat16)


def shards(
    projections,
    phase_kernel,
    image,
    tile_library,
    tile_entry,
    tile_image,
    tile_slot,
    tile_count,
    slot_block,
):
    tile_size = tile_library.shape[-1]
    angles, slices, columns = projections.shape
    phase = phase_filter(projections, phase_kernel, tile_size)
    gathered = lax.all_to_all(phase, "dom", split_axis=1, concat_axis=0, tiled=True)
    stripe = stripe_profile(gathered)
    fixed_rows = (gathered.astype(jnp.float32) - stripe.astype(jnp.float32)[None]).astype(
        jnp.bfloat16
    )
    corrected = lax.all_to_all(fixed_rows, "dom", split_axis=0, concat_axis=1, tiled=True)
    owners = lax.axis_size("dom")
    library = tile_library[0, 0]
    entries = tile_entry[0, 0]
    images = tile_image[0, 0]
    slots = tile_slot[0, 0]
    capacity = entries.shape[0]
    block_size = 64
    turn_count = capacity // block_size
    image_blocks = image.reshape(-1, tile_size, slices)
    block_total = image_blocks.shape[0]
    live_mask = jnp.arange(capacity) < tile_count[0, 0]
    slot_target = jnp.where(live_mask, slots, owners)
    image_target = jnp.where(live_mask, images, block_total)

    def forward_turn(turn_index, partial_value):
        first_tile = turn_index * block_size
        chosen = lax.dynamic_slice_in_dim(entries, first_tile, block_size)
        placed = lax.dynamic_slice_in_dim(images, first_tile, block_size)
        destined = lax.dynamic_slice_in_dim(slot_target, first_tile, block_size)
        product = jnp.einsum(
            "krp,kps->ksr",
            library[chosen],
            image_blocks[placed],
            preferred_element_type=jnp.float32,
        )
        return partial_value.at[destined].add(product, mode="drop")

    partial_value = lax.fori_loop(
        0, turn_count, forward_turn, jnp.zeros((owners, slices, tile_size), jnp.float32)
    )
    received = lax.all_to_all(
        partial_value.astype(jnp.bfloat16), "dom", split_axis=0, concat_axis=0, tiled=True
    )
    per_owner = columns // tile_size
    carried = slot_block[0, 0]
    block_ids = jnp.arange(angles * per_owner).reshape(angles, per_owner)
    selector = (block_ids[:, :, None] == carried[None, None, :]).astype(jnp.bfloat16)
    forward = jnp.einsum("abd,dst->asbt", selector, received, preferred_element_type=jnp.float32)
    residual = (corrected.astype(jnp.float32) - forward.reshape(angles, slices, columns)).astype(
        jnp.bfloat16
    )
    back = jnp.einsum(
        "abd,asbt->dst",
        selector,
        residual.reshape(angles, slices, per_owner, tile_size),
        preferred_element_type=jnp.float32,
    ).astype(jnp.bfloat16)
    returned = lax.all_to_all(back, "dom", split_axis=0, concat_axis=0, tiled=True)

    def adjoint_turn(turn_index, gradient):
        first_tile = turn_index * block_size
        chosen = lax.dynamic_slice_in_dim(entries, first_tile, block_size)
        sourced = lax.dynamic_slice_in_dim(slots, first_tile, block_size)
        destined = lax.dynamic_slice_in_dim(image_target, first_tile, block_size)
        product = jnp.einsum(
            "krp,ksr->kps", library[chosen], returned[sourced], preferred_element_type=jnp.float32
        )
        return gradient.at[destined].add(product, mode="drop")

    gradient = lax.fori_loop(
        0, turn_count, adjoint_turn, jnp.zeros((block_total, tile_size, slices), jnp.float32)
    )
    gradient = gradient.reshape(-1, slices)
    rows_own = gradient.shape[0] // lax.axis_size("ray")
    update = lax.psum_scatter(gradient, "ray", scatter_dimension=0, tiled=True)
    own_image = lax.dynamic_slice_in_dim(image, lax.axis_index("ray") * rows_own, rows_own)
    image_next = own_image.astype(jnp.float32) + relax_factor * update
    return (residual, image_next)


MESH = pl.DeviceIdType.MESH
NT = (((1,), (1,)), ((), ()))
NN = (((1,), (0,)), ((), ()))
SUB = 16
PARTS = 4


def dot(a, b, dims):
    return lax.dot_general(a, b, dims, preferred_element_type=jnp.float32)


def ordered(a, b):
    return jnp.minimum(a, b), jnp.maximum(a, b)


def sorted_four(a, b, c, d):
    a, b = ordered(a, b)
    c, d = ordered(c, d)
    a, c = ordered(a, c)
    b, d = ordered(b, d)
    b, c = ordered(b, c)
    return a, b, c, d


def median_of_eight(values):
    low = sorted_four(*values[:4])
    high = sorted_four(*values[4:])
    below = [jnp.minimum(low[i], high[3 - i]) for i in range(4)]
    above = [jnp.maximum(low[i], high[3 - i]) for i in range(4)]
    fourth = jnp.maximum(jnp.maximum(below[0], below[1]), jnp.maximum(below[2], below[3]))
    fifth = jnp.minimum(jnp.minimum(above[0], above[1]), jnp.minimum(above[2], above[3]))
    return (fourth + fifth) * 0.5


def step_kernel(
    owners,
    quarters,
    taps_any,
    proj_any,
    image_any,
    library_any,
    entry_any,
    place_any,
    slot_any,
    carried_any,
    count_ref,
    residual_ref,
    next_ref,
    taps_ref,
    proj_ref,
    image_ref,
    library_ref,
    lists_ref,
    carried_own,
    carried_all,
    carried_ref,
    taps_wide,
    rim,
    phase_out,
    phase_in,
    profile_ref,
    fixed,
    counted,
    spread_ref,
    matrix,
    partial_out,
    partial_in,
    same_ref,
    back_out,
    back_in,
    rest_out,
    rest_in,
    stripe_own,
    stripe_far,
    twin_in,
    forward,
    gathered,
    own_update,
    update_out,
    update_in,
    load_sem,
    halo_send,
    halo_recv,
    carried_send,
    carried_recv,
    phase_send,
    phase_recv,
    partial_send,
    partial_recv,
    back_send,
    back_recv,
    rest_send,
    rest_recv,
    stripe_send,
    stripe_recv,
    twin_send,
    twin_recv,
    update_send,
    update_recv,
):
    f32, bf16 = jnp.float32, jnp.bfloat16
    me, ray = lax.axis_index("dom"), lax.axis_index("ray")
    slices, columns = proj_ref.shape
    entries, tile = library_ref.shape[0], library_ref.shape[-1]
    places = image_ref.shape[1] // tile
    count = columns // tile
    ring = count + 1
    inner = count - 2
    per = slices // owners
    side = owners // 2
    half = tile // 2
    share = places * tile // quarters
    rows_half = side * per
    some = owners // PARTS

    group, spot = me // side, lax.rem(me, side)

    def dom_peer(k):
        if k >= side:
            return (1 - group) * side + lax.rem(spot + k - side, side)
        return group * side + lax.rem(spot + k, side)

    dom_order = list(range(1, owners))

    chip, core = ray // 2, lax.rem(ray, 2)

    def ray_twin(k):
        chip_to = 1 - chip if k >= 2 else chip
        core_to = 1 - core if k % 2 else core
        return chip_to * 2 + core_to

    def ray_next(k):
        return lax.rem(ray + k, quarters)

    barrier = pltpu.get_barrier_semaphore()
    for k in range(1, owners):
        pl.semaphore_signal(barrier, inc=1, device_id=(dom_peer(k), ray), device_id_type=MESH)
    for k in range(1, quarters):
        pl.semaphore_signal(barrier, inc=1, device_id=(me, ray_next(k)), device_id_type=MESH)

    pairs = [
        (proj_any.at[0], proj_ref, 0),
        (taps_any, taps_ref, 1),
        (carried_any, carried_own, 2),
        (entry_any, lists_ref.at[0], 3),
        (place_any, lists_ref.at[1], 3),
        (slot_any, lists_ref.at[2], 3),
        (library_any.at[0, 0], library_ref, 4),
        (image_any, image_ref, 5),
    ]
    for src, dst, i in pairs:
        pltpu.make_async_copy(src, dst, load_sem.at[i]).start()

    def await_bytes(ref, sem):
        pltpu.make_async_copy(ref, ref, sem).wait()

    def dom_copy(src, dst, send, recv, k):
        pltpu.make_async_remote_copy(
            src_ref=src,
            dst_ref=dst,
            send_sem=send,
            recv_sem=recv,
            device_id=(dom_peer(k), ray),
            device_id_type=MESH,
        ).start()

    def ray_copy(src, dst, send, recv, peer):
        pltpu.make_async_remote_copy(
            src_ref=src,
            dst_ref=dst,
            send_sem=send,
            recv_sem=recv,
            device_id=(me, peer),
            device_id_type=MESH,
        ).start()

    def block(b):
        return proj_ref[:, b * tile : (b + 1) * tile]

    await_bytes(taps_ref, load_sem.at[1])
    taps_wide[...] = jnp.zeros(taps_wide.shape, f32)
    taps_wide[:, : taps_ref.shape[0]] = taps_ref[...].astype(f32)[None]
    spread = jnp.broadcast_to(taps_wide[...], (tile, taps_wide.shape[1]))
    weights = pltpu.roll(spread, half, 1, stride=1, stride_axis=0).astype(bf16)
    await_bytes(proj_ref, load_sem.at[0])
    two = jnp.concatenate(
        [proj_ref[:, (b - 1) * tile : (b + 1) * tile] for b in range(1, count - 1)], axis=0
    )
    third = jnp.concatenate([block(b + 1) for b in range(1, count - 1)], axis=0)
    phase = dot(two, weights[:, : 2 * tile], NT) + dot(third, weights[:, 2 * tile :], NT)
    phase = phase.reshape(inner, owners, per, tile)
    for owner in range(owners):
        phase_out[owner, :inner] = phase[:, owner].astype(bf16)

    await_bytes(carried_own, load_sem.at[2])
    pl.semaphore_wait(barrier, owners + quarters - 2)

    for k in dom_order:
        dom_copy(carried_own, carried_all.at[me], carried_send.at[0], carried_recv.at[0], k)
    ray_copy(
        proj_ref.at[:, pl.ds(columns - tile, tile)],
        rim.at[0],
        halo_send.at[0],
        halo_recv.at[0],
        ray_next(1),
    )
    ray_copy(
        proj_ref.at[:, pl.ds(0, tile)],
        rim.at[1],
        halo_send.at[0],
        halo_recv.at[0],
        ray_next(quarters - 1),
    )
    for k in dom_order:
        dom_copy(
            phase_out.at[dom_peer(k), pl.ds(0, inner)],
            phase_in.at[me, pl.ds(0, inner)],
            phase_send.at[0],
            phase_recv.at[0],
            k,
        )

    await_bytes(lists_ref, load_sem.at[3])
    capacity = lists_ref.shape[2]
    entry, place, slot = lists_ref[0], lists_ref[1], lists_ref[2]
    alive = lax.broadcasted_iota(jnp.int32, (1, capacity), 1) < count_ref[0, 0]
    code = jnp.where(alive, slot * places + place, -1)
    pick = jnp.where(
        lax.broadcasted_iota(jnp.int32, (owners * places, capacity), 0) == code, 1.0, 0.0
    ).astype(bf16)
    which = jnp.where(
        lax.broadcasted_iota(jnp.int32, (entries * SUB, capacity), 0) // SUB == entry,
        1.0,
        0.0,
    ).astype(bf16)
    counted[...] = dot(pick, which, NT)
    diagonal = lax.rem(
        lax.broadcasted_iota(jnp.int32, (SUB, entries * SUB), 1), SUB
    ) == lax.broadcasted_iota(jnp.int32, (SUB, entries * SUB), 0)

    def widen(step, carry):
        for i in range(8):
            at = step * 8 + i
            row = jnp.broadcast_to(counted[pl.ds(at, 1), :], (SUB, entries * SUB))
            start = pl.multiple_of(at * SUB, SUB)
            spread_ref[pl.ds(start, SUB), :] = jnp.where(diagonal, row, 0.0).astype(bf16)
        return carry

    lax.fori_loop(0, owners * places // 8, widen, 0)

    await_bytes(library_ref, load_sem.at[4])

    def build(step, carry):
        first = pl.multiple_of(step * 2 * SUB, 2 * SUB)
        right = jnp.concatenate(
            [
                library_ref[:, pl.ds(first + i * SUB, SUB), :].reshape(entries * SUB, tile)
                for i in range(2)
            ],
            axis=1,
        )
        for owner in range(owners):
            rows = places * SUB
            made = dot(spread_ref[owner * rows : (owner + 1) * rows, :], right, NN)
            for place in range(places):
                for i in range(2):
                    start = pl.multiple_of(first + owner * tile + i * SUB, SUB)
                    matrix[pl.ds(start, SUB), place * tile : (place + 1) * tile] = made[
                        place * SUB : (place + 1) * SUB, i * tile : (i + 1) * tile
                    ].astype(bf16)
        return carry

    lax.fori_loop(0, tile // (2 * SUB), build, 0)

    await_bytes(rim, halo_recv.at[0])

    @pl.when(ray == 0)
    def _():
        rim[0] = jnp.zeros((slices, tile), bf16)

    @pl.when(ray == quarters - 1)
    def _():
        rim[1] = jnp.zeros((slices, tile), bf16)

    before, after = rim[0], rim[1]
    two = jnp.concatenate(
        [
            proj_ref[:, (count - 2) * tile : count * tile],
            jnp.concatenate([block(count - 1), after], axis=1),
            jnp.concatenate([before, block(0)], axis=1),
            jnp.concatenate([before, before], axis=1),
        ],
        axis=0,
    )
    third = jnp.concatenate([after, after, block(1), block(0)], axis=0)
    edge = dot(two, weights[:, : 2 * tile], NT) + dot(third, weights[:, 2 * tile :], NT)
    edge = edge.reshape(4, owners, per, tile)
    lane = lax.broadcasted_iota(jnp.int32, (owners, per, tile), 2)
    phase_out[:, inner] = edge[0].astype(bf16)
    phase_out[:, inner + 1] = jnp.where(lane < half, edge[1], edge[3]).astype(bf16)
    phase_out[:, inner + 2] = edge[2].astype(bf16)
    for k in dom_order:
        dom_copy(
            phase_out.at[dom_peer(k), pl.ds(inner, 3)],
            phase_in.at[me, pl.ds(inner, 3)],
            phase_send.at[1],
            phase_recv.at[1],
            k,
        )
    phase_in[me] = phase_out[me]

    def send_partials(part):
        chosen = pl.ds(part * some, some)
        for k in dom_order:
            dom_copy(
                partial_out.at[dom_peer(k), chosen],
                partial_in.at[me, chosen],
                partial_send.at[0],
                partial_recv.at[part],
                k,
            )

    def send_all_partials():
        for part in range(PARTS):
            send_partials(part)

    await_bytes(image_ref, load_sem.at[5])
    for part in range(PARTS):
        for owner in range(part * some, (part + 1) * some, 2):
            made = dot(image_ref[...], matrix[owner * tile : (owner + 2) * tile, :], NT)
            for i in range(2):
                partial_out[:, owner + i] = (
                    made[:, i * tile : (i + 1) * tile].reshape(owners, per, tile).astype(bf16)
                )
        pl.when(core == 0)(functools.partial(send_partials, part))
    partial_in[me] = partial_out[me]

    def send_twins():
        for k in dom_order:
            dom_copy(
                partial_out.at[pl.ds((1 - dom_peer(k) // side) * side, side), dom_peer(k)],
                twin_in.at[me],
                twin_send.at[0],
                twin_recv.at[0],
                k,
            )

    twin_in[me] = partial_out[pl.ds((1 - group) * side, side), me]

    carried_all[me] = carried_own[...]
    await_bytes(carried_all.at[pl.ds(0, owners - 1)], carried_recv.at[0])
    to_scalar = pltpu.make_async_copy(carried_all, carried_ref, load_sem.at[6])
    to_scalar.start()
    to_scalar.wait()
    duos = [(a, b) for a in range(owners) for b in range(a + 1, owners)]

    def compare(owner, carry):
        for i, (a, b) in enumerate(duos):
            same = jnp.where(carried_ref[owner, 0, a] == carried_ref[owner, 0, b], 1.0, 0.0)
            same_ref[owner, i : i + 1, :] = jnp.full((1, tile), same, f32)
        return carry

    lax.fori_loop(0, owners, compare, 0)

    def profile_of(i):
        return median_of_eight([phase_in[a, i].astype(f32) for a in range(owners)])

    others = pl.ds(0, owners - 1)
    await_bytes(phase_in.at[others, pl.ds(0, inner)], phase_recv.at[0])
    for i in range(inner):
        profile_ref[:, i * tile : (i + 1) * tile] = profile_of(i)
    await_bytes(phase_in.at[others, pl.ds(inner, 3)], phase_recv.at[1])
    pl.when(core == 1)(send_all_partials)
    for i in range(inner, ring):
        profile_ref[:, i * tile : (i + 1) * tile] = profile_of(i)

    width = ring * tile
    detector = quarters * columns
    at = lax.broadcasted_iota(jnp.int32, (1, width), 1)
    position = ray * columns + jnp.where(at < count * tile - half, at + tile, at - columns)
    profile = jnp.where((position >= 0) & (position < detector), profile_ref[...], 0.0)
    run = profile
    reach = 1
    while reach < 2 * SMOOTH:
        run = run + pltpu.roll(run, reach, 1)
        reach *= 2
    window = pltpu.roll(run, width - (SMOOTH - 1), 1) + pltpu.roll(profile, width - SMOOTH, 1)
    in_range = (
        jnp.minimum(position + SMOOTH, detector - 1) - jnp.maximum(position - SMOOTH, 0) + 1
    ).astype(f32)
    stripe = (profile - window / in_range).astype(bf16).astype(f32)
    for b in range(count):
        i = (b - 1) % ring
        stripe_own[b] = stripe[:, i * tile : (i + 1) * tile].astype(bf16)
    for a in range(owners):
        for i in range(ring):
            if i != count - 1:
                fixed[a, i] = (
                    (phase_in[a, i].astype(f32) - stripe[:, i * tile : (i + 1) * tile])
                    .astype(bf16)
                    .astype(f32)
                )

    def ring_spot(b):
        return jnp.where(b == 0, ring - 1, b - 1)

    def carry_back(owner, carry):
        part = [partial_in[d, owner].astype(f32) for d in range(owners)]
        total = list(part)
        for i, (a, b) in enumerate(duos):
            same = jnp.broadcast_to(same_ref[owner, i : i + 1, :], (per, tile))
            total[a] = total[a] + same * part[b]
            total[b] = total[b] + same * part[a]
        for d in range(owners):
            back_out[d, owner] = (
                fixed[owner, ring_spot(carried_ref[owner, 0, d])] - total[d]
            ).astype(bf16)
        return carry

    for part in range(PARTS):
        chosen = pl.ds(part * some, some)
        await_bytes(partial_in.at[others, chosen], partial_recv.at[part])
        lax.fori_loop(part * some, (part + 1) * some, carry_back, 0)
        for k in dom_order:
            dom_copy(
                back_out.at[dom_peer(k), chosen],
                back_in.at[me, chosen],
                back_send.at[0],
                back_recv.at[part * 2 + k // side],
                k,
            )
    back_in[me] = back_out[me]

    def whole(i, carry):
        owner = group * side + i
        part = [partial_in[d, owner].astype(f32) for d in range(owners)]
        where_to = [carried_ref[owner, 0, d] for d in range(owners)]
        for b in range(count):
            total = fixed[owner, (b - 1) % ring]
            taken = jnp.zeros((per, tile), f32)
            for d in range(owners):
                taken = taken + jnp.where(where_to[d] == b, 1.0, 0.0).astype(f32) * part[d]
            rest_out[i, b] = (total - taken).astype(bf16)
        return carry

    lax.fori_loop(0, side, whole, 0)
    dom_copy(stripe_own, stripe_far.at[spot], stripe_send.at[0], stripe_recv.at[0], side)
    for k in range(1, side):
        dom_copy(
            rest_out.at[lax.rem(spot + k, side)],
            rest_in.at[me],
            rest_send.at[0],
            rest_recv.at[0],
            k,
        )
    rest_in[me] = rest_out[spot]

    def rows_of(turn, part):
        first = (group if turn == 0 else 1 - group) * side
        return jnp.concatenate(
            [
                back_in[pl.ds(first, side), owner]
                .astype(f32)
                .reshape(rows_half, tile)
                .astype(bf16)
                for owner in range(part * some, (part + 1) * some)
            ],
            axis=1,
        )

    def send_update(turn, k, sem):
        ray_copy(
            update_out.at[turn, k],
            update_in.at[turn, k],
            update_send.at[0],
            update_recv.at[sem],
            ray_twin(k),
        )

    for turn in range(2):
        for part in range(PARTS):
            await_bytes(
                back_in.at[pl.ds(0, side - 1 + turn), pl.ds(part * some, some)],
                back_recv.at[part * 2 + turn],
            )
            left = rows_of(turn, part)
            rows = slice(part * some * tile, (part + 1) * some * tile)
            for k in (2, 3):
                start = pl.multiple_of(ray_twin(k) * share, share)
                made = dot(left, matrix[rows, pl.ds(start, share)], NN)
                if part > 0:
                    made = made + gathered[k - 2]
                if part < PARTS - 1:
                    gathered[k - 2] = made
                else:
                    update_out[turn, k] = made.astype(bf16)
                    send_update(turn, k, turn)
        if turn == 0:
            send_twins()

    left = jnp.concatenate(
        [
            jnp.concatenate([rows_of(turn, part) for part in range(PARTS)], axis=1)
            for turn in range(2)
        ],
        axis=0,
    )
    start = pl.multiple_of(ray_twin(1) * share, share)
    made = dot(left, matrix[:, pl.ds(start, share)], NN).reshape(2, rows_half, share)
    update_out[:, 1] = made.astype(bf16)
    for turn in range(2):
        send_update(turn, 1, 2)

    await_bytes(stripe_own, stripe_recv.at[0])
    for k in range(1, side):
        dom_copy(
            stripe_far.at[spot], stripe_far.at[spot], stripe_send.at[0], stripe_recv.at[1], k
        )

    start = pl.multiple_of(ray * share, share)
    own_update[...] = dot(left, matrix[:, pl.ds(start, share)], NN).reshape(2, rows_half, share)

    await_bytes(twin_in.at[others], twin_recv.at[0])
    other = pl.ds((1 - group) * side, side)
    own_spots = [carried_ref[me, 0, d] for d in range(owners)]
    taken_by = [twin_in[d].astype(f32) for d in range(owners)]
    for b in range(count):
        taken = jnp.zeros((side, per, tile), f32)
        for d in range(owners):
            taken = taken + jnp.where(own_spots[d] == b, 1.0, 0.0).astype(f32) * taken_by[d]
        forward[b] = taken
    await_bytes(stripe_far.at[pl.ds(0, side - 1)], stripe_recv.at[1])
    for b in range(count):
        clean = (
            (phase_out[other, (b - 1) % ring].astype(f32) - stripe_far[:, b].astype(f32))
            .astype(bf16)
            .astype(f32)
        )
        rest_in[other, b] = (clean - forward[b]).astype(bf16)
    await_bytes(rest_in.at[pl.ds(0, side - 1)], rest_recv.at[0])
    for b in range(count):
        residual_ref[:, b * tile : (b + 1) * tile] = (
            rest_in[:, b].astype(f32).reshape(slices, tile).astype(bf16)
        )

    await_bytes(update_in.at[:, 1], update_recv.at[2])
    for turn in range(2):
        held = group if turn == 0 else 1 - group
        await_bytes(update_in.at[turn, pl.ds(2, quarters - 2)], update_recv.at[turn])
        amount = own_update[turn]
        for k in range(1, quarters):
            amount = amount + update_in[turn, k].astype(f32)
        rows = pl.ds(pl.multiple_of(held * rows_half, rows_half), rows_half)
        old = image_ref[rows, pl.ds(pl.multiple_of(ray * share, share), share)].astype(f32)
        next_ref[rows, :] = old + relax_factor * amount
    await_bytes(carried_all.at[others], carried_send.at[0])
    await_bytes(rim, halo_send.at[0])
    await_bytes(phase_out.at[others, pl.ds(0, inner)], phase_send.at[0])
    await_bytes(phase_out.at[others, pl.ds(inner, 3)], phase_send.at[1])
    await_bytes(partial_out.at[others], partial_send.at[0])
    await_bytes(back_out.at[others], back_send.at[0])
    await_bytes(twin_in.at[others], twin_send.at[0])
    await_bytes(rest_out.at[pl.ds(0, side - 1)], rest_send.at[0])
    await_bytes(stripe_far, stripe_send.at[0])
    await_bytes(update_out.at[:, pl.ds(1, quarters - 1)], update_send.at[0])


def store_kernel(residual_ref, next_ref, residual_out, next_out, sem):
    copies = [
        pltpu.make_async_copy(residual_ref, residual_out, sem.at[0]),
        pltpu.make_async_copy(next_ref, next_out, sem.at[1]),
    ]
    for copy in copies:
        copy.start()
    for copy in copies:
        copy.wait()


def fast_shards(
    projections,
    phase_kernel,
    image,
    tile_library,
    tile_entry,
    tile_image,
    tile_slot,
    tile_count,
    slot_block,
):
    f32, bf16 = jnp.float32, jnp.bfloat16
    i32 = jnp.int32
    owners, quarters = lax.axis_size("dom"), lax.axis_size("ray")
    entries, tile = tile_library.shape[2], tile_library.shape[-1]
    _, slices, columns = projections.shape
    count = columns // tile
    ring = count + 1
    places = image.shape[0] // tile
    per = slices // owners
    capacity = tile_entry.shape[2]
    share = places * tile // quarters
    rows_half = slices // 2
    hbm = pl.BlockSpec(memory_space=pltpu.HBM)
    vmem = pl.BlockSpec(memory_space=pltpu.VMEM)
    sems = pltpu.SemaphoreType.DMA
    residual, image_next = pl.pallas_call(
        functools.partial(step_kernel, owners, quarters),
        out_shape=(
            jax.ShapeDtypeStruct((slices, columns), bf16),
            jax.ShapeDtypeStruct((slices, share), f32),
        ),
        in_specs=[hbm] * 8 + [pl.BlockSpec(memory_space=pltpu.SMEM)],
        out_specs=(vmem, vmem),
        scratch_shapes=[
            pltpu.VMEM(phase_kernel.shape, bf16),
            pltpu.VMEM((slices, columns), bf16),
            pltpu.VMEM((slices, places * tile), bf16),
            pltpu.VMEM((entries, tile, tile), bf16),
            pltpu.VMEM((3, 1, capacity), i32),
            pltpu.VMEM((1, owners), i32),
            pltpu.VMEM((owners, 1, owners), i32),
            pltpu.SMEM((owners, 1, owners), i32),
            pltpu.VMEM((1, 3 * tile), f32),
            pltpu.VMEM((2, slices, tile), bf16),
            pltpu.VMEM((owners, ring, per, tile), bf16),
            pltpu.VMEM((owners, ring, per, tile), bf16),
            pltpu.VMEM((per, ring * tile), f32),
            pltpu.VMEM((owners, ring, per, tile), f32),
            pltpu.VMEM((owners * places, entries * SUB), f32),
            pltpu.VMEM((owners * places * SUB, entries * SUB), bf16),
            pltpu.VMEM((owners * tile, places * tile), bf16),
            pltpu.VMEM((owners, owners, per, tile), bf16),
            pltpu.VMEM((owners, owners, per, tile), bf16),
            pltpu.VMEM((owners, 32, tile), f32),
            pltpu.VMEM((owners, owners, per, tile), bf16),
            pltpu.VMEM((owners, owners, per, tile), bf16),
            pltpu.VMEM((owners // 2, count, per, tile), bf16),
            pltpu.VMEM((owners, count, per, tile), bf16),
            pltpu.VMEM((count, per, tile), bf16),
            pltpu.VMEM((owners // 2, count, per, tile), bf16),
            pltpu.VMEM((owners, owners // 2, per, tile), bf16),
            pltpu.VMEM((count, owners // 2, per, tile), f32),
            pltpu.VMEM((2, rows_half, share), f32),
            pltpu.VMEM((2, rows_half, share), f32),
            pltpu.VMEM((2, quarters, rows_half, share), bf16),
            pltpu.VMEM((2, quarters, rows_half, share), bf16),
            sems((7,)),
            sems((1,)),
            sems((1,)),
            sems((1,)),
            sems((1,)),
            sems((2,)),
            sems((2,)),
            sems((1,)),
            sems((PARTS,)),
            sems((1,)),
            sems((2 * PARTS,)),
            sems((1,)),
            sems((1,)),
            sems((1,)),
            sems((2,)),
            sems((1,)),
            sems((1,)),
            sems((1,)),
            sems((3,)),
        ],
        compiler_params=pltpu.CompilerParams(
            collective_id=0, has_side_effects=True, vmem_limit_bytes=48 * 1024 * 1024
        ),
    )(
        *[
            pltpu.with_memory_space_constraint(x, pltpu.HBM)
            for x in (
                phase_kernel,
                projections,
                image.T,
                tile_library,
                tile_entry[0],
                tile_image[0],
                tile_slot[0],
                slot_block[0],
            )
        ],
        tile_count,
    )
    residual, image_next = pl.pallas_call(
        store_kernel,
        out_shape=(
            jax.ShapeDtypeStruct(residual.shape, bf16),
            jax.ShapeDtypeStruct(image_next.shape, f32),
        ),
        in_specs=[pl.BlockSpec(memory_space=pl.ANY)] * 2,
        out_specs=[pl.BlockSpec(memory_space=pl.ANY)] * 2,
        scratch_shapes=[sems((2,))],
    )(
        pltpu.with_memory_space_constraint(residual, pltpu.VMEM),
        pltpu.with_memory_space_constraint(image_next, pltpu.VMEM),
    )
    return residual[None], image_next.T


def fits_kernel(projections, phase_kernel, image, tile_library, tile_entry, *rest):
    owners, quarters = lax.axis_size("dom"), lax.axis_size("ray")
    tile = tile_library.shape[-1]
    angles, slices, columns = projections.shape
    return (
        angles == 1
        and slices % 16 == 0
        and slices == 8 * owners
        and owners == 8
        and tile == 128
        and phase_kernel.shape[0] == tile + 1
        and columns % tile == 0
        and tile_library.shape[2] == 16
        and quarters == 4
        and image.shape[0] == 16 * tile
        and tile_entry.shape[2] <= 256
    )


def any_shards(*args):
    if fits_kernel(*args):
        return fast_shards(*args)
    return shards(*args)


def solution(mesh):
    return jax.shard_map(
        any_shards,
        mesh=mesh,
        in_specs=(
            P("dom", None, "ray"),
            P(),
            P("dom", None),
            P("dom", "ray", None, None, None),
            P("dom", "ray", None),
            P("dom", "ray", None),
            P("dom", "ray", None),
            P("dom", "ray"),
            P("dom", "ray", None),
        ),
        out_specs=(P("dom", None, "ray"), P(("dom", "ray"), None)),
        check_vma=False,
    )
```

```python
import functools

import jax
import jax.numpy as jnp
from jax import lax
from jax.experimental import pallas as pl
from jax.experimental.pallas import tpu as pltpu
from jax.sharding import PartitionSpec as P

SMOOTH = 8


relax_factor = 0.25


def with_halo(cells, sides, width):
    for axis, dim in sides:
        count = lax.axis_size(axis)
        ends = count - 1
        head = lax.slice_in_dim(cells, 0, width, axis=dim)
        tail = lax.slice_in_dim(cells, cells.shape[dim] - width, cells.shape[dim], axis=dim)
        cells = jnp.concatenate(
            [
                lax.ppermute(tail, axis, [(i, (i + 1) % count) for i in range(ends)]),
                cells,
                lax.ppermute(head, axis, [((i + 1) % count, i) for i in range(ends)]),
            ],
            axis=dim,
        )
    return cells


def toeplitz(kernel, tile_size):
    taps = kernel.shape[0]
    padded = jnp.concatenate([kernel, jnp.zeros((2 * tile_size + 1 - taps,), kernel.dtype)])
    tiled = jnp.tile(padded, tile_size)[: 2 * tile_size * tile_size]
    return tiled.reshape(tile_size, 2 * tile_size).T


def phase_filter(projections, phase_kernel, tile_size):
    half_width = (phase_kernel.shape[0] - 1) // 2
    angles, slices, columns = projections.shape
    block_count = columns // tile_size
    rimmed = with_halo(projections, (("ray", 2),), half_width)
    padded = jnp.pad(rimmed, ((0, 0), (0, 0), (0, 2 * tile_size - 2 * half_width)))
    blocks = padded.reshape(angles, slices, block_count + 2, tile_size)
    windows = jnp.concatenate(
        [blocks[:, :, :block_count], blocks[:, :, 1 : block_count + 1]], axis=-1
    )
    filtered = jnp.einsum(
        "asbi,ij->asbj",
        windows,
        toeplitz(phase_kernel, tile_size),
        preferred_element_type=jnp.float32,
    )
    return filtered.reshape(angles, slices, columns).astype(jnp.bfloat16)


def stripe_profile(gathered):
    profile = jnp.median(gathered.astype(jnp.float32), axis=0)
    columns = profile.shape[1]
    rimmed = with_halo(profile, (("ray", 1),), SMOOTH)
    window_sum = jnp.zeros_like(profile)
    for offset in range(2 * SMOOTH + 1):
        window_sum = window_sum + rimmed[:, offset : offset + columns]
    position = lax.axis_index("ray") * columns + jnp.arange(columns)
    detector = lax.axis_size("ray") * columns
    in_range = (
        jnp.minimum(position + SMOOTH, detector - 1) - jnp.maximum(position - SMOOTH, 0) + 1
    ).astype(jnp.float32)
    return (profile - window_sum / in_range).astype(jnp.bfloat16)


def shards(
    projections,
    phase_kernel,
    image,
    tile_library,
    tile_entry,
    tile_image,
    tile_slot,
    tile_count,
    slot_block,
):
    tile_size = tile_library.shape[-1]
    angles, slices, columns = projections.shape
    phase = phase_filter(projections, phase_kernel, tile_size)
    gathered = lax.all_to_all(phase, "dom", split_axis=1, concat_axis=0, tiled=True)
    stripe = stripe_profile(gathered)
    fixed_rows = (gathered.astype(jnp.float32) - stripe.astype(jnp.float32)[None]).astype(
        jnp.bfloat16
    )
    corrected = lax.all_to_all(fixed_rows, "dom", split_axis=0, concat_axis=1, tiled=True)
    owners = lax.axis_size("dom")
    library = tile_library[0, 0]
    entries = tile_entry[0, 0]
    images = tile_image[0, 0]
    slots = tile_slot[0, 0]
    capacity = entries.shape[0]
    block_size = 64
    turn_count = capacity // block_size
    image_blocks = image.reshape(-1, tile_size, slices)
    block_total = image_blocks.shape[0]
    live_mask = jnp.arange(capacity) < tile_count[0, 0]
    slot_target = jnp.where(live_mask, slots, owners)
    image_target = jnp.where(live_mask, images, block_total)

    def forward_turn(turn_index, partial_value):
        first_tile = turn_index * block_size
        chosen = lax.dynamic_slice_in_dim(entries, first_tile, block_size)
        placed = lax.dynamic_slice_in_dim(images, first_tile, block_size)
        destined = lax.dynamic_slice_in_dim(slot_target, first_tile, block_size)
        product = jnp.einsum(
            "krp,kps->ksr",
            library[chosen],
            image_blocks[placed],
            preferred_element_type=jnp.float32,
        )
        return partial_value.at[destined].add(product, mode="drop")

    partial_value = lax.fori_loop(
        0, turn_count, forward_turn, jnp.zeros((owners, slices, tile_size), jnp.float32)
    )
    received = lax.all_to_all(
        partial_value.astype(jnp.bfloat16), "dom", split_axis=0, concat_axis=0, tiled=True
    )
    per_owner = columns // tile_size
    carried = slot_block[0, 0]
    block_ids = jnp.arange(angles * per_owner).reshape(angles, per_owner)
    selector = (block_ids[:, :, None] == carried[None, None, :]).astype(jnp.bfloat16)
    forward = jnp.einsum("abd,dst->asbt", selector, received, preferred_element_type=jnp.float32)
    residual = (corrected.astype(jnp.float32) - forward.reshape(angles, slices, columns)).astype(
        jnp.bfloat16
    )
    back = jnp.einsum(
        "abd,asbt->dst",
        selector,
        residual.reshape(angles, slices, per_owner, tile_size),
        preferred_element_type=jnp.float32,
    ).astype(jnp.bfloat16)
    returned = lax.all_to_all(back, "dom", split_axis=0, concat_axis=0, tiled=True)

    def adjoint_turn(turn_index, gradient):
        first_tile = turn_index * block_size
        chosen = lax.dynamic_slice_in_dim(entries, first_tile, block_size)
        sourced = lax.dynamic_slice_in_dim(slots, first_tile, block_size)
        destined = lax.dynamic_slice_in_dim(image_target, first_tile, block_size)
        product = jnp.einsum(
            "krp,ksr->kps", library[chosen], returned[sourced], preferred_element_type=jnp.float32
        )
        return gradient.at[destined].add(product, mode="drop")

    gradient = lax.fori_loop(
        0, turn_count, adjoint_turn, jnp.zeros((block_total, tile_size, slices), jnp.float32)
    )
    gradient = gradient.reshape(-1, slices)
    rows_own = gradient.shape[0] // lax.axis_size("ray")
    update = lax.psum_scatter(gradient, "ray", scatter_dimension=0, tiled=True)
    own_image = lax.dynamic_slice_in_dim(image, lax.axis_index("ray") * rows_own, rows_own)
    image_next = own_image.astype(jnp.float32) + relax_factor * update
    return (residual, image_next)


MESH = pl.DeviceIdType.MESH
NT = (((1,), (1,)), ((), ()))
NN = (((1,), (0,)), ((), ()))
SUB = 16
PARTS = 4


def dot(a, b, dims):
    return lax.dot_general(a, b, dims, preferred_element_type=jnp.float32)


def ordered(a, b):
    return jnp.minimum(a, b), jnp.maximum(a, b)


def sorted_four(a, b, c, d):
    a, b = ordered(a, b)
    c, d = ordered(c, d)
    a, c = ordered(a, c)
    b, d = ordered(b, d)
    b, c = ordered(b, c)
    return a, b, c, d


def median_of_eight(values):
    low = sorted_four(*values[:4])
    high = sorted_four(*values[4:])
    below = [jnp.minimum(low[i], high[3 - i]) for i in range(4)]
    above = [jnp.maximum(low[i], high[3 - i]) for i in range(4)]
    fourth = jnp.maximum(jnp.maximum(below[0], below[1]), jnp.maximum(below[2], below[3]))
    fifth = jnp.minimum(jnp.minimum(above[0], above[1]), jnp.minimum(above[2], above[3]))
    return (fourth + fifth) * 0.5


def step_kernel(
    owners,
    quarters,
    taps_any,
    proj_any,
    image_any,
    library_any,
    entry_any,
    place_any,
    slot_any,
    carried_any,
    count_ref,
    residual_ref,
    next_ref,
    taps_ref,
    proj_ref,
    image_ref,
    library_ref,
    lists_ref,
    carried_own,
    carried_all,
    carried_ref,
    taps_wide,
    rim,
    phase_out,
    phase_in,
    profile_ref,
    fixed,
    counted,
    spread_ref,
    matrix,
    partial_out,
    partial_in,
    same_ref,
    back_out,
    back_in,
    rest_out,
    rest_in,
    stripe_own,
    stripe_far,
    twin_in,
    forward,
    gathered,
    own_update,
    update_out,
    update_in,
    load_sem,
    halo_send,
    halo_recv,
    carried_send,
    carried_recv,
    phase_send,
    phase_recv,
    partial_send,
    partial_recv,
    back_send,
    back_recv,
    rest_send,
    rest_recv,
    stripe_send,
    stripe_recv,
    twin_send,
    twin_recv,
    update_send,
    update_recv,
):
    f32, bf16 = jnp.float32, jnp.bfloat16
    me, ray = lax.axis_index("dom"), lax.axis_index("ray")
    slices, columns = proj_ref.shape
    entries, tile = library_ref.shape[0], library_ref.shape[-1]
    places = image_ref.shape[1] // tile
    count = columns // tile
    ring = count + 1
    inner = count - 2
    per = slices // owners
    side = owners // 2
    half = tile // 2
    share = places * tile // quarters
    rows_half = side * per
    some = owners // PARTS

    group, spot = me // side, lax.rem(me, side)

    def dom_peer(k):
        if k >= side:
            return (1 - group) * side + lax.rem(spot + k - side, side)
        return group * side + lax.rem(spot + k, side)

    dom_order = list(range(1, owners))
    far_order = list(range(side, owners)) + list(range(1, side))

    chip, core = ray // 2, lax.rem(ray, 2)

    def ray_twin(k):
        chip_to = 1 - chip if k >= 2 else chip
        core_to = 1 - core if k % 2 else core
        return chip_to * 2 + core_to

    def ray_next(k):
        return lax.rem(ray + k, quarters)

    barrier = pltpu.get_barrier_semaphore()
    for k in range(1, owners):
        pl.semaphore_signal(barrier, inc=1, device_id=(dom_peer(k), ray), device_id_type=MESH)
    for k in range(1, quarters):
        pl.semaphore_signal(barrier, inc=1, device_id=(me, ray_next(k)), device_id_type=MESH)

    pairs = [
        (proj_any.at[0], proj_ref, 0),
        (taps_any, taps_ref, 1),
        (carried_any, carried_own, 2),
        (entry_any, lists_ref.at[0], 3),
        (place_any, lists_ref.at[1], 3),
        (slot_any, lists_ref.at[2], 3),
        (library_any.at[0, 0], library_ref, 4),
        (image_any, image_ref, 5),
    ]
    for src, dst, i in pairs:
        pltpu.make_async_copy(src, dst, load_sem.at[i]).start()

    def await_bytes(ref, sem):
        pltpu.make_async_copy(ref, ref, sem).wait()

    def dom_copy(src, dst, send, recv, k):
        pltpu.make_async_remote_copy(
            src_ref=src,
            dst_ref=dst,
            send_sem=send,
            recv_sem=recv,
            device_id=(dom_peer(k), ray),
            device_id_type=MESH,
        ).start()

    def ray_copy(src, dst, send, recv, peer):
        pltpu.make_async_remote_copy(
            src_ref=src,
            dst_ref=dst,
            send_sem=send,
            recv_sem=recv,
            device_id=(me, peer),
            device_id_type=MESH,
        ).start()

    def block(b):
        return proj_ref[:, b * tile : (b + 1) * tile]

    await_bytes(taps_ref, load_sem.at[1])
    taps_wide[...] = jnp.zeros(taps_wide.shape, f32)
    taps_wide[:, : taps_ref.shape[0]] = taps_ref[...].astype(f32)[None]
    spread = jnp.broadcast_to(taps_wide[...], (tile, taps_wide.shape[1]))
    weights = pltpu.roll(spread, half, 1, stride=1, stride_axis=0).astype(bf16)
    await_bytes(proj_ref, load_sem.at[0])
    two = jnp.concatenate(
        [proj_ref[:, (b - 1) * tile : (b + 1) * tile] for b in range(1, count - 1)], axis=0
    )
    third = jnp.concatenate([block(b + 1) for b in range(1, count - 1)], axis=0)
    phase = dot(two, weights[:, : 2 * tile], NT) + dot(third, weights[:, 2 * tile :], NT)
    phase = phase.reshape(inner, owners, per, tile)
    for owner in range(owners):
        phase_out[owner, :inner] = phase[:, owner].astype(bf16)

    await_bytes(carried_own, load_sem.at[2])
    pl.semaphore_wait(barrier, owners + quarters - 2)

    for k in dom_order:
        dom_copy(carried_own, carried_all.at[me], carried_send.at[0], carried_recv.at[0], k)
    ray_copy(
        proj_ref.at[:, pl.ds(columns - tile, tile)],
        rim.at[0],
        halo_send.at[0],
        halo_recv.at[0],
        ray_next(1),
    )
    ray_copy(
        proj_ref.at[:, pl.ds(0, tile)],
        rim.at[1],
        halo_send.at[0],
        halo_recv.at[0],
        ray_next(quarters - 1),
    )
    for k in far_order:
        dom_copy(
            phase_out.at[dom_peer(k), pl.ds(0, inner)],
            phase_in.at[me, pl.ds(0, inner)],
            phase_send.at[0],
            phase_recv.at[0],
            k,
        )

    await_bytes(lists_ref, load_sem.at[3])
    capacity = lists_ref.shape[2]
    entry, place, slot = lists_ref[0], lists_ref[1], lists_ref[2]
    alive = lax.broadcasted_iota(jnp.int32, (1, capacity), 1) < count_ref[0, 0]
    code = jnp.where(alive, slot * places + place, -1)
    pick = jnp.where(
        lax.broadcasted_iota(jnp.int32, (owners * places, capacity), 0) == code, 1.0, 0.0
    ).astype(bf16)
    which = jnp.where(
        lax.broadcasted_iota(jnp.int32, (entries * SUB, capacity), 0) // SUB == entry,
        1.0,
        0.0,
    ).astype(bf16)
    counted[...] = dot(pick, which, NT)
    diagonal = lax.rem(
        lax.broadcasted_iota(jnp.int32, (SUB, entries * SUB), 1), SUB
    ) == lax.broadcasted_iota(jnp.int32, (SUB, entries * SUB), 0)

    def widen(step, carry):
        for i in range(8):
            at = step * 8 + i
            row = jnp.broadcast_to(counted[pl.ds(at, 1), :], (SUB, entries * SUB))
            start = pl.multiple_of(at * SUB, SUB)
            spread_ref[pl.ds(start, SUB), :] = jnp.where(diagonal, row, 0.0).astype(bf16)
        return carry

    lax.fori_loop(0, owners * places // 8, widen, 0)

    await_bytes(library_ref, load_sem.at[4])

    def build(step, carry):
        first = pl.multiple_of(step * 2 * SUB, 2 * SUB)
        right = jnp.concatenate(
            [
                library_ref[:, pl.ds(first + i * SUB, SUB), :].reshape(entries * SUB, tile)
                for i in range(2)
            ],
            axis=1,
        )
        for owner in range(owners):
            rows = places * SUB
            made = dot(spread_ref[owner * rows : (owner + 1) * rows, :], right, NN)
            for place in range(places):
                for i in range(2):
                    start = pl.multiple_of(first + owner * tile + i * SUB, SUB)
                    matrix[pl.ds(start, SUB), place * tile : (place + 1) * tile] = made[
                        place * SUB : (place + 1) * SUB, i * tile : (i + 1) * tile
                    ].astype(bf16)
        return carry

    lax.fori_loop(0, tile // (2 * SUB), build, 0)

    await_bytes(rim, halo_recv.at[0])

    @pl.when(ray == 0)
    def _():
        rim[0] = jnp.zeros((slices, tile), bf16)

    @pl.when(ray == quarters - 1)
    def _():
        rim[1] = jnp.zeros((slices, tile), bf16)

    before, after = rim[0], rim[1]
    two = jnp.concatenate(
        [
            proj_ref[:, (count - 2) * tile : count * tile],
            jnp.concatenate([block(count - 1), after], axis=1),
            jnp.concatenate([before, block(0)], axis=1),
            jnp.concatenate([before, before], axis=1),
        ],
        axis=0,
    )
    third = jnp.concatenate([after, after, block(1), block(0)], axis=0)
    edge = dot(two, weights[:, : 2 * tile], NT) + dot(third, weights[:, 2 * tile :], NT)
    edge = edge.reshape(4, owners, per, tile)
    lane = lax.broadcasted_iota(jnp.int32, (owners, per, tile), 2)
    phase_out[:, inner] = edge[0].astype(bf16)
    phase_out[:, inner + 1] = jnp.where(lane < half, edge[1], edge[3]).astype(bf16)
    phase_out[:, inner + 2] = edge[2].astype(bf16)
    for k in far_order:
        dom_copy(
            phase_out.at[dom_peer(k), pl.ds(inner, 3)],
            phase_in.at[me, pl.ds(inner, 3)],
            phase_send.at[1],
            phase_recv.at[1],
            k,
        )
    phase_in[me] = phase_out[me]

    def send_partials(part):
        chosen = pl.ds(part * some, some)
        for k in far_order:
            dom_copy(
                partial_out.at[dom_peer(k), chosen],
                partial_in.at[me, chosen],
                partial_send.at[0],
                partial_recv.at[part],
                k,
            )

    def send_all_partials():
        for part in range(PARTS):
            send_partials(part)

    await_bytes(image_ref, load_sem.at[5])
    for part in range(PARTS):
        for owner in range(part * some, (part + 1) * some, 2):
            made = dot(image_ref[...], matrix[owner * tile : (owner + 2) * tile, :], NT)
            for i in range(2):
                partial_out[:, owner + i] = (
                    made[:, i * tile : (i + 1) * tile].reshape(owners, per, tile).astype(bf16)
                )
        pl.when(core == 0)(functools.partial(send_partials, part))
    partial_in[me] = partial_out[me]

    def send_twins():
        for k in dom_order:
            dom_copy(
                partial_out.at[pl.ds((1 - dom_peer(k) // side) * side, side), dom_peer(k)],
                twin_in.at[me],
                twin_send.at[0],
                twin_recv.at[0],
                k,
            )

    twin_in[me] = partial_out[pl.ds((1 - group) * side, side), me]

    carried_all[me] = carried_own[...]
    await_bytes(carried_all.at[pl.ds(0, owners - 1)], carried_recv.at[0])
    to_scalar = pltpu.make_async_copy(carried_all, carried_ref, load_sem.at[6])
    to_scalar.start()
    to_scalar.wait()
    duos = [(a, b) for a in range(owners) for b in range(a + 1, owners)]

    def compare(owner, carry):
        for i, (a, b) in enumerate(duos):
            same = jnp.where(carried_ref[owner, 0, a] == carried_ref[owner, 0, b], 1.0, 0.0)
            same_ref[owner, i : i + 1, :] = jnp.full((1, tile), same, f32)
        return carry

    lax.fori_loop(0, owners, compare, 0)

    def profile_of(i):
        return median_of_eight([phase_in[a, i].astype(f32) for a in range(owners)])

    others = pl.ds(0, owners - 1)
    await_bytes(phase_in.at[others, pl.ds(0, inner)], phase_recv.at[0])
    for i in range(inner):
        profile_ref[:, i * tile : (i + 1) * tile] = profile_of(i)
    await_bytes(phase_in.at[others, pl.ds(inner, 3)], phase_recv.at[1])
    pl.when(core == 1)(send_all_partials)
    for i in range(inner, ring):
        profile_ref[:, i * tile : (i + 1) * tile] = profile_of(i)

    width = ring * tile
    detector = quarters * columns
    at = lax.broadcasted_iota(jnp.int32, (1, width), 1)
    position = ray * columns + jnp.where(at < count * tile - half, at + tile, at - columns)
    profile = jnp.where((position >= 0) & (position < detector), profile_ref[...], 0.0)
    run = profile
    reach = 1
    while reach < 2 * SMOOTH:
        run = run + pltpu.roll(run, reach, 1)
        reach *= 2
    window = pltpu.roll(run, width - (SMOOTH - 1), 1) + pltpu.roll(profile, width - SMOOTH, 1)
    in_range = (
        jnp.minimum(position + SMOOTH, detector - 1) - jnp.maximum(position - SMOOTH, 0) + 1
    ).astype(f32)
    stripe = (profile - window / in_range).astype(bf16).astype(f32)
    for b in range(count):
        i = (b - 1) % ring
        stripe_own[b] = stripe[:, i * tile : (i + 1) * tile].astype(bf16)
    for a in range(owners):
        for i in range(ring):
            if i != count - 1:
                fixed[a, i] = (
                    (phase_in[a, i].astype(f32) - stripe[:, i * tile : (i + 1) * tile])
                    .astype(bf16)
                    .astype(f32)
                )

    def ring_spot(b):
        return jnp.where(b == 0, ring - 1, b - 1)

    def carry_back(owner, carry):
        part = [partial_in[d, owner].astype(f32) for d in range(owners)]
        total = list(part)
        for i, (a, b) in enumerate(duos):
            same = jnp.broadcast_to(same_ref[owner, i : i + 1, :], (per, tile))
            total[a] = total[a] + same * part[b]
            total[b] = total[b] + same * part[a]
        for d in range(owners):
            back_out[d, owner] = (
                fixed[owner, ring_spot(carried_ref[owner, 0, d])] - total[d]
            ).astype(bf16)
        return carry

    for part in range(PARTS):
        chosen = pl.ds(part * some, some)
        await_bytes(partial_in.at[others, chosen], partial_recv.at[part])
        lax.fori_loop(part * some, (part + 1) * some, carry_back, 0)
        for k in dom_order:
            dom_copy(
                back_out.at[dom_peer(k), chosen],
                back_in.at[me, chosen],
                back_send.at[0],
                back_recv.at[part * 2 + k // side],
                k,
            )
    back_in[me] = back_out[me]

    def whole(i, carry):
        owner = group * side + i
        part = [partial_in[d, owner].astype(f32) for d in range(owners)]
        where_to = [carried_ref[owner, 0, d] for d in range(owners)]
        for b in range(count):
            total = fixed[owner, (b - 1) % ring]
            taken = jnp.zeros((per, tile), f32)
            for d in range(owners):
                taken = taken + jnp.where(where_to[d] == b, 1.0, 0.0).astype(f32) * part[d]
            rest_out[i, b] = (total - taken).astype(bf16)
        return carry

    lax.fori_loop(0, side, whole, 0)
    dom_copy(stripe_own, stripe_far.at[spot], stripe_send.at[0], stripe_recv.at[0], side)
    for k in range(1, side):
        dom_copy(
            rest_out.at[lax.rem(spot + k, side)],
            rest_in.at[me],
            rest_send.at[0],
            rest_recv.at[0],
            k,
        )
    rest_in[me] = rest_out[spot]

    def rows_of(turn, part):
        first = (group if turn == 0 else 1 - group) * side
        return jnp.concatenate(
            [
                back_in[pl.ds(first, side), owner]
                .astype(f32)
                .reshape(rows_half, tile)
                .astype(bf16)
                for owner in range(part * some, (part + 1) * some)
            ],
            axis=1,
        )

    def send_update(turn, k, sem):
        ray_copy(
            update_out.at[turn, k],
            update_in.at[turn, k],
            update_send.at[0],
            update_recv.at[sem],
            ray_twin(k),
        )

    for turn in range(2):
        for part in range(PARTS):
            await_bytes(
                back_in.at[pl.ds(0, side - 1 + turn), pl.ds(part * some, some)],
                back_recv.at[part * 2 + turn],
            )
            left = rows_of(turn, part)
            rows = slice(part * some * tile, (part + 1) * some * tile)
            for k in (2, 3):
                start = pl.multiple_of(ray_twin(k) * share, share)
                made = dot(left, matrix[rows, pl.ds(start, share)], NN)
                if part > 0:
                    made = made + gathered[k - 2]
                if part < PARTS - 1:
                    gathered[k - 2] = made
                else:
                    update_out[turn, k] = made.astype(bf16)
                    send_update(turn, k, turn)
        if turn == 0:
            send_twins()

    left = jnp.concatenate(
        [
            jnp.concatenate([rows_of(turn, part) for part in range(PARTS)], axis=1)
            for turn in range(2)
        ],
        axis=0,
    )
    start = pl.multiple_of(ray_twin(1) * share, share)
    made = dot(left, matrix[:, pl.ds(start, share)], NN).reshape(2, rows_half, share)
    update_out[:, 1] = made.astype(bf16)
    for turn in range(2):
        send_update(turn, 1, 2)

    await_bytes(stripe_own, stripe_recv.at[0])
    for k in range(1, side):
        dom_copy(
            stripe_far.at[spot], stripe_far.at[spot], stripe_send.at[0], stripe_recv.at[1], k
        )

    start = pl.multiple_of(ray * share, share)
    own_update[...] = dot(left, matrix[:, pl.ds(start, share)], NN).reshape(2, rows_half, share)

    await_bytes(twin_in.at[others], twin_recv.at[0])
    other = pl.ds((1 - group) * side, side)
    own_spots = [carried_ref[me, 0, d] for d in range(owners)]
    taken_by = [twin_in[d].astype(f32) for d in range(owners)]
    for b in range(count):
        taken = jnp.zeros((side, per, tile), f32)
        for d in range(owners):
            taken = taken + jnp.where(own_spots[d] == b, 1.0, 0.0).astype(f32) * taken_by[d]
        forward[b] = taken
    await_bytes(stripe_far.at[pl.ds(0, side - 1)], stripe_recv.at[1])
    for b in range(count):
        clean = (
            (phase_out[other, (b - 1) % ring].astype(f32) - stripe_far[:, b].astype(f32))
            .astype(bf16)
            .astype(f32)
        )
        rest_in[other, b] = (clean - forward[b]).astype(bf16)
    await_bytes(rest_in.at[pl.ds(0, side - 1)], rest_recv.at[0])
    for b in range(count):
        residual_ref[:, b * tile : (b + 1) * tile] = (
            rest_in[:, b].astype(f32).reshape(slices, tile).astype(bf16)
        )

    await_bytes(update_in.at[:, 1], update_recv.at[2])
    for turn in range(2):
        held = group if turn == 0 else 1 - group
        await_bytes(update_in.at[turn, pl.ds(2, quarters - 2)], update_recv.at[turn])
        amount = own_update[turn]
        for k in range(1, quarters):
            amount = amount + update_in[turn, k].astype(f32)
        rows = pl.ds(pl.multiple_of(held * rows_half, rows_half), rows_half)
        old = image_ref[rows, pl.ds(pl.multiple_of(ray * share, share), share)].astype(f32)
        next_ref[rows, :] = old + relax_factor * amount
    await_bytes(carried_all.at[others], carried_send.at[0])
    await_bytes(rim, halo_send.at[0])
    await_bytes(phase_out.at[others, pl.ds(0, inner)], phase_send.at[0])
    await_bytes(phase_out.at[others, pl.ds(inner, 3)], phase_send.at[1])
    await_bytes(partial_out.at[others], partial_send.at[0])
    await_bytes(back_out.at[others], back_send.at[0])
    await_bytes(twin_in.at[others], twin_send.at[0])
    await_bytes(rest_out.at[pl.ds(0, side - 1)], rest_send.at[0])
    await_bytes(stripe_far, stripe_send.at[0])
    await_bytes(update_out.at[:, pl.ds(1, quarters - 1)], update_send.at[0])


def store_kernel(residual_ref, next_ref, residual_out, next_out, sem):
    pairs = [(residual_ref, residual_out), (next_ref, next_out)]
    for i, (src, dst) in enumerate(pairs):
        rows = src.shape[0] // 2
        for part in range(2):
            piece = pl.ds(part * rows, rows)
            pltpu.make_async_copy(src.at[piece], dst.at[piece], sem.at[i]).start()
    for i, (src, dst) in enumerate(pairs):
        pltpu.make_async_copy(src, dst, sem.at[i]).wait()


def fast_shards(
    projections,
    phase_kernel,
    image,
    tile_library,
    tile_entry,
    tile_image,
    tile_slot,
    tile_count,
    slot_block,
):
    f32, bf16 = jnp.float32, jnp.bfloat16
    i32 = jnp.int32
    owners, quarters = lax.axis_size("dom"), lax.axis_size("ray")
    entries, tile = tile_library.shape[2], tile_library.shape[-1]
    _, slices, columns = projections.shape
    count = columns // tile
    ring = count + 1
    places = image.shape[0] // tile
    per = slices // owners
    capacity = tile_entry.shape[2]
    share = places * tile // quarters
    rows_half = slices // 2
    hbm = pl.BlockSpec(memory_space=pltpu.HBM)
    vmem = pl.BlockSpec(memory_space=pltpu.VMEM)
    sems = pltpu.SemaphoreType.DMA
    residual, image_next = pl.pallas_call(
        functools.partial(step_kernel, owners, quarters),
        out_shape=(
            jax.ShapeDtypeStruct((slices, columns), bf16),
            jax.ShapeDtypeStruct((slices, share), f32),
        ),
        in_specs=[hbm] * 8 + [pl.BlockSpec(memory_space=pltpu.SMEM)],
        out_specs=(vmem, vmem),
        scratch_shapes=[
            pltpu.VMEM(phase_kernel.shape, bf16),
            pltpu.VMEM((slices, columns), bf16),
            pltpu.VMEM((slices, places * tile), bf16),
            pltpu.VMEM((entries, tile, tile), bf16),
            pltpu.VMEM((3, 1, capacity), i32),
            pltpu.VMEM((1, owners), i32),
            pltpu.VMEM((owners, 1, owners), i32),
            pltpu.SMEM((owners, 1, owners), i32),
            pltpu.VMEM((1, 3 * tile), f32),
            pltpu.VMEM((2, slices, tile), bf16),
            pltpu.VMEM((owners, ring, per, tile), bf16),
            pltpu.VMEM((owners, ring, per, tile), bf16),
            pltpu.VMEM((per, ring * tile), f32),
            pltpu.VMEM((owners, ring, per, tile), f32),
            pltpu.VMEM((owners * places, entries * SUB), f32),
            pltpu.VMEM((owners * places * SUB, entries * SUB), bf16),
            pltpu.VMEM((owners * tile, places * tile), bf16),
            pltpu.VMEM((owners, owners, per, tile), bf16),
            pltpu.VMEM((owners, owners, per, tile), bf16),
            pltpu.VMEM((owners, 32, tile), f32),
            pltpu.VMEM((owners, owners, per, tile), bf16),
            pltpu.VMEM((owners, owners, per, tile), bf16),
            pltpu.VMEM((owners // 2, count, per, tile), bf16),
            pltpu.VMEM((owners, count, per, tile), bf16),
            pltpu.VMEM((count, per, tile), bf16),
            pltpu.VMEM((owners // 2, count, per, tile), bf16),
            pltpu.VMEM((owners, owners // 2, per, tile), bf16),
            pltpu.VMEM((count, owners // 2, per, tile), f32),
            pltpu.VMEM((2, rows_half, share), f32),
            pltpu.VMEM((2, rows_half, share), f32),
            pltpu.VMEM((2, quarters, rows_half, share), bf16),
            pltpu.VMEM((2, quarters, rows_half, share), bf16),
            sems((7,)),
            sems((1,)),
            sems((1,)),
            sems((1,)),
            sems((1,)),
            sems((2,)),
            sems((2,)),
            sems((1,)),
            sems((PARTS,)),
            sems((1,)),
            sems((2 * PARTS,)),
            sems((1,)),
            sems((1,)),
            sems((1,)),
            sems((2,)),
            sems((1,)),
            sems((1,)),
            sems((1,)),
            sems((3,)),
        ],
        compiler_params=pltpu.CompilerParams(
            collective_id=0, has_side_effects=True, vmem_limit_bytes=48 * 1024 * 1024
        ),
    )(
        *[
            pltpu.with_memory_space_constraint(x, pltpu.HBM)
            for x in (
                phase_kernel,
                projections,
                image.T,
                tile_library,
                tile_entry[0],
                tile_image[0],
                tile_slot[0],
                slot_block[0],
            )
        ],
        tile_count,
    )
    residual, image_next = pl.pallas_call(
        store_kernel,
        out_shape=(
            jax.ShapeDtypeStruct(residual.shape, bf16),
            jax.ShapeDtypeStruct(image_next.shape, f32),
        ),
        in_specs=[pl.BlockSpec(memory_space=pl.ANY)] * 2,
        out_specs=[pl.BlockSpec(memory_space=pl.ANY)] * 2,
        scratch_shapes=[sems((2,))],
    )(
        pltpu.with_memory_space_constraint(residual, pltpu.VMEM),
        pltpu.with_memory_space_constraint(image_next, pltpu.VMEM),
    )
    return residual[None], image_next.T


def fits_kernel(projections, phase_kernel, image, tile_library, tile_entry, *rest):
    owners, quarters = lax.axis_size("dom"), lax.axis_size("ray")
    tile = tile_library.shape[-1]
    angles, slices, columns = projections.shape
    return (
        angles == 1
        and slices % 16 == 0
        and slices == 8 * owners
        and owners == 8
        and tile == 128
        and phase_kernel.shape[0] == tile + 1
        and columns % tile == 0
        and tile_library.shape[2] == 16
        and quarters == 4
        and image.shape[0] == 16 * tile
        and tile_entry.shape[2] <= 256
    )


def any_shards(*args):
    if fits_kernel(*args):
        return fast_shards(*args)
    return shards(*args)


def solution(mesh):
    return jax.shard_map(
        any_shards,
        mesh=mesh,
        in_specs=(
            P("dom", None, "ray"),
            P(),
            P("dom", None),
            P("dom", "ray", None, None, None),
            P("dom", "ray", None),
            P("dom", "ray", None),
            P("dom", "ray", None),
            P("dom", "ray"),
            P("dom", "ray", None),
        ),
        out_specs=(P("dom", None, "ray"), P(("dom", "ray"), None)),
        check_vma=False,
    )
```

```python
import functools

import jax
import jax.numpy as jnp
from jax import lax
from jax.experimental import pallas as pl
from jax.experimental.pallas import tpu as pltpu
from jax.sharding import PartitionSpec as P

SMOOTH = 8


relax_factor = 0.25


def with_halo(cells, sides, width):
    for axis, dim in sides:
        count = lax.axis_size(axis)
        ends = count - 1
        head = lax.slice_in_dim(cells, 0, width, axis=dim)
        tail = lax.slice_in_dim(cells, cells.shape[dim] - width, cells.shape[dim], axis=dim)
        cells = jnp.concatenate(
            [
                lax.ppermute(tail, axis, [(i, (i + 1) % count) for i in range(ends)]),
                cells,
                lax.ppermute(head, axis, [((i + 1) % count, i) for i in range(ends)]),
            ],
            axis=dim,
        )
    return cells


def toeplitz(kernel, tile_size):
    taps = kernel.shape[0]
    padded = jnp.concatenate([kernel, jnp.zeros((2 * tile_size + 1 - taps,), kernel.dtype)])
    tiled = jnp.tile(padded, tile_size)[: 2 * tile_size * tile_size]
    return tiled.reshape(tile_size, 2 * tile_size).T


def phase_filter(projections, phase_kernel, tile_size):
    half_width = (phase_kernel.shape[0] - 1) // 2
    angles, slices, columns = projections.shape
    block_count = columns // tile_size
    rimmed = with_halo(projections, (("ray", 2),), half_width)
    padded = jnp.pad(rimmed, ((0, 0), (0, 0), (0, 2 * tile_size - 2 * half_width)))
    blocks = padded.reshape(angles, slices, block_count + 2, tile_size)
    windows = jnp.concatenate(
        [blocks[:, :, :block_count], blocks[:, :, 1 : block_count + 1]], axis=-1
    )
    filtered = jnp.einsum(
        "asbi,ij->asbj",
        windows,
        toeplitz(phase_kernel, tile_size),
        preferred_element_type=jnp.float32,
    )
    return filtered.reshape(angles, slices, columns).astype(jnp.bfloat16)


def stripe_profile(gathered):
    profile = jnp.median(gathered.astype(jnp.float32), axis=0)
    columns = profile.shape[1]
    rimmed = with_halo(profile, (("ray", 1),), SMOOTH)
    window_sum = jnp.zeros_like(profile)
    for offset in range(2 * SMOOTH + 1):
        window_sum = window_sum + rimmed[:, offset : offset + columns]
    position = lax.axis_index("ray") * columns + jnp.arange(columns)
    detector = lax.axis_size("ray") * columns
    in_range = (
        jnp.minimum(position + SMOOTH, detector - 1) - jnp.maximum(position - SMOOTH, 0) + 1
    ).astype(jnp.float32)
    return (profile - window_sum / in_range).astype(jnp.bfloat16)


def shards(
    projections,
    phase_kernel,
    image,
    tile_library,
    tile_entry,
    tile_image,
    tile_slot,
    tile_count,
    slot_block,
):
    tile_size = tile_library.shape[-1]
    angles, slices, columns = projections.shape
    phase = phase_filter(projections, phase_kernel, tile_size)
    gathered = lax.all_to_all(phase, "dom", split_axis=1, concat_axis=0, tiled=True)
    stripe = stripe_profile(gathered)
    fixed_rows = (gathered.astype(jnp.float32) - stripe.astype(jnp.float32)[None]).astype(
        jnp.bfloat16
    )
    corrected = lax.all_to_all(fixed_rows, "dom", split_axis=0, concat_axis=1, tiled=True)
    owners = lax.axis_size("dom")
    library = tile_library[0, 0]
    entries = tile_entry[0, 0]
    images = tile_image[0, 0]
    slots = tile_slot[0, 0]
    capacity = entries.shape[0]
    block_size = 64
    turn_count = capacity // block_size
    image_blocks = image.reshape(-1, tile_size, slices)
    block_total = image_blocks.shape[0]
    live_mask = jnp.arange(capacity) < tile_count[0, 0]
    slot_target = jnp.where(live_mask, slots, owners)
    image_target = jnp.where(live_mask, images, block_total)

    def forward_turn(turn_index, partial_value):
        first_tile = turn_index * block_size
        chosen = lax.dynamic_slice_in_dim(entries, first_tile, block_size)
        placed = lax.dynamic_slice_in_dim(images, first_tile, block_size)
        destined = lax.dynamic_slice_in_dim(slot_target, first_tile, block_size)
        product = jnp.einsum(
            "krp,kps->ksr",
            library[chosen],
            image_blocks[placed],
            preferred_element_type=jnp.float32,
        )
        return partial_value.at[destined].add(product, mode="drop")

    partial_value = lax.fori_loop(
        0, turn_count, forward_turn, jnp.zeros((owners, slices, tile_size), jnp.float32)
    )
    received = lax.all_to_all(
        partial_value.astype(jnp.bfloat16), "dom", split_axis=0, concat_axis=0, tiled=True
    )
    per_owner = columns // tile_size
    carried = slot_block[0, 0]
    block_ids = jnp.arange(angles * per_owner).reshape(angles, per_owner)
    selector = (block_ids[:, :, None] == carried[None, None, :]).astype(jnp.bfloat16)
    forward = jnp.einsum("abd,dst->asbt", selector, received, preferred_element_type=jnp.float32)
    residual = (corrected.astype(jnp.float32) - forward.reshape(angles, slices, columns)).astype(
        jnp.bfloat16
    )
    back = jnp.einsum(
        "abd,asbt->dst",
        selector,
        residual.reshape(angles, slices, per_owner, tile_size),
        preferred_element_type=jnp.float32,
    ).astype(jnp.bfloat16)
    returned = lax.all_to_all(back, "dom", split_axis=0, concat_axis=0, tiled=True)

    def adjoint_turn(turn_index, gradient):
        first_tile = turn_index * block_size
        chosen = lax.dynamic_slice_in_dim(entries, first_tile, block_size)
        sourced = lax.dynamic_slice_in_dim(slots, first_tile, block_size)
        destined = lax.dynamic_slice_in_dim(image_target, first_tile, block_size)
        product = jnp.einsum(
            "krp,ksr->kps", library[chosen], returned[sourced], preferred_element_type=jnp.float32
        )
        return gradient.at[destined].add(product, mode="drop")

    gradient = lax.fori_loop(
        0, turn_count, adjoint_turn, jnp.zeros((block_total, tile_size, slices), jnp.float32)
    )
    gradient = gradient.reshape(-1, slices)
    rows_own = gradient.shape[0] // lax.axis_size("ray")
    update = lax.psum_scatter(gradient, "ray", scatter_dimension=0, tiled=True)
    own_image = lax.dynamic_slice_in_dim(image, lax.axis_index("ray") * rows_own, rows_own)
    image_next = own_image.astype(jnp.float32) + relax_factor * update
    return (residual, image_next)


MESH = pl.DeviceIdType.MESH
NT = (((1,), (1,)), ((), ()))
NN = (((1,), (0,)), ((), ()))
SUB = 16
PARTS = 4


def dot(a, b, dims):
    return lax.dot_general(a, b, dims, preferred_element_type=jnp.float32)


def ordered(a, b):
    return jnp.minimum(a, b), jnp.maximum(a, b)


def sorted_four(a, b, c, d):
    a, b = ordered(a, b)
    c, d = ordered(c, d)
    a, c = ordered(a, c)
    b, d = ordered(b, d)
    b, c = ordered(b, c)
    return a, b, c, d


def median_of_eight(values):
    low = sorted_four(*values[:4])
    high = sorted_four(*values[4:])
    below = [jnp.minimum(low[i], high[3 - i]) for i in range(4)]
    above = [jnp.maximum(low[i], high[3 - i]) for i in range(4)]
    fourth = jnp.maximum(jnp.maximum(below[0], below[1]), jnp.maximum(below[2], below[3]))
    fifth = jnp.minimum(jnp.minimum(above[0], above[1]), jnp.minimum(above[2], above[3]))
    return (fourth + fifth) * 0.5


def step_kernel(
    owners,
    quarters,
    taps_any,
    proj_any,
    image_any,
    library_any,
    entry_any,
    place_any,
    slot_any,
    carried_any,
    count_ref,
    residual_ref,
    next_ref,
    taps_ref,
    proj_ref,
    image_ref,
    library_ref,
    lists_ref,
    carried_own,
    carried_all,
    carried_ref,
    taps_wide,
    rim,
    phase_out,
    phase_in,
    profile_ref,
    fixed,
    counted,
    spread_ref,
    matrix,
    partial_out,
    partial_in,
    same_ref,
    back_out,
    back_in,
    rest_out,
    rest_in,
    stripe_own,
    stripe_far,
    twin_in,
    forward,
    gathered,
    own_update,
    update_out,
    update_in,
    load_sem,
    halo_send,
    halo_recv,
    carried_send,
    carried_recv,
    phase_send,
    phase_recv,
    partial_send,
    partial_recv,
    back_send,
    back_recv,
    rest_send,
    rest_recv,
    stripe_send,
    stripe_recv,
    twin_send,
    twin_recv,
    update_send,
    update_recv,
):
    f32, bf16 = jnp.float32, jnp.bfloat16
    me, ray = lax.axis_index("dom"), lax.axis_index("ray")
    slices, columns = proj_ref.shape
    entries, tile = library_ref.shape[0], library_ref.shape[-1]
    places = image_ref.shape[1] // tile
    count = columns // tile
    ring = count + 1
    inner = count - 2
    per = slices // owners
    side = owners // 2
    half = tile // 2
    share = places * tile // quarters
    rows_half = side * per
    some = owners // PARTS

    group, spot = me // side, lax.rem(me, side)

    def dom_peer(k):
        if k >= side:
            return (1 - group) * side + lax.rem(spot + k - side, side)
        return group * side + lax.rem(spot + k, side)

    dom_order = list(range(1, owners))
    far_order = list(range(side, owners)) + list(range(1, side))

    chip, core = ray // 2, lax.rem(ray, 2)

    def ray_twin(k):
        chip_to = 1 - chip if k >= 2 else chip
        core_to = 1 - core if k % 2 else core
        return chip_to * 2 + core_to

    def ray_next(k):
        return lax.rem(ray + k, quarters)

    barrier = pltpu.get_barrier_semaphore()
    for k in range(1, owners):
        pl.semaphore_signal(barrier, inc=1, device_id=(dom_peer(k), ray), device_id_type=MESH)
    for k in range(1, quarters):
        pl.semaphore_signal(barrier, inc=1, device_id=(me, ray_next(k)), device_id_type=MESH)

    pairs = [
        (proj_any.at[0], proj_ref, 0),
        (taps_any, taps_ref, 1),
        (carried_any, carried_own, 2),
        (entry_any, lists_ref.at[0], 3),
        (place_any, lists_ref.at[1], 3),
        (slot_any, lists_ref.at[2], 3),
        (library_any.at[0, 0], library_ref, 4),
        (image_any, image_ref, 5),
    ]
    for src, dst, i in pairs:
        pltpu.make_async_copy(src, dst, load_sem.at[i]).start()

    def await_bytes(ref, sem):
        pltpu.make_async_copy(ref, ref, sem).wait()

    def dom_copy(src, dst, send, recv, k):
        pltpu.make_async_remote_copy(
            src_ref=src,
            dst_ref=dst,
            send_sem=send,
            recv_sem=recv,
            device_id=(dom_peer(k), ray),
            device_id_type=MESH,
        ).start()

    def ray_copy(src, dst, send, recv, peer):
        pltpu.make_async_remote_copy(
            src_ref=src,
            dst_ref=dst,
            send_sem=send,
            recv_sem=recv,
            device_id=(me, peer),
            device_id_type=MESH,
        ).start()

    def block(b):
        return proj_ref[:, b * tile : (b + 1) * tile]

    await_bytes(taps_ref, load_sem.at[1])
    taps_wide[...] = jnp.zeros(taps_wide.shape, f32)
    taps_wide[:, : taps_ref.shape[0]] = taps_ref[...].astype(f32)[None]
    spread = jnp.broadcast_to(taps_wide[...], (tile, taps_wide.shape[1]))
    weights = pltpu.roll(spread, half, 1, stride=1, stride_axis=0).astype(bf16)
    await_bytes(proj_ref, load_sem.at[0])
    two = jnp.concatenate(
        [proj_ref[:, (b - 1) * tile : (b + 1) * tile] for b in range(1, count - 1)], axis=0
    )
    third = jnp.concatenate([block(b + 1) for b in range(1, count - 1)], axis=0)
    phase = dot(two, weights[:, : 2 * tile], NT) + dot(third, weights[:, 2 * tile :], NT)
    phase = phase.reshape(inner, owners, per, tile)
    for owner in range(owners):
        phase_out[owner, :inner] = phase[:, owner].astype(bf16)

    await_bytes(carried_own, load_sem.at[2])
    pl.semaphore_wait(barrier, owners + quarters - 2)

    for k in dom_order:
        dom_copy(carried_own, carried_all.at[me], carried_send.at[0], carried_recv.at[0], k)
    ray_copy(
        proj_ref.at[:, pl.ds(columns - tile, tile)],
        rim.at[0],
        halo_send.at[0],
        halo_recv.at[0],
        ray_next(1),
    )
    ray_copy(
        proj_ref.at[:, pl.ds(0, tile)],
        rim.at[1],
        halo_send.at[0],
        halo_recv.at[0],
        ray_next(quarters - 1),
    )
    for k in far_order:
        dom_copy(
            phase_out.at[dom_peer(k), pl.ds(0, inner)],
            phase_in.at[me, pl.ds(0, inner)],
            phase_send.at[0],
            phase_recv.at[0],
            k,
        )

    await_bytes(lists_ref, load_sem.at[3])
    capacity = lists_ref.shape[2]
    entry, place, slot = lists_ref[0], lists_ref[1], lists_ref[2]
    alive = lax.broadcasted_iota(jnp.int32, (1, capacity), 1) < count_ref[0, 0]
    code = jnp.where(alive, slot * places + place, -1)
    pick = jnp.where(
        lax.broadcasted_iota(jnp.int32, (owners * places, capacity), 0) == code, 1.0, 0.0
    ).astype(bf16)
    which = jnp.where(
        lax.broadcasted_iota(jnp.int32, (entries * SUB, capacity), 0) // SUB == entry,
        1.0,
        0.0,
    ).astype(bf16)
    counted[...] = dot(pick, which, NT)
    diagonal = lax.rem(
        lax.broadcasted_iota(jnp.int32, (SUB, entries * SUB), 1), SUB
    ) == lax.broadcasted_iota(jnp.int32, (SUB, entries * SUB), 0)

    def widen(step, carry):
        for i in range(8):
            at = step * 8 + i
            row = jnp.broadcast_to(counted[pl.ds(at, 1), :], (SUB, entries * SUB))
            start = pl.multiple_of(at * SUB, SUB)
            spread_ref[pl.ds(start, SUB), :] = jnp.where(diagonal, row, 0.0).astype(bf16)
        return carry

    lax.fori_loop(0, owners * places // 8, widen, 0)

    await_bytes(library_ref, load_sem.at[4])

    def build(step, carry):
        first = pl.multiple_of(step * 2 * SUB, 2 * SUB)
        right = jnp.concatenate(
            [
                library_ref[:, pl.ds(first + i * SUB, SUB), :].reshape(entries * SUB, tile)
                for i in range(2)
            ],
            axis=1,
        )
        for owner in range(owners):
            rows = places * SUB
            made = dot(spread_ref[owner * rows : (owner + 1) * rows, :], right, NN)
            for place in range(places):
                for i in range(2):
                    start = pl.multiple_of(first + owner * tile + i * SUB, SUB)
                    matrix[pl.ds(start, SUB), place * tile : (place + 1) * tile] = made[
                        place * SUB : (place + 1) * SUB, i * tile : (i + 1) * tile
                    ].astype(bf16)
        return carry

    lax.fori_loop(0, tile // (2 * SUB), build, 0)

    await_bytes(rim, halo_recv.at[0])

    @pl.when(ray == 0)
    def _():
        rim[0] = jnp.zeros((slices, tile), bf16)

    @pl.when(ray == quarters - 1)
    def _():
        rim[1] = jnp.zeros((slices, tile), bf16)

    before, after = rim[0], rim[1]
    two = jnp.concatenate(
        [
            proj_ref[:, (count - 2) * tile : count * tile],
            jnp.concatenate([block(count - 1), after], axis=1),
            jnp.concatenate([before, block(0)], axis=1),
            jnp.concatenate([before, before], axis=1),
        ],
        axis=0,
    )
    third = jnp.concatenate([after, after, block(1), block(0)], axis=0)
    edge = dot(two, weights[:, : 2 * tile], NT) + dot(third, weights[:, 2 * tile :], NT)
    edge = edge.reshape(4, owners, per, tile)
    lane = lax.broadcasted_iota(jnp.int32, (owners, per, tile), 2)
    phase_out[:, inner] = edge[0].astype(bf16)
    phase_out[:, inner + 1] = jnp.where(lane < half, edge[1], edge[3]).astype(bf16)
    phase_out[:, inner + 2] = edge[2].astype(bf16)
    for k in far_order:
        dom_copy(
            phase_out.at[dom_peer(k), pl.ds(inner, 3)],
            phase_in.at[me, pl.ds(inner, 3)],
            phase_send.at[1],
            phase_recv.at[1],
            k,
        )
    phase_in[me] = phase_out[me]

    def send_partials(part, order):
        chosen = pl.ds(part * some, some)
        for k in order:
            dom_copy(
                partial_out.at[dom_peer(k), chosen],
                partial_in.at[me, chosen],
                partial_send.at[0],
                partial_recv.at[part],
                k,
            )

    def send_all_partials():
        for part in range(PARTS):
            send_partials(part, far_order[:side])

    await_bytes(image_ref, load_sem.at[5])
    for part in range(PARTS):
        for owner in range(part * some, (part + 1) * some, 2):
            made = dot(image_ref[...], matrix[owner * tile : (owner + 2) * tile, :], NT)
            for i in range(2):
                partial_out[:, owner + i] = (
                    made[:, i * tile : (i + 1) * tile].reshape(owners, per, tile).astype(bf16)
                )
        pl.when(core == 0)(functools.partial(send_partials, part, far_order[:side]))
        send_partials(part, far_order[side:])
    partial_in[me] = partial_out[me]

    def send_twins():
        for k in dom_order:
            dom_copy(
                partial_out.at[pl.ds((1 - dom_peer(k) // side) * side, side), dom_peer(k)],
                twin_in.at[me],
                twin_send.at[0],
                twin_recv.at[0],
                k,
            )

    twin_in[me] = partial_out[pl.ds((1 - group) * side, side), me]

    carried_all[me] = carried_own[...]
    await_bytes(carried_all.at[pl.ds(0, owners - 1)], carried_recv.at[0])
    to_scalar = pltpu.make_async_copy(carried_all, carried_ref, load_sem.at[6])
    to_scalar.start()
    to_scalar.wait()
    duos = [(a, b) for a in range(owners) for b in range(a + 1, owners)]

    def compare(owner, carry):
        for i, (a, b) in enumerate(duos):
            same = jnp.where(carried_ref[owner, 0, a] == carried_ref[owner, 0, b], 1.0, 0.0)
            same_ref[owner, i : i + 1, :] = jnp.full((1, tile), same, f32)
        return carry

    lax.fori_loop(0, owners, compare, 0)

    def profile_of(i):
        return median_of_eight([phase_in[a, i].astype(f32) for a in range(owners)])

    others = pl.ds(0, owners - 1)
    await_bytes(phase_in.at[others, pl.ds(0, inner)], phase_recv.at[0])
    for i in range(inner):
        profile_ref[:, i * tile : (i + 1) * tile] = profile_of(i)
    await_bytes(phase_in.at[others, pl.ds(inner, 3)], phase_recv.at[1])
    pl.when(core == 1)(send_all_partials)
    for i in range(inner, ring):
        profile_ref[:, i * tile : (i + 1) * tile] = profile_of(i)

    width = ring * tile
    detector = quarters * columns
    at = lax.broadcasted_iota(jnp.int32, (1, width), 1)
    position = ray * columns + jnp.where(at < count * tile - half, at + tile, at - columns)
    profile = jnp.where((position >= 0) & (position < detector), profile_ref[...], 0.0)
    run = profile
    reach = 1
    while reach < 2 * SMOOTH:
        run = run + pltpu.roll(run, reach, 1)
        reach *= 2
    window = pltpu.roll(run, width - (SMOOTH - 1), 1) + pltpu.roll(profile, width - SMOOTH, 1)
    in_range = (
        jnp.minimum(position + SMOOTH, detector - 1) - jnp.maximum(position - SMOOTH, 0) + 1
    ).astype(f32)
    stripe = (profile - window / in_range).astype(bf16).astype(f32)
    for b in range(count):
        i = (b - 1) % ring
        stripe_own[b] = stripe[:, i * tile : (i + 1) * tile].astype(bf16)
    for a in range(owners):
        for i in range(ring):
            if i != count - 1:
                fixed[a, i] = (
                    (phase_in[a, i].astype(f32) - stripe[:, i * tile : (i + 1) * tile])
                    .astype(bf16)
                    .astype(f32)
                )

    def ring_spot(b):
        return jnp.where(b == 0, ring - 1, b - 1)

    def carry_back(owner, carry):
        part = [partial_in[d, owner].astype(f32) for d in range(owners)]
        total = list(part)
        for i, (a, b) in enumerate(duos):
            same = jnp.broadcast_to(same_ref[owner, i : i + 1, :], (per, tile))
            total[a] = total[a] + same * part[b]
            total[b] = total[b] + same * part[a]
        for d in range(owners):
            back_out[d, owner] = (
                fixed[owner, ring_spot(carried_ref[owner, 0, d])] - total[d]
            ).astype(bf16)
        return carry

    for part in range(PARTS):
        chosen = pl.ds(part * some, some)
        await_bytes(partial_in.at[others, chosen], partial_recv.at[part])
        lax.fori_loop(part * some, (part + 1) * some, carry_back, 0)
        for k in dom_order:
            dom_copy(
                back_out.at[dom_peer(k), chosen],
                back_in.at[me, chosen],
                back_send.at[0],
                back_recv.at[part * 2 + k // side],
                k,
            )
    back_in[me] = back_out[me]

    def whole(i, carry):
        owner = group * side + i
        part = [partial_in[d, owner].astype(f32) for d in range(owners)]
        where_to = [carried_ref[owner, 0, d] for d in range(owners)]
        for b in range(count):
            total = fixed[owner, (b - 1) % ring]
            taken = jnp.zeros((per, tile), f32)
            for d in range(owners):
                taken = taken + jnp.where(where_to[d] == b, 1.0, 0.0).astype(f32) * part[d]
            rest_out[i, b] = (total - taken).astype(bf16)
        return carry

    dom_copy(stripe_own, stripe_far.at[spot], stripe_send.at[0], stripe_recv.at[0], side)
    lax.fori_loop(0, side, whole, 0)
    for k in range(1, side):
        dom_copy(
            rest_out.at[lax.rem(spot + k, side)],
            rest_in.at[me],
            rest_send.at[0],
            rest_recv.at[0],
            k,
        )
    rest_in[me] = rest_out[spot]

    def rows_of(turn, part):
        first = (group if turn == 0 else 1 - group) * side
        return jnp.concatenate(
            [
                back_in[pl.ds(first, side), owner]
                .astype(f32)
                .reshape(rows_half, tile)
                .astype(bf16)
                for owner in range(part * some, (part + 1) * some)
            ],
            axis=1,
        )

    def send_update(turn, k, sem):
        ray_copy(
            update_out.at[turn, k],
            update_in.at[turn, k],
            update_send.at[0],
            update_recv.at[sem],
            ray_twin(k),
        )

    for turn in range(2):
        for part in range(PARTS):
            await_bytes(
                back_in.at[pl.ds(0, side - 1 + turn), pl.ds(part * some, some)],
                back_recv.at[part * 2 + turn],
            )
            left = rows_of(turn, part)
            rows = slice(part * some * tile, (part + 1) * some * tile)
            for k in (2, 3):
                start = pl.multiple_of(ray_twin(k) * share, share)
                made = dot(left, matrix[rows, pl.ds(start, share)], NN)
                if part > 0:
                    made = made + gathered[k - 2]
                if part < PARTS - 1:
                    gathered[k - 2] = made
                else:
                    update_out[turn, k] = made.astype(bf16)
                    send_update(turn, k, turn)
        if turn == 0:
            send_twins()

    left = jnp.concatenate(
        [
            jnp.concatenate([rows_of(turn, part) for part in range(PARTS)], axis=1)
            for turn in range(2)
        ],
        axis=0,
    )
    start = pl.multiple_of(ray_twin(1) * share, share)
    made = dot(left, matrix[:, pl.ds(start, share)], NN).reshape(2, rows_half, share)
    update_out[:, 1] = made.astype(bf16)
    for turn in range(2):
        send_update(turn, 1, 2)

    await_bytes(stripe_own, stripe_recv.at[0])
    for k in range(1, side):
        dom_copy(
            stripe_far.at[spot], stripe_far.at[spot], stripe_send.at[0], stripe_recv.at[1], k
        )

    start = pl.multiple_of(ray * share, share)
    own_update[...] = dot(left, matrix[:, pl.ds(start, share)], NN).reshape(2, rows_half, share)

    await_bytes(twin_in.at[others], twin_recv.at[0])
    other = pl.ds((1 - group) * side, side)
    own_spots = [carried_ref[me, 0, d] for d in range(owners)]
    taken_by = [twin_in[d].astype(f32) for d in range(owners)]
    for b in range(count):
        taken = jnp.zeros((side, per, tile), f32)
        for d in range(owners):
            taken = taken + jnp.where(own_spots[d] == b, 1.0, 0.0).astype(f32) * taken_by[d]
        forward[b] = taken
    await_bytes(stripe_far.at[pl.ds(0, side - 1)], stripe_recv.at[1])
    for b in range(count):
        clean = (
            (phase_out[other, (b - 1) % ring].astype(f32) - stripe_far[:, b].astype(f32))
            .astype(bf16)
            .astype(f32)
        )
        rest_in[other, b] = (clean - forward[b]).astype(bf16)
    await_bytes(rest_in.at[pl.ds(0, side - 1)], rest_recv.at[0])
    for b in range(count):
        residual_ref[:, b * tile : (b + 1) * tile] = (
            rest_in[:, b].astype(f32).reshape(slices, tile).astype(bf16)
        )

    await_bytes(update_in.at[:, 1], update_recv.at[2])
    for turn in range(2):
        held = group if turn == 0 else 1 - group
        await_bytes(update_in.at[turn, pl.ds(2, quarters - 2)], update_recv.at[turn])
        amount = own_update[turn]
        for k in range(1, quarters):
            amount = amount + update_in[turn, k].astype(f32)
        rows = pl.ds(pl.multiple_of(held * rows_half, rows_half), rows_half)
        old = image_ref[rows, pl.ds(pl.multiple_of(ray * share, share), share)].astype(f32)
        next_ref[rows, :] = old + relax_factor * amount
    await_bytes(carried_all.at[others], carried_send.at[0])
    await_bytes(rim, halo_send.at[0])
    await_bytes(phase_out.at[others, pl.ds(0, inner)], phase_send.at[0])
    await_bytes(phase_out.at[others, pl.ds(inner, 3)], phase_send.at[1])
    await_bytes(partial_out.at[others], partial_send.at[0])
    await_bytes(back_out.at[others], back_send.at[0])
    await_bytes(twin_in.at[others], twin_send.at[0])
    await_bytes(rest_out.at[pl.ds(0, side - 1)], rest_send.at[0])
    await_bytes(stripe_far, stripe_send.at[0])
    await_bytes(update_out.at[:, pl.ds(1, quarters - 1)], update_send.at[0])


def store_kernel(residual_ref, next_ref, residual_out, next_out, sem):
    pairs = [(residual_ref, residual_out), (next_ref, next_out)]
    for i, (src, dst) in enumerate(pairs):
        rows = src.shape[0] // 2
        for part in range(2):
            piece = pl.ds(part * rows, rows)
            pltpu.make_async_copy(src.at[piece], dst.at[piece], sem.at[i]).start()
    for i, (src, dst) in enumerate(pairs):
        pltpu.make_async_copy(src, dst, sem.at[i]).wait()


def fast_shards(
    projections,
    phase_kernel,
    image,
    tile_library,
    tile_entry,
    tile_image,
    tile_slot,
    tile_count,
    slot_block,
):
    f32, bf16 = jnp.float32, jnp.bfloat16
    i32 = jnp.int32
    owners, quarters = lax.axis_size("dom"), lax.axis_size("ray")
    entries, tile = tile_library.shape[2], tile_library.shape[-1]
    _, slices, columns = projections.shape
    count = columns // tile
    ring = count + 1
    places = image.shape[0] // tile
    per = slices // owners
    capacity = tile_entry.shape[2]
    share = places * tile // quarters
    rows_half = slices // 2
    hbm = pl.BlockSpec(memory_space=pltpu.HBM)
    vmem = pl.BlockSpec(memory_space=pltpu.VMEM)
    sems = pltpu.SemaphoreType.DMA
    residual, image_next = pl.pallas_call(
        functools.partial(step_kernel, owners, quarters),
        out_shape=(
            jax.ShapeDtypeStruct((slices, columns), bf16),
            jax.ShapeDtypeStruct((slices, share), f32),
        ),
        in_specs=[hbm] * 8 + [pl.BlockSpec(memory_space=pltpu.SMEM)],
        out_specs=(vmem, vmem),
        scratch_shapes=[
            pltpu.VMEM(phase_kernel.shape, bf16),
            pltpu.VMEM((slices, columns), bf16),
            pltpu.VMEM((slices, places * tile), bf16),
            pltpu.VMEM((entries, tile, tile), bf16),
            pltpu.VMEM((3, 1, capacity), i32),
            pltpu.VMEM((1, owners), i32),
            pltpu.VMEM((owners, 1, owners), i32),
            pltpu.SMEM((owners, 1, owners), i32),
            pltpu.VMEM((1, 3 * tile), f32),
            pltpu.VMEM((2, slices, tile), bf16),
            pltpu.VMEM((owners, ring, per, tile), bf16),
            pltpu.VMEM((owners, ring, per, tile), bf16),
            pltpu.VMEM((per, ring * tile), f32),
            pltpu.VMEM((owners, ring, per, tile), f32),
            pltpu.VMEM((owners * places, entries * SUB), f32),
            pltpu.VMEM((owners * places * SUB, entries * SUB), bf16),
            pltpu.VMEM((owners * tile, places * tile), bf16),
            pltpu.VMEM((owners, owners, per, tile), bf16),
            pltpu.VMEM((owners, owners, per, tile), bf16),
            pltpu.VMEM((owners, 32, tile), f32),
            pltpu.VMEM((owners, owners, per, tile), bf16),
            pltpu.VMEM((owners, owners, per, tile), bf16),
            pltpu.VMEM((owners // 2, count, per, tile), bf16),
            pltpu.VMEM((owners, count, per, tile), bf16),
            pltpu.VMEM((count, per, tile), bf16),
            pltpu.VMEM((owners // 2, count, per, tile), bf16),
            pltpu.VMEM((owners, owners // 2, per, tile), bf16),
            pltpu.VMEM((count, owners // 2, per, tile), f32),
            pltpu.VMEM((2, rows_half, share), f32),
            pltpu.VMEM((2, rows_half, share), f32),
            pltpu.VMEM((2, quarters, rows_half, share), bf16),
            pltpu.VMEM((2, quarters, rows_half, share), bf16),
            sems((7,)),
            sems((1,)),
            sems((1,)),
            sems((1,)),
            sems((1,)),
            sems((2,)),
            sems((2,)),
            sems((1,)),
            sems((PARTS,)),
            sems((1,)),
            sems((2 * PARTS,)),
            sems((1,)),
            sems((1,)),
            sems((1,)),
            sems((2,)),
            sems((1,)),
            sems((1,)),
            sems((1,)),
            sems((3,)),
        ],
        compiler_params=pltpu.CompilerParams(
            collective_id=0, has_side_effects=True, vmem_limit_bytes=48 * 1024 * 1024
        ),
    )(
        *[
            pltpu.with_memory_space_constraint(x, pltpu.HBM)
            for x in (
                phase_kernel,
                projections,
                image.T,
                tile_library,
                tile_entry[0],
                tile_image[0],
                tile_slot[0],
                slot_block[0],
            )
        ],
        tile_count,
    )
    residual, image_next = pl.pallas_call(
        store_kernel,
        out_shape=(
            jax.ShapeDtypeStruct(residual.shape, bf16),
            jax.ShapeDtypeStruct(image_next.shape, f32),
        ),
        in_specs=[pl.BlockSpec(memory_space=pl.ANY)] * 2,
        out_specs=[pl.BlockSpec(memory_space=pl.ANY)] * 2,
        scratch_shapes=[sems((2,))],
    )(
        pltpu.with_memory_space_constraint(residual, pltpu.VMEM),
        pltpu.with_memory_space_constraint(image_next, pltpu.VMEM),
    )
    return residual[None], image_next.T


def fits_kernel(projections, phase_kernel, image, tile_library, tile_entry, *rest):
    owners, quarters = lax.axis_size("dom"), lax.axis_size("ray")
    tile = tile_library.shape[-1]
    angles, slices, columns = projections.shape
    return (
        angles == 1
        and slices % 16 == 0
        and slices == 8 * owners
        and owners == 8
        and tile == 128
        and phase_kernel.shape[0] == tile + 1
        and columns % tile == 0
        and tile_library.shape[2] == 16
        and quarters == 4
        and image.shape[0] == 16 * tile
        and tile_entry.shape[2] <= 256
    )


def any_shards(*args):
    if fits_kernel(*args):
        return fast_shards(*args)
    return shards(*args)


def solution(mesh):
    return jax.shard_map(
        any_shards,
        mesh=mesh,
        in_specs=(
            P("dom", None, "ray"),
            P(),
            P("dom", None),
            P("dom", "ray", None, None, None),
            P("dom", "ray", None),
            P("dom", "ray", None),
            P("dom", "ray", None),
            P("dom", "ray"),
            P("dom", "ray", None),
        ),
        out_specs=(P("dom", None, "ray"), P(("dom", "ray"), None)),
        check_vma=False,
    )
```
